32 devices in a mesh: dp: 4 (over y, x), fsdp: 8 (over z, core).
Axes of the slice: x: 2, y: 2, z: 4, core: 2. Of those that a mesh axis runs over, the one named last changes fastest.
Arguments:
- tokens: bfloat16 [32, 1536, 768], P(('dp', 'fsdp')), may hold values from -6 to 6
- cotangent: bfloat16 [32, 1536, 768], P(('dp', 'fsdp')), may hold values from -6 to 6
- lengths: int32 [32, 6], P(('dp', 'fsdp')), may hold values from 0 to 1374, as said below
- step: int32 [1], replicated, may hold values from 2 to 20
- weight_qkv: float32 [768, 2304], P(('dp', 'fsdp')), may hold values from -0.21875 to 0.21875
- weight_proj: float32 [768, 768], P(('dp', 'fsdp')), may hold values from -1.5 to 1.5
- weight_fc1: float32 [768, 3072], P(('dp', 'fsdp')), may hold values from -0.21875 to 0.21875
- weight_fc2: float32 [3072, 768], P(('dp', 'fsdp')), may hold values from -0.109375 to 0.109375
- vectors: float32 [768, 14], P(('dp', 'fsdp'))
- first_qkv: float32 [768, 2304], P(('dp', 'fsdp')), may hold values from -0.00061035156 to 0.00061035156
- second_qkv: float32 [768, 2304], P(('dp', 'fsdp')), may hold values from 5.642831e-10 to 8.464247e-09
- first_proj: float32 [768, 768], P(('dp', 'fsdp')), may hold values from -0.00061035156 to 0.00061035156
- second_proj: float32 [768, 768], P(('dp', 'fsdp')), may hold values from 5.642831e-10 to 8.464247e-09
- first_fc1: float32 [768, 3072], P(('dp', 'fsdp')), may hold values from -0.00061035156 to 0.00061035156
- second_fc1: float32 [768, 3072], P(('dp', 'fsdp')), may hold values from 5.642831e-10 to 8.464247e-09
- first_fc2: float32 [3072, 768], P(('dp', 'fsdp')), may hold values from -0.00061035156 to 0.00061035156
- second_fc2: float32 [3072, 768], P(('dp', 'fsdp')), may hold values from 5.642831e-10 to 8.464247e-09
- first_vectors: float32 [768, 14], P(('dp', 'fsdp')), may hold values from -0.001953125 to 0.001953125
- second_vectors: float32 [768, 14], P(('dp', 'fsdp')), may hold values from 5.6428315e-09 to 8.464247e-08
Outputs:
- out_tokens: bfloat16 [32, 1536, 768], P(('dp', 'fsdp'))
- grad_tokens: bfloat16 [32, 1536, 768], P(('dp', 'fsdp'))
- grad_norm: float32 [1], replicated
- new_qkv: float32 [768, 2304], P(('dp', 'fsdp'))
- new_proj: float32 [768, 768], P(('dp', 'fsdp'))
- new_fc1: float32 [768, 3072], P(('dp', 'fsdp'))
- new_fc2: float32 [3072, 768], P(('dp', 'fsdp'))
- new_vectors: float32 [768, 14], P(('dp', 'fsdp'))
- new_first_qkv: float32 [768, 2304], P(('dp', 'fsdp'))
- new_second_qkv: float32 [768, 2304], P(('dp', 'fsdp'))
- new_first_proj: float32 [768, 768], P(('dp', 'fsdp'))
- new_second_proj: float32 [768, 768], P(('dp', 'fsdp'))
- new_first_fc1: float32 [768, 3072], P(('dp', 'fsdp'))
- new_second_fc1: float32 [768, 3072], P(('dp', 'fsdp'))
- new_first_fc2: float32 [3072, 768], P(('dp', 'fsdp'))
- new_second_fc2: float32 [3072, 768], P(('dp', 'fsdp'))
- new_first_vectors: float32 [768, 14], P(('dp', 'fsdp'))
- new_second_vectors: float32 [768, 14], P(('dp', 'fsdp'))
The draws below stay inside these ranges and needn't reach their ends.
Inputs may be any that keep to these rules, and one draw needn't show every extreme that they name: `lengths`: each row holds either one sequence of 1374 tokens in its first slot or 5 sequences of 261 tokens; other slots are 0; the positions after a row's sequences form one more segment. Both kinds of rows occur.
All inputs are finite; a program needn't handle non-finite values.
Results may differ from the reference program's by a relative error of at most 0.01.
The reference program's roundings to bfloat16 on the way count: a program that leaves them out, or rounds other values in their place, can miss the bound.
Values may be sent and summed in bfloat16 or wider, within the bound.
No kernel may reach another device: no remote copies, remote signals or barrier semaphores. Data moves between devices by JAX's collectives and lax.ppermute only.
A program may use at most 192 MiB of HBM per device.

```python
import math
import jax
import jax.numpy as jnp
from jax import lax

D = 768
HEADS = 12
HEAD_DIM = 64
FF = 3072
GLEN = 1374
LLEN = 261
SEGS = 6
ROW = 1536
ROWS = 32
NVEC = 14
PARAMS = 7088640


def draw_lengths(key, part):
    kinds = jax.random.randint(key, (ROWS,), 0, 2)
    places = jnp.arange(ROWS, dtype=jnp.int32)
    kinds = jnp.where(places == 0, 1, jnp.where(places == 1, 0, kinds))
    slots = jnp.arange(SEGS, dtype=jnp.int32)
    global_row = jnp.where(slots == 0, GLEN, 0)
    local_row = jnp.where(slots < SEGS - 1, LLEN, 0)
    return jnp.where(kinds[:, None] == 1, global_row[None, :], local_row[None, :]).astype(jnp.int32)


def draw_vectors(key, part):
    keys = jax.random.split(key, 3)
    wide = FF // D
    place = jnp.arange(D, dtype=jnp.float32) / D
    rise = 0.5 * jnp.exp(math.log(3.0) * place)
    gains = rise[:, None] * jax.random.uniform(keys[0], (D, 2), jnp.float32, 0.85, 1.15)
    normals = jax.random.normal(keys[1], (D, 6 + wide), jnp.float32)
    layer = jax.random.uniform(keys[2], (D, 2), jnp.float32, 0.5, 1.5)
    columns = [gains[:, 0], 0.3 * normals[:, 0], 0.5 * normals[:, 1], 0.5 * normals[:, 2], 0.3 * normals[:, 3], layer[:, 0], gains[:, 1], 0.3 * normals[:, 4]]
    columns = columns + [0.5 * normals[:, 6 + i] for i in range(wide)]
    columns = columns + [0.3 * normals[:, 5], layer[:, 1]]
    return jnp.stack(columns, axis=1)


def block_levels(rng, extent, cuts, least, high):
    level = 1.0
    for position, shards_of in cuts:
        draws = jax.random.uniform(jax.random.fold_in(jax.random.fold_in(rng, 6), position), (shards_of,), jnp.float32, least / len(cuts), high / len(cuts))
        level = level * jnp.repeat(jnp.exp(draws), extent[position] // shards_of).reshape((-1,) + (1,) * (len(extent) - 1 - position))
    return level


def noise(key, dims, deviation, reach, shards=(), held_as=jnp.bfloat16):
    level = block_levels(key, dims, shards, -0.22, 0.18) if shards else 1.0
    drawn = jax.random.normal(key, dims, jnp.float32) * deviation * level
    return jnp.minimum(jnp.maximum(drawn, -reach), reach).astype(held_as)


def setup_inputs(seed: int = 0) -> dict:
    seeds = jax.random.split(jax.random.key(seed), 20)
    tokens = noise(seeds[0], (ROWS, ROW, D), 1.0, 6.0, ((0, 32),))
    cotangent = noise(seeds[1], (ROWS, ROW, D), 1.0, 6.0, ((0, 32),))
    lengths = draw_lengths(jax.random.fold_in(seeds[19], 71), 0)
    step = jax.random.randint(seeds[3], (1,), 2, 21).astype(jnp.int32)
    weight_qkv = noise(seeds[4], (D, 3 * D), D ** -0.5, 0.21875, ((0, 32),), jnp.float32)
    weight_proj = noise(seeds[5], (D, D), (D // 48) ** -0.5, 1.5, ((0, 32),), jnp.float32)
    weight_fc1 = noise(seeds[6], (D, FF), D ** -0.5, 0.21875, ((0, 32),), jnp.float32)
    weight_fc2 = noise(seeds[7], (FF, D), FF ** -0.5, 0.109375, ((0, 32),), jnp.float32)
    vectors = draw_vectors(jax.random.fold_in(seeds[19], 71), 0)
    first_qkv = noise(seeds[9], (D, 3 * D), (0.3 / PARAMS ** 0.5), 0.00061035156, ((0, 32),), jnp.float32)
    second_qkv = jnp.clip(jnp.exp(math.log(8.464247081008125e-09) - 2.7080502 * jax.random.uniform(seeds[10], (D, 3 * D), jnp.float32) ** block_levels(seeds[10], (D, 3 * D), ((0, 32),), -0.2, 0.2)), 5.642831202301579e-10, 8.464247081008125e-09)
    first_proj = noise(seeds[11], (D, D), (0.3 / PARAMS ** 0.5), 0.00061035156, ((0, 32),), jnp.float32)
    second_proj = jnp.clip(jnp.exp(math.log(8.464247081008125e-09) - 2.7080502 * jax.random.uniform(seeds[12], (D, D), jnp.float32) ** block_levels(seeds[12], (D, D), ((0, 32),), -0.2, 0.2)), 5.642831202301579e-10, 8.464247081008125e-09)
    first_fc1 = noise(seeds[13], (D, FF), (0.3 / PARAMS ** 0.5), 0.00061035156, ((0, 32),), jnp.float32)
    second_fc1 = jnp.clip(jnp.exp(math.log(8.464247081008125e-09) - 2.7080502 * jax.random.uniform(seeds[14], (D, FF), jnp.float32) ** block_levels(seeds[14], (D, FF), ((0, 32),), -0.2, 0.2)), 5.642831202301579e-10, 8.464247081008125e-09)
    first_fc2 = noise(seeds[15], (FF, D), (0.3 / PARAMS ** 0.5), 0.00061035156, ((0, 32),), jnp.float32)
    second_fc2 = jnp.clip(jnp.exp(math.log(8.464247081008125e-09) - 2.7080502 * jax.random.uniform(seeds[16], (FF, D), jnp.float32) ** block_levels(seeds[16], (FF, D), ((0, 32),), -0.2, 0.2)), 5.642831202301579e-10, 8.464247081008125e-09)
    first_vectors = noise(seeds[17], (D, NVEC), (1.0 / PARAMS ** 0.5), 0.001953125, ((0, 32),), jnp.float32)
    second_vectors = jnp.clip(jnp.exp(math.log(8.464247258643809e-08) - 2.7080502 * jax.random.uniform(seeds[18], (D, NVEC), jnp.float32) ** block_levels(seeds[18], (D, NVEC), ((0, 32),), -0.2, 0.2)), 5.6428315353684866e-09, 8.464247258643809e-08)
    return {"tokens": tokens, "cotangent": cotangent, "lengths": lengths, "step": step, "weight_qkv": weight_qkv, "weight_proj": weight_proj, "weight_fc1": weight_fc1, "weight_fc2": weight_fc2, "vectors": vectors, "first_qkv": first_qkv, "second_qkv": second_qkv, "first_proj": first_proj, "second_proj": second_proj, "first_fc1": first_fc1, "second_fc1": second_fc1, "first_fc2": first_fc2, "second_fc2": second_fc2, "first_vectors": first_vectors, "second_vectors": second_vectors}


@jax.custom_vjp
def low(v):
    return lax.optimization_barrier(v.astype(jnp.bfloat16)).astype(jnp.float32)

@jax.custom_vjp
def low_back(v):
    return v

def low_keep(v):
    return (low(v), None)

def low_pass(kept, grad):
    return (grad,)

def back_keep(v):
    return (v, None)

def back_low(kept, grad):
    return (low(grad),)
low.defvjp(low_keep, low_pass)
low_back.defvjp(back_keep, back_low)
HIGH = lax.Precision.HIGHEST
NORM_EPS = 1e-06
BETA_ONE = 0.9
BETA_TWO = 0.999
ADAM_EPS = 1e-08
CLIP_LIMIT = 3.0

def layer_norm(values, gain, shift):
    center = values - lax.optimization_barrier(jnp.mean(values, axis=-1, keepdims=True))
    spread = lax.optimization_barrier(jnp.mean(center * center, axis=-1, keepdims=True))
    return center * lax.rsqrt(spread + NORM_EPS) * gain + shift

def segment_ids(line, count):
    ends = jnp.cumsum(line, dtype=jnp.int32)
    places = jnp.arange(count, dtype=jnp.int32)
    return lax.optimization_barrier(jnp.sum((places[:, None] >= ends[None, :]).astype(jnp.int32), axis=1))

def unpack(vec):
    wide = FF // D
    fc1_bias = vec[:, 8:8 + wide].T.reshape(FF)
    return (vec[:, 0], vec[:, 1], vec[:, 2], vec[:, 3], vec[:, 4], vec[:, 5], vec[:, 6], vec[:, 7], fc1_bias, vec[:, 8 + wide], vec[:, 9 + wide])

def block_row(params, row_x, row_ids):
    w_qkv, w_proj, w_fc1, w_fc2, vec = params
    gain_one, shift_one, bias_q, bias_v, bias_o, scale_one, gain_two, shift_two, bias_up, bias_down, scale_two = unpack(vec)
    normed = low(layer_norm(row_x, gain_one, shift_one))
    bias = jnp.concatenate([bias_q, jnp.zeros_like(bias_q), bias_v])
    qkv = low(low_back(jnp.dot(normed, w_qkv, precision=HIGH) + bias))
    heads = qkv.reshape(ROW, 3, HEADS, HEAD_DIM)
    query, keys, values = (heads[:, 0], heads[:, 1], heads[:, 2])
    raw = jnp.einsum('qhd,khd->hqk', query, keys, precision=HIGH)
    scores = low_back(raw * HEAD_DIM ** (-0.5))
    same = row_ids[:, None] == row_ids[None, :]
    scores = jnp.where(same[None], scores, -1000000000.0)
    top = lax.optimization_barrier(jnp.max(scores, axis=-1, keepdims=True))
    total = top + jnp.log(lax.optimization_barrier(jnp.sum(jnp.exp(scores - top), axis=-1, keepdims=True)))
    probs = low(jnp.exp(scores - total))
    mixed = jnp.einsum('hqk,khd->qhd', probs, values, precision=HIGH).reshape(ROW, D)
    mixed = low(low_back(mixed))
    branch = low_back(jnp.dot(mixed, w_proj, precision=HIGH) + bias_o)
    middle = row_x + scale_one * branch
    normed_two = low(layer_norm(middle, gain_two, shift_two))
    inner = low_back(jnp.dot(normed_two, w_fc1, precision=HIGH) + bias_up)
    active = low(jax.nn.gelu(inner, approximate=False))
    out_branch = low_back(jnp.dot(active, w_fc2, precision=HIGH) + bias_down)
    return middle + scale_two * out_branch

def adam_update(weight, grad, first, second, rate, decay, fix_one, fix_two):
    first = BETA_ONE * first + (1.0 - BETA_ONE) * grad
    second = BETA_TWO * second + (1.0 - BETA_TWO) * grad * grad
    stride = first / fix_one / (jnp.sqrt(second / fix_two) + ADAM_EPS)
    return (weight - rate * (stride + decay * weight), first, second)

def reference(tokens, cotangent, lengths, step, weight_qkv, weight_proj, weight_fc1, weight_fc2, vectors, first_qkv, second_qkv, first_proj, second_proj, first_fc1, second_fc1, first_fc2, second_fc2, first_vectors, second_vectors):
    ids = jax.vmap(lambda line: segment_ids(line, ROW))(lengths)
    inputs = tokens.astype(jnp.float32)
    masters = (weight_qkv, weight_proj, weight_fc1, weight_fc2, vectors)
    row_step = jax.checkpoint(block_row)

    def forward(params, values):
        rounded = tuple((low(p) for p in params))
        return lax.map(lambda pair: row_step(rounded, pair[0], pair[1]), (values, ids))
    result, pull = jax.vjp(forward, masters, inputs)
    grads, grad_x = pull(cotangent.astype(jnp.float32))
    total = jnp.sum(grads[0] * grads[0]) + jnp.sum(grads[1] * grads[1]) + jnp.sum(grads[2] * grads[2])
    total = total + jnp.sum(grads[3] * grads[3]) + jnp.sum(grads[4] * grads[4])
    norm = jnp.sqrt(total)
    factor = jnp.minimum(1.0, CLIP_LIMIT / (norm + 1e-06))
    count = step[0].astype(jnp.float32)
    fix_one = 1.0 - jnp.power(BETA_ONE, count)
    fix_two = 1.0 - jnp.power(BETA_TWO, count)
    rate_in = 2.0 / math.sqrt(D)
    new_qkv, new_first_qkv, new_second_qkv = adam_update(weight_qkv, factor * grads[0], first_qkv, second_qkv, rate_in, 0.04, fix_one, fix_two)
    new_proj, new_first_proj, new_second_proj = adam_update(weight_proj, factor * grads[1], first_proj, second_proj, 2.0 / math.sqrt(D // 48), 0.04, fix_one, fix_two)
    new_fc1, new_first_fc1, new_second_fc1 = adam_update(weight_fc1, factor * grads[2], first_fc1, second_fc1, rate_in, 0.04, fix_one, fix_two)
    new_fc2, new_first_fc2, new_second_fc2 = adam_update(weight_fc2, factor * grads[3], first_fc2, second_fc2, 2.0 / math.sqrt(FF), 0.04, fix_one, fix_two)
    new_vectors, new_first_vectors, new_second_vectors = adam_update(vectors, factor * grads[4], first_vectors, second_vectors, 1.0, 0.0, fix_one, fix_two)
    return (result.astype(jnp.bfloat16), grad_x.astype(jnp.bfloat16), norm.reshape(1), new_qkv, new_proj, new_fc1, new_fc2, new_vectors, new_first_qkv, new_second_qkv, new_first_proj, new_second_proj, new_first_fc1, new_second_fc1, new_first_fc2, new_second_fc2, new_first_vectors, new_second_vectors)
```

```python
import math

import jax
import jax.numpy as jnp
from jax import lax
from jax.experimental import pallas as pl
from jax.experimental.pallas import tpu as pltpu
from jax.sharding import PartitionSpec as P

bf=jnp.bfloat16
f32=jnp.float32

D = 768
HEADS = 12
HEAD_DIM = 64
FF = 3072


NORM_EPS = 1e-06
BETA_ONE = 0.9
BETA_TWO = 0.999
ADAM_EPS = 1e-08
CLIP_LIMIT = 3.0


def layer_norm(values, gain, shift):
    center = values - jnp.mean(values, axis=-1, keepdims=True)
    spread = jnp.mean(center * center, axis=-1, keepdims=True)
    return center * lax.rsqrt(spread + NORM_EPS) * gain + shift


def exact_gelu(values):
    return jax.nn.gelu(values, approximate=False)


def segment_ids(line, count):
    ends = jnp.cumsum(line, dtype=jnp.int32)
    places = jnp.arange(count, dtype=jnp.int32)
    return jnp.sum((places[:, None] >= ends[None, :]).astype(jnp.int32), axis=1)


def unpack(vec):
    wide = FF // D
    fc1_bias = vec[:, 8 : 8 + wide].T.reshape(FF)
    return (
        vec[:, 0],
        vec[:, 1],
        vec[:, 2],
        vec[:, 3],
        vec[:, 4],
        vec[:, 5],
        vec[:, 6],
        vec[:, 7],
        fc1_bias,
        vec[:, 8 + wide],
        vec[:, 9 + wide],
    )


ROW=1536; BQ=256; NQ=ROW//BQ; SEGS=6
LOG2E=1.4426950408889634
BIG=float(2**30)
def nt(a,b): return lax.dot_general(a,b,(((1,),(1,)),((),())),preferred_element_type=f32)
def nn(a,b): return jnp.dot(a,b,preferred_element_type=f32)
def seg_onehot(len_ref, rows):
    pos=lax.broadcasted_iota(jnp.int32,(rows,128),0)
    lane=lax.broadcasted_iota(jnp.int32,(rows,128),1)
    idx=jnp.zeros((rows,128),jnp.int32)
    end=jnp.int32(0)
    for s in range(SEGS):
        end=end+len_ref[0,s]
        idx=idx+(pos>=end).astype(jnp.int32)
    return (idx==lane).astype(f32)
def prep(len_ref,q_ref,k_ref,qa,qb,ka,kb,first):
    lane=lax.broadcasted_iota(jnp.int32,(ROW,128),1); low=lane<64
    @pl.when(first)
    def _():
        oh=seg_onehot(len_ref,ROW)
        qa[:,128:256]=oh.astype(bf); qb[:,128:256]=oh.astype(bf)
        km=((oh-1.0)*BIG).astype(bf)
        ka[:,128:256]=km; kb[:,128:256]=km
    k=k_ref[...].astype(f32); kr=pltpu.roll(k,64,axis=1)
    ka[:,0:128]=jnp.where(low,k,kr).astype(bf); kb[:,0:128]=jnp.where(low,kr,k).astype(bf)
    q=q_ref[...].astype(f32)*(LOG2E*0.125); hi=q.astype(bf).astype(f32); lo=q-hi
    qa[:,0:128]=jnp.where(low,hi,pltpu.roll(lo,64,axis=1)).astype(bf)
    qb[:,0:128]=jnp.where(low,pltpu.roll(hi,64,axis=1),lo).astype(bf)
def fwd_kernel(len_ref,q_ref,k_ref,v_ref,o_ref,lse_ref,qa,qb,ka,kb,va,vb,sa,sb,ot):
    hp=pl.program_id(0)
    prep(len_ref,q_ref,k_ref,qa,qb,ka,kb,hp==0)
    vt=v_ref[...].T
    @pl.when(hp==0)
    def _():
        one=(lax.broadcasted_iota(jnp.int32,(16,ROW),0)==0).astype(bf)
        va[64:80,:]=one; vb[64:80,:]=one
    va[0:64,:]=vt[0:64,:]; vb[0:64,:]=vt[64:128,:]
    sa[...]=nt(ka[...],qa[0:BQ,:])
    def soft(s_ref,v_sc,j,r):
        s=s_ref[...]
        m=jnp.max(s,axis=0,keepdims=True)
        e=jnp.exp2(s-m).astype(bf)
        o=nn(v_sc[...],e)
        l=o[64:65,:]
        cols=pl.ds(pl.multiple_of(j*BQ,BQ),BQ)
        ot[64*r:64*r+64,cols]=o[0:64,:]*(1.0/l)
        lse_ref[0,r:r+1,cols]=m+jnp.log2(l)
    def body(j,c):
        rows=pl.ds(pl.multiple_of(j*BQ,BQ),BQ)
        nrow=pl.ds(pl.multiple_of(jnp.minimum(j+1,NQ-1)*BQ,BQ),BQ)
        sb[...]=nt(kb[...],qb[rows,:])
        soft(sa,va,j,0)
        sa[...]=nt(ka[...],qa[nrow,:])
        soft(sb,vb,j,1)
        return c
    lax.fori_loop(0,NQ,body,0)
    o_ref[...]=ot[...].T.astype(bf)
def attn_fwd(lengths,qkv):
    H=6
    return pl.pallas_call(fwd_kernel,grid=(H,),
        in_specs=[pl.BlockSpec(memory_space=pltpu.SMEM),
            pl.BlockSpec((ROW,128),lambda h:(0,h)),pl.BlockSpec((ROW,128),lambda h:(0,6+h)),pl.BlockSpec((ROW,128),lambda h:(0,12+h))],
        out_specs=[pl.BlockSpec((ROW,128),lambda h:(0,h)),pl.BlockSpec((1,8,ROW),lambda h:(h,0,0))],
        out_shape=[jax.ShapeDtypeStruct((ROW,768),bf),jax.ShapeDtypeStruct((6,8,ROW),f32)],
        scratch_shapes=[pltpu.VMEM((ROW,256),bf)]*4+[pltpu.VMEM((80,ROW),bf)]*2+[pltpu.VMEM((ROW,BQ),f32)]*2+[pltpu.VMEM((128,ROW),f32)],
        compiler_params=pltpu.CompilerParams(vmem_limit_bytes=60<<20),name="attn_fwd")(lengths,qkv,qkv,qkv)

def bwd_kernel(len_ref,q_ref,k_ref,v_ref,o_ref,do_ref,lse_ref,dq_ref,dk_ref,dv_ref,
               qa,qb,ka,kb,kt,da,db,qma,qmb,drow,xa,ya,xb,yb,dqt,dka,dva):
    hp=pl.program_id(0)
    prep(len_ref,q_ref,k_ref,qa,qb,ka,kb,hp==0)
    lane=lax.broadcasted_iota(jnp.int32,(ROW,128),1); low=lane<64
    kt[...]=k_ref[...].T
    do=do_ref[...]; z=jnp.zeros_like(do)
    da[...]=jnp.where(low,do,z); db[...]=jnp.where(low,z,do)
    q=q_ref[...]
    qma[...]=jnp.where(low,q,z); qmb[...]=jnp.where(low,z,q)
    pr=(do.astype(f32)*o_ref[...].astype(f32)).T
    drow[0:1,:]=jnp.sum(pr[0:64],axis=0,keepdims=True)
    drow[1:2,:]=jnp.sum(pr[64:128],axis=0,keepdims=True)
    dka[...]=jnp.zeros_like(dka); dva[...]=jnp.zeros_like(dva)
    def mm(k_sc,q_sc,d_sc,x,y,rows):
        x[...]=nt(k_sc[...],q_sc[rows,:])
        y[...]=nt(v_ref[...],d_sc[rows,:])
    def rest(x,y,d_sc,qm,r,rows):
        p=jnp.exp2(x[...]-lse_ref[0,r:r+1,rows])
        ds=(p*(y[...]-drow[r:r+1,rows])).astype(bf)
        dva[...]+=nn(p.astype(bf),d_sc[rows,:])
        dka[...]+=nn(ds,qm[rows,:])
        dqt[64*r:64*r+64,rows]=nn(kt[64*r:64*r+64,:],ds)
    mm(ka,qa,da,xa,ya,pl.ds(0,BQ))
    def body(j,c):
        rows=pl.ds(pl.multiple_of(j*BQ,BQ),BQ)
        nrow=pl.ds(pl.multiple_of(jnp.minimum(j+1,NQ-1)*BQ,BQ),BQ)
        mm(kb,qb,db,xb,yb,rows)
        rest(xa,ya,da,qma,0,rows)
        mm(ka,qa,da,xa,ya,nrow)
        rest(xb,yb,db,qmb,1,rows)
        return c
    lax.fori_loop(0,NQ,body,0)
    dq_ref[...]=(dqt[...].T*0.125).astype(bf)
    dk_ref[...]=(dka[...]*0.125).astype(bf)
    dv_ref[...]=dva[...].astype(bf)
def attn_bwd(lengths,qkv,o,do,lse):
    blk=lambda off: pl.BlockSpec((ROW,128),lambda h:(0,off+h))
    return pl.pallas_call(bwd_kernel,grid=(6,),
        in_specs=[pl.BlockSpec(memory_space=pltpu.SMEM),blk(0),blk(6),blk(12),blk(0),blk(0),pl.BlockSpec((1,8,ROW),lambda h:(h,0,0))],
        out_specs=[blk(0),blk(0),blk(0)],
        out_shape=[jax.ShapeDtypeStruct((ROW,768),bf)]*3,
        scratch_shapes=[pltpu.VMEM((ROW,256),bf)]*4+[pltpu.VMEM((128,ROW),bf)]+[pltpu.VMEM((ROW,128),bf)]*4+[pltpu.VMEM((8,ROW),f32)]
          +[pltpu.VMEM((ROW,BQ),f32)]*4+[pltpu.VMEM((128,ROW),f32)]+[pltpu.VMEM((ROW,128),f32)]*2,
        compiler_params=pltpu.CompilerParams(vmem_limit_bytes=62<<20),name="attn_bwd")(lengths,qkv,qkv,qkv,o,do,lse)


def adam_update(weight, grad, first, second, rate, decay, fix_one, fix_two):
    first = BETA_ONE * first + (1.0 - BETA_ONE) * grad
    second = BETA_TWO * second + (1.0 - BETA_TWO) * grad * grad
    stride = first / fix_one / (jnp.sqrt(second / fix_two) + ADAM_EPS)
    return (weight - rate * (stride + decay * weight), first, second)


def local(
    tokens,
    cotangent,
    lengths,
    step,
    weight_qkv,
    weight_proj,
    weight_fc1,
    weight_fc2,
    vectors,
    first_qkv,
    second_qkv,
    first_proj,
    second_proj,
    first_fc1,
    second_fc1,
    first_fc2,
    second_fc2,
    first_vectors,
    second_vectors,
):
    rows_dev, row, _ = tokens.shape
    count = rows_dev * row
    low_shards = (
        weight_qkv.astype(jnp.bfloat16),
        weight_proj.astype(jnp.bfloat16),
        weight_fc1.astype(jnp.bfloat16),
        weight_fc2.astype(jnp.bfloat16),
        vectors.astype(jnp.bfloat16),
    )
    full = (
        lax.all_gather(low_shards[0], ("dp", "fsdp"), axis=0, tiled=True),
        lax.all_gather(low_shards[1], ("dp", "fsdp"), axis=0, tiled=True),
        lax.all_gather(low_shards[2], ("dp", "fsdp"), axis=0, tiled=True),
        lax.all_gather(low_shards[3], ("dp", "fsdp"), axis=0, tiled=True),
        lax.all_gather(low_shards[4], ("dp", "fsdp"), axis=0, tiled=True),
    )
    mat_qkv, mat_proj, mat_fc1, mat_fc2 = (full[0], full[1], full[2], full[3])
    (
        gain_one,
        shift_one,
        bias_q,
        bias_v,
        bias_o,
        scale_one,
        gain_two,
        shift_two,
        bias_up,
        bias_down,
        scale_two,
    ) = unpack(full[4].astype(jnp.float32))
    inputs = tokens.reshape(count, D).astype(jnp.float32)
    normed_f, norm_pull_one = jax.vjp(layer_norm, inputs, gain_one, shift_one)
    normed = normed_f.astype(jnp.bfloat16)
    bias = jnp.concatenate([bias_q, jnp.zeros_like(bias_q), bias_v])
    qkv = (jnp.dot(normed, mat_qkv, preferred_element_type=jnp.float32) + bias).astype(jnp.bfloat16)
    mixed, lse = attn_fwd(lengths, qkv)
    branch = jnp.dot(mixed, mat_proj, preferred_element_type=jnp.float32) + bias_o
    middle = inputs + scale_one * branch
    normed_two_f, norm_pull_two = jax.vjp(layer_norm, middle, gain_two, shift_two)
    normed_two = normed_two_f.astype(jnp.bfloat16)
    inner = jnp.dot(normed_two, mat_fc1, preferred_element_type=jnp.float32) + bias_up
    active_f, gelu_pull = jax.vjp(exact_gelu, inner)
    active = active_f.astype(jnp.bfloat16)
    out_branch = jnp.dot(active, mat_fc2, preferred_element_type=jnp.float32) + bias_down
    result = middle + scale_two * out_branch
    out_tokens = result.astype(jnp.bfloat16).reshape(rows_dev, row, D)
    again = (
        lax.all_gather(low_shards[0], ("dp", "fsdp"), axis=0, tiled=True),
        lax.all_gather(low_shards[1], ("dp", "fsdp"), axis=0, tiled=True),
        lax.all_gather(low_shards[2], ("dp", "fsdp"), axis=0, tiled=True),
        lax.all_gather(low_shards[3], ("dp", "fsdp"), axis=0, tiled=True),
        lax.all_gather(low_shards[4], ("dp", "fsdp"), axis=0, tiled=True),
    )
    back_qkv, back_proj, back_fc1, back_fc2 = (again[0], again[1], again[2], again[3])
    grad_out = cotangent.reshape(count, D).astype(jnp.float32)
    grad_scale_two = jnp.sum(grad_out * out_branch, axis=0)
    grad_down = (scale_two * grad_out).astype(jnp.bfloat16)
    grad_bias_down = jnp.sum(grad_down.astype(jnp.float32), axis=0)
    grad_fc2 = jnp.einsum("nf,nd->fd", active, grad_down, preferred_element_type=jnp.float32)
    grad_active = jnp.einsum("nd,fd->nf", grad_down, back_fc2, preferred_element_type=jnp.float32)
    grad_inner = gelu_pull(grad_active)[0].astype(jnp.bfloat16)
    grad_bias_up = jnp.sum(grad_inner.astype(jnp.float32), axis=0)
    grad_fc1 = jnp.einsum("nd,nf->df", normed_two, grad_inner, preferred_element_type=jnp.float32)
    grad_normed_two = jnp.einsum(
        "nf,df->nd", grad_inner, back_fc1, preferred_element_type=jnp.float32
    )
    grad_ln_two, grad_gain_two, grad_shift_two = norm_pull_two(grad_normed_two)
    grad_middle = grad_out + grad_ln_two
    grad_scale_one = jnp.sum(grad_middle * branch, axis=0)
    grad_branch = (scale_one * grad_middle).astype(jnp.bfloat16)
    grad_bias_o = jnp.sum(grad_branch.astype(jnp.float32), axis=0)
    grad_proj = jnp.einsum("nd,ne->de", mixed, grad_branch, preferred_element_type=jnp.float32)
    grad_mixed = jnp.einsum(
        "ne,de->nd", grad_branch, back_proj, preferred_element_type=jnp.float32
    ).astype(jnp.bfloat16)
    grad_qkv = jnp.concatenate(attn_bwd(lengths, qkv, mixed, grad_mixed, lse), axis=1)
    grad_qkv_sums = jnp.sum(grad_qkv.astype(jnp.float32), axis=0)
    grad_weight_qkv = jnp.einsum("nd,ne->de", normed, grad_qkv, preferred_element_type=jnp.float32)
    grad_normed = jnp.einsum("ne,de->nd", grad_qkv, back_qkv, preferred_element_type=jnp.float32)
    grad_ln_one, grad_gain_one, grad_shift_one = norm_pull_one(grad_normed)
    grad_inputs = grad_middle + grad_ln_one
    grad_tokens = grad_inputs.astype(jnp.bfloat16).reshape(rows_dev, row, D)
    grad_vectors = jnp.concatenate(
        [
            jnp.stack(
                [
                    grad_gain_one,
                    grad_shift_one,
                    grad_qkv_sums[:D],
                    grad_qkv_sums[2 * D :],
                    grad_bias_o,
                    grad_scale_one,
                    grad_gain_two,
                    grad_shift_two,
                ],
                axis=1,
            ),
            grad_bias_up.reshape(FF // D, D).T,
            jnp.stack([grad_bias_down, grad_scale_two], axis=1),
        ],
        axis=1,
    )
    owned = (
        lax.psum_scatter(grad_weight_qkv, ("dp", "fsdp"), scatter_dimension=0, tiled=True),
        lax.psum_scatter(grad_proj, ("dp", "fsdp"), scatter_dimension=0, tiled=True),
        lax.psum_scatter(grad_fc1, ("dp", "fsdp"), scatter_dimension=0, tiled=True),
        lax.psum_scatter(grad_fc2, ("dp", "fsdp"), scatter_dimension=0, tiled=True),
        lax.psum_scatter(grad_vectors, ("dp", "fsdp"), scatter_dimension=0, tiled=True),
    )
    local_squares = (
        jnp.sum(owned[0] * owned[0]) + jnp.sum(owned[1] * owned[1]) + jnp.sum(owned[2] * owned[2])
    )
    local_squares = local_squares + jnp.sum(owned[3] * owned[3]) + jnp.sum(owned[4] * owned[4])
    total_squares = lax.psum(local_squares, ("dp", "fsdp"))
    norm = jnp.sqrt(total_squares)
    factor = jnp.minimum(1.0, CLIP_LIMIT / (norm + 1e-06))
    steps_taken = step[0].astype(jnp.float32)
    fix_one = 1.0 - jnp.power(BETA_ONE, steps_taken)
    fix_two = 1.0 - jnp.power(BETA_TWO, steps_taken)
    rate_in = 2.0 / math.sqrt(D)
    new_qkv, new_first_qkv, new_second_qkv = adam_update(
        weight_qkv, factor * owned[0], first_qkv, second_qkv, rate_in, 0.04, fix_one, fix_two
    )
    new_proj, new_first_proj, new_second_proj = adam_update(
        weight_proj,
        factor * owned[1],
        first_proj,
        second_proj,
        2.0 / math.sqrt(D // 48),
        0.04,
        fix_one,
        fix_two,
    )
    new_fc1, new_first_fc1, new_second_fc1 = adam_update(
        weight_fc1, factor * owned[2], first_fc1, second_fc1, rate_in, 0.04, fix_one, fix_two
    )
    new_fc2, new_first_fc2, new_second_fc2 = adam_update(
        weight_fc2,
        factor * owned[3],
        first_fc2,
        second_fc2,
        2.0 / math.sqrt(FF),
        0.04,
        fix_one,
        fix_two,
    )
    new_vectors, new_first_vectors, new_second_vectors = adam_update(
        vectors, factor * owned[4], first_vectors, second_vectors, 1.0, 0.0, fix_one, fix_two
    )
    return (
        out_tokens,
        grad_tokens,
        norm.reshape(1),
        new_qkv,
        new_proj,
        new_fc1,
        new_fc2,
        new_vectors,
        new_first_qkv,
        new_second_qkv,
        new_first_proj,
        new_second_proj,
        new_first_fc1,
        new_second_fc1,
        new_first_fc2,
        new_second_fc2,
        new_first_vectors,
        new_second_vectors,
    )


def solution(mesh):
    return jax.shard_map(
        local,
        mesh=mesh,
        in_specs=(
            P(("dp", "fsdp"), None, None),
            P(("dp", "fsdp"), None, None),
            P(("dp", "fsdp"), None),
            P(),
            P(("dp", "fsdp"), None),
            P(("dp", "fsdp"), None),
            P(("dp", "fsdp"), None),
            P(("dp", "fsdp"), None),
            P(("dp", "fsdp"), None),
            P(("dp", "fsdp"), None),
            P(("dp", "fsdp"), None),
            P(("dp", "fsdp"), None),
            P(("dp", "fsdp"), None),
            P(("dp", "fsdp"), None),
            P(("dp", "fsdp"), None),
            P(("dp", "fsdp"), None),
            P(("dp", "fsdp"), None),
            P(("dp", "fsdp"), None),
            P(("dp", "fsdp"), None),
        ),
        out_specs=(
            P(("dp", "fsdp"), None, None),
            P(("dp", "fsdp"), None, None),
            P(),
            P(("dp", "fsdp"), None),
            P(("dp", "fsdp"), None),
            P(("dp", "fsdp"), None),
            P(("dp", "fsdp"), None),
            P(("dp", "fsdp"), None),
            P(("dp", "fsdp"), None),
            P(("dp", "fsdp"), None),
            P(("dp", "fsdp"), None),
            P(("dp", "fsdp"), None),
            P(("dp", "fsdp"), None),
            P(("dp", "fsdp"), None),
            P(("dp", "fsdp"), None),
            P(("dp", "fsdp"), None),
            P(("dp", "fsdp"), None),
            P(("dp", "fsdp"), None),
        ),
        check_vma=False,
    )
```

```python
import math

import jax
import jax.numpy as jnp
from jax import lax
from jax.experimental import pallas as pl
from jax.experimental.pallas import tpu as pltpu
from jax.sharding import PartitionSpec as P

D = 768
FF = 3072
NORM_EPS = 1e-06
BETA_ONE = 0.9
BETA_TWO = 0.999
ADAM_EPS = 1e-08
CLIP_LIMIT = 3.0
AXES = ("dp", "fsdp")
PACK = 32
bf = jnp.bfloat16
f32 = jnp.float32


def nt(a, b):
    return lax.dot_general(a, b, (((1,), (1,)), ((), ())), preferred_element_type=f32)


def nn(a, b):
    return jnp.dot(a, b, preferred_element_type=f32)


def tn(a, b):
    return lax.dot_general(a, b, (((0,), (0,)), ((), ())), preferred_element_type=f32)


ROW=1536; BQ=256; NQ=ROW//BQ; SEGS=6
LOG2E=1.4426950408889634
BIG=float(2**30)
def seg_onehot(len_ref, rows):
    pos=lax.broadcasted_iota(jnp.int32,(rows,128),0)
    lane=lax.broadcasted_iota(jnp.int32,(rows,128),1)
    idx=jnp.zeros((rows,128),jnp.int32)
    end=jnp.int32(0)
    for s in range(SEGS):
        end=end+len_ref[0,s]
        idx=idx+(pos>=end).astype(jnp.int32)
    return (idx==lane).astype(f32)
def prep(len_ref,q_ref,k_ref,qa,qb,ka,kb,first):
    lane=lax.broadcasted_iota(jnp.int32,(ROW,128),1); low=lane<64
    @pl.when(first)
    def _():
        oh=seg_onehot(len_ref,ROW)
        qa[:,128:256]=oh.astype(bf); qb[:,128:256]=oh.astype(bf)
        km=((oh-1.0)*BIG).astype(bf)
        ka[:,128:256]=km; kb[:,128:256]=km
    k=k_ref[...].astype(f32); kr=pltpu.roll(k,64,axis=1)
    ka[:,0:128]=jnp.where(low,k,kr).astype(bf); kb[:,0:128]=jnp.where(low,kr,k).astype(bf)
    q=q_ref[...].astype(f32)*(LOG2E*0.125); hi=q.astype(bf).astype(f32); lo=q-hi
    qa[:,0:128]=jnp.where(low,hi,pltpu.roll(lo,64,axis=1)).astype(bf)
    qb[:,0:128]=jnp.where(low,pltpu.roll(hi,64,axis=1),lo).astype(bf)
def fwd_kernel(len_ref,q_ref,k_ref,v_ref,o_ref,lse_ref,qa,qb,ka,kb,va,vb,sa,sb,ot):
    hp=pl.program_id(0)
    prep(len_ref,q_ref,k_ref,qa,qb,ka,kb,hp==0)
    vt=v_ref[...].T
    @pl.when(hp==0)
    def _():
        one=(lax.broadcasted_iota(jnp.int32,(16,ROW),0)==0).astype(bf)
        va[64:80,:]=one; vb[64:80,:]=one
    va[0:64,:]=vt[0:64,:]; vb[0:64,:]=vt[64:128,:]
    sa[...]=nt(ka[...],qa[0:BQ,:])
    def soft(s_ref,v_sc,j,r):
        s=s_ref[...]
        m=jnp.max(s,axis=0,keepdims=True)
        e=jnp.exp2(s-m).astype(bf)
        o=nn(v_sc[...],e)
        l=o[64:65,:]
        cols=pl.ds(pl.multiple_of(j*BQ,BQ),BQ)
        ot[64*r:64*r+64,cols]=o[0:64,:]*(1.0/l)
        lse_ref[0,r:r+1,cols]=m+jnp.log2(l)
    def body(j,c):
        rows=pl.ds(pl.multiple_of(j*BQ,BQ),BQ)
        nrow=pl.ds(pl.multiple_of(jnp.minimum(j+1,NQ-1)*BQ,BQ),BQ)
        sb[...]=nt(kb[...],qb[rows,:])
        soft(sa,va,j,0)
        sa[...]=nt(ka[...],qa[nrow,:])
        soft(sb,vb,j,1)
        return c
    lax.fori_loop(0,NQ,body,0)
    o_ref[...]=ot[...].T.astype(bf)
def attn_fwd(lengths,qkv):
    H=6
    return pl.pallas_call(fwd_kernel,grid=(H,),
        in_specs=[pl.BlockSpec(memory_space=pltpu.SMEM),
            pl.BlockSpec((ROW,128),lambda h:(0,h)),pl.BlockSpec((ROW,128),lambda h:(0,6+h)),pl.BlockSpec((ROW,128),lambda h:(0,12+h))],
        out_specs=[pl.BlockSpec((ROW,128),lambda h:(0,h)),pl.BlockSpec((1,8,ROW),lambda h:(h,0,0))],
        out_shape=[jax.ShapeDtypeStruct((ROW,768),bf),jax.ShapeDtypeStruct((6,8,ROW),f32)],
        scratch_shapes=[pltpu.VMEM((ROW,256),bf)]*4+[pltpu.VMEM((80,ROW),bf)]*2+[pltpu.VMEM((ROW,BQ),f32)]*2+[pltpu.VMEM((128,ROW),f32)],
        compiler_params=pltpu.CompilerParams(vmem_limit_bytes=60<<20),name="attn_fwd")(lengths,qkv,qkv,qkv)

def bwd_kernel(len_ref,q_ref,k_ref,v_ref,o_ref,do_ref,lse_ref,dq_ref,dk_ref,dv_ref,
               qa,qb,ka,kb,kt,da,db,qma,qmb,drow,xa,ya,xb,yb,dqt,dka,dva):
    hp=pl.program_id(0)
    prep(len_ref,q_ref,k_ref,qa,qb,ka,kb,hp==0)
    lane=lax.broadcasted_iota(jnp.int32,(ROW,128),1); low=lane<64
    kt[...]=k_ref[...].T
    do=do_ref[...]; z=jnp.zeros_like(do)
    da[...]=jnp.where(low,do,z); db[...]=jnp.where(low,z,do)
    q=q_ref[...]
    qma[...]=jnp.where(low,q,z); qmb[...]=jnp.where(low,z,q)
    pr=(do.astype(f32)*o_ref[...].astype(f32)).T
    drow[0:1,:]=jnp.sum(pr[0:64],axis=0,keepdims=True)
    drow[1:2,:]=jnp.sum(pr[64:128],axis=0,keepdims=True)
    dka[...]=jnp.zeros_like(dka); dva[...]=jnp.zeros_like(dva)
    def mm(k_sc,q_sc,d_sc,x,y,rows):
        x[...]=nt(k_sc[...],q_sc[rows,:])
        y[...]=nt(v_ref[...],d_sc[rows,:])
    def rest(x,y,d_sc,qm,r,rows):
        p=jnp.exp2(x[...]-lse_ref[0,r:r+1,rows])
        ds=(p*(y[...]-drow[r:r+1,rows])).astype(bf)
        dva[...]+=nn(p.astype(bf),d_sc[rows,:])
        dka[...]+=nn(ds,qm[rows,:])
        dqt[64*r:64*r+64,rows]=nn(kt[64*r:64*r+64,:],ds)
    mm(ka,qa,da,xa,ya,pl.ds(0,BQ))
    def body(j,c):
        rows=pl.ds(pl.multiple_of(j*BQ,BQ),BQ)
        nrow=pl.ds(pl.multiple_of(jnp.minimum(j+1,NQ-1)*BQ,BQ),BQ)
        mm(kb,qb,db,xb,yb,rows)
        rest(xa,ya,da,qma,0,rows)
        mm(ka,qa,da,xa,ya,nrow)
        rest(xb,yb,db,qmb,1,rows)
        return c
    lax.fori_loop(0,NQ,body,0)
    dq_ref[...]=(dqt[...].T*0.125).astype(bf)
    dk_ref[...]=(dka[...]*0.125).astype(bf)
    dv_ref[...]=dva[...].astype(bf)
def attn_bwd(lengths,qkv,o,do,lse):
    blk=lambda off: pl.BlockSpec((ROW,128),lambda h:(0,off+h))
    return pl.pallas_call(bwd_kernel,grid=(6,),
        in_specs=[pl.BlockSpec(memory_space=pltpu.SMEM),blk(0),blk(6),blk(12),blk(0),blk(0),pl.BlockSpec((1,8,ROW),lambda h:(h,0,0))],
        out_specs=[blk(0),blk(0),blk(0)],
        out_shape=[jax.ShapeDtypeStruct((ROW,768),bf)]*3,
        scratch_shapes=[pltpu.VMEM((ROW,256),bf)]*4+[pltpu.VMEM((128,ROW),bf)]+[pltpu.VMEM((ROW,128),bf)]*4+[pltpu.VMEM((8,ROW),f32)]
          +[pltpu.VMEM((ROW,BQ),f32)]*4+[pltpu.VMEM((128,ROW),f32)]+[pltpu.VMEM((ROW,128),f32)]*2,
        compiler_params=pltpu.CompilerParams(vmem_limit_bytes=62<<20),name="attn_bwd")(lengths,qkv,qkv,qkv,o,do,lse)


BM=512
INV_SQRT2=0.7071067811865476
INV_SQRT_2PI=0.3989422804014327
VMEM_CAP=62<<20


def norm_stats(v):
    center=v-jnp.mean(v,axis=1,keepdims=True)
    rstd=lax.rsqrt(jnp.mean(center*center,axis=1,keepdims=True)+NORM_EPS)
    return center*rstd,rstd


def params(**kw):
    return pltpu.CompilerParams(vmem_limit_bytes=VMEM_CAP,**kw)


def once(shape,index=None):
    return pl.BlockSpec(shape,index or (lambda i:(0,)*len(shape)),pipeline_mode=pl.Buffered(1))


def tile(width):
    return pl.BlockSpec((BM,width),lambda i:(i,0))


def qkv_kernel(x_ref,vec_ref,wq_ref,wk_ref,wv_ref,h_ref,qkv_ref):
    n,_=norm_stats(x_ref[...].astype(f32))
    h=(n*vec_ref[0:1,:]+vec_ref[1:2,:]).astype(bf)
    h_ref[...]=h
    qkv_ref[:,0:D]=(nn(h,wq_ref[...].reshape(D,D))+vec_ref[2:3,:]).astype(bf)
    qkv_ref[:,D:2*D]=nn(h,wk_ref[...].reshape(D,D)).astype(bf)
    qkv_ref[:,2*D:3*D]=(nn(h,wv_ref[...].reshape(D,D))+vec_ref[3:4,:]).astype(bf)


def qkv_forward(x,vec,w):
    rows=x.shape[0]
    n,r=w.shape[0],D//w.shape[0]
    blk=lambda b: pl.BlockSpec((n,r,D),lambda i:(0,b,0),pipeline_mode=pl.Buffered(1))
    return pl.pallas_call(qkv_kernel,grid=(rows//BM,),
        in_specs=[tile(D),once((16,D)),blk(0),blk(1),blk(2)],
        out_specs=[tile(D),tile(3*D)],
        out_shape=[jax.ShapeDtypeStruct((rows,D),bf),jax.ShapeDtypeStruct((rows,3*D),bf)],
        compiler_params=params(),name="qkv_forward",
        cost_estimate=pl.CostEstimate(flops=2*rows*D*3*D,bytes_accessed=14<<20,transcendentals=0))(x,vec,w,w,w)


CH=768


def mlp_kernel(x_ref,o_ref,dy_ref,vec_ref,w2_ref,wa_ref,wb_ref,wc_ref,wd_ref,wp_ref,
               out_ref,h_ref,dm_ref,z_ref,du_ref,dx_ref,da_ref,do_ref,sum_ref,
               a_s,x1_s,n2_s,mo_s,dh_s,ua,ub,ga,gb,w1_s):
    step=pl.program_id(0)
    @pl.when(step==0)
    def _():
        for b,ref in enumerate((wa_ref,wb_ref,wc_ref,wd_ref)):
            w1_s[b]=ref[...].reshape(D,D)
        sum_ref[...]=jnp.zeros_like(sum_ref)
    row=lambda i: vec_ref[i:i+1,:]
    def add(i,v):
        sum_ref[i:i+1,:]+=jnp.sum(v,axis=0,keepdims=True)
    wp=wp_ref[...].reshape(D,D)
    a=nn(o_ref[...],wp)+row(4)
    a_s[...]=a
    x1=x_ref[...].astype(f32)+row(5)*a
    x1_s[...]=x1
    n2,r2=norm_stats(x1)
    n2_s[...]=n2
    h=(n2*row(6)+row(7)).astype(bf)
    h_ref[...]=h
    dm=(row(13)*dy_ref[...].astype(f32)).astype(bf)
    dm_ref[...]=dm
    add(12,dm.astype(f32))
    mo_s[...]=jnp.zeros_like(mo_s)
    dh_s[...]=jnp.zeros_like(dh_s)
    def w2(c):
        return w2_ref[pl.ds(8*c,8)].reshape(D,D)
    def up(c,u,g):
        u[...]=nn(h_ref[...],w1_s[c])
        g[...]=nt(dm_ref[...],w2(c))
    def down(c,u,g):
        cols=pl.ds(pl.multiple_of(c*CH,CH),CH)
        v=u[...]+vec_ref[pl.ds(8+c,1),:]
        cdf=0.5+0.5*lax.erf(v*INV_SQRT2)
        z=(v*cdf).astype(bf)
        z_ref[:,cols]=z
        slope=cdf+v*(INV_SQRT_2PI*jnp.exp(v*v*(-0.5)))
        du=(g[...]*slope).astype(bf)
        du_ref[:,cols]=du
        sum_ref[pl.ds(8+c,1),:]+=jnp.sum(du.astype(f32),axis=0,keepdims=True)
        mo_s[...]+=nn(z,w2(c))
        dh_s[...]+=nt(du,w1_s[c])
    up(0,ua,ga)
    def body(i,carry):
        up(2*i+1,ub,gb)
        down(2*i,ua,ga)
        up(jnp.minimum(2*i+2,FF//CH-1),ua,ga)
        down(2*i+1,ub,gb)
        return carry
    lax.fori_loop(0,FF//CH//2,body,0)
    mo=mo_s[...]+row(12)
    out_ref[...]=(x1_s[...]+row(13)*mo).astype(bf)
    dy=dy_ref[...].astype(f32)
    add(13,dy*mo)
    dh=dh_s[...]; n2=n2_s[...]
    add(6,dh*n2); add(7,dh)
    t=dh*row(6)
    dx=dy+r2*(t-jnp.mean(t,axis=1,keepdims=True)-n2*jnp.mean(t*n2,axis=1,keepdims=True))
    dx_ref[...]=dx
    add(5,dx*a_s[...])
    da=(row(5)*dx).astype(bf)
    da_ref[...]=da
    add(4,da.astype(f32))
    do_ref[...]=nt(da,wp_ref[...].reshape(D,D)).astype(bf)


def mlp_block(x,o,dy,vec,packed):
    rows=x.shape[0]
    n,r=packed.shape[0],D//packed.shape[0]
    sd=jax.ShapeDtypeStruct
    return pl.pallas_call(mlp_kernel,grid=(rows//BM,),
        in_specs=[tile(D),tile(D),tile(D),once((16,D)),once((n,4*r,D))]+[once((n,r,D),lambda i,b=b:(0,b,0)) for b in range(4,9)],
        out_specs=[tile(D),tile(D),tile(D),tile(FF),tile(FF),tile(D),tile(D),tile(D),pl.BlockSpec((16,D),lambda i:(0,0))],
        out_shape=[sd((rows,D),bf),sd((rows,D),bf),sd((rows,D),bf),sd((rows,FF),bf),sd((rows,FF),bf),sd((rows,D),f32),sd((rows,D),bf),sd((rows,D),bf),sd((16,D),f32)],
        scratch_shapes=[pltpu.VMEM((BM,D),f32)]*5+[pltpu.VMEM((BM,CH),f32)]*4+[pltpu.VMEM((4,D,D),bf)],
        compiler_params=params(),name="mlp_block",
        cost_estimate=pl.CostEstimate(flops=2*rows*D*(2*D+4*FF),bytes_accessed=48<<20,transcendentals=0))(x,o,dy,vec,*[packed]*6)


def outer_kernel(a_ref,b_ref,g_ref):
    g_ref[...]=tn(a_ref[...],b_ref[...]).reshape(g_ref.shape).astype(bf)


def fc2_grad(z,dm,n,extra):
    rows=z.shape[0]
    per=FF//n
    return pl.pallas_call(outer_kernel,grid=(FF//D,),
        in_specs=[pl.BlockSpec((rows,D),lambda i:(0,i)),once((rows,D))],
        out_specs=pl.BlockSpec((n*D//FF,per,D),lambda i:(i,0,0)),
        out_shape=jax.ShapeDtypeStruct((n,per+extra,D),bf),
        compiler_params=params(),name="fc2_grad",
        cost_estimate=pl.CostEstimate(flops=2*rows*D*FF,bytes_accessed=16<<20,transcendentals=0))(z,dm)


def fc1_proj_kernel(h_ref,du_ref,o_ref,da_ref,old_ref,g_ref):
    i=pl.program_id(0)
    @pl.when(i<4)
    def _():
        g_ref[...]=tn(h_ref[...],du_ref[...]).reshape(g_ref.shape).astype(bf)
    @pl.when(i==4)
    def _():
        g_ref[...]=tn(o_ref[...],da_ref[...]).reshape(g_ref.shape).astype(bf)


def fc1_proj_grad(h,du,o,da,packed):
    rows=h.shape[0]
    n=packed.shape[0]; r=D//n
    base=packed.shape[1]//r-5
    return pl.pallas_call(fc1_proj_kernel,grid=(5,),
        in_specs=[once((rows,D)),pl.BlockSpec((rows,D),lambda i:(0,jnp.minimum(i,3))),once((rows,D)),once((rows,D)),pl.BlockSpec(memory_space=pl.ANY)],
        out_specs=pl.BlockSpec((n,r,D),lambda i:(0,base+i,0)),
        out_shape=jax.ShapeDtypeStruct(packed.shape,bf),input_output_aliases={4:0},
        compiler_params=params(),name="fc1_proj_grad",
        cost_estimate=pl.CostEstimate(flops=2*rows*D*(FF+D),bytes_accessed=24<<20,transcendentals=0))(h,du,o,da,packed)


def qkv_grad_kernel(h_ref,dq_ref,dk_ref,dv_ref,g_ref):
    i=pl.program_id(0)
    for b,ref in enumerate((dq_ref,dk_ref,dv_ref)):
        @pl.when(i==b)
        def _():
            g_ref[...]=tn(h_ref[...],ref[...]).reshape(g_ref.shape).astype(bf)


def qkv_grad(h,dq,dk,dv,n,extra):
    rows=h.shape[0]; r=D//n
    return pl.pallas_call(qkv_grad_kernel,grid=(3,),
        in_specs=[once((rows,D))]*4,
        out_specs=pl.BlockSpec((n,r,D),lambda i:(0,i,0)),
        out_shape=jax.ShapeDtypeStruct((n,3*r+extra,D),bf),
        compiler_params=params(),name="qkv_grad",
        cost_estimate=pl.CostEstimate(flops=2*rows*D*3*D,bytes_accessed=14<<20,transcendentals=0))(h,dq,dk,dv)


def input_kernel(x_ref,dq_ref,dk_ref,dv_ref,dx1_ref,vec_ref,old_ref,wq_ref,wk_ref,wv_ref,gx_ref,sum_ref):
    @pl.when(pl.program_id(0)==0)
    def _():
        sum_ref[...]=old_ref[...]
    def add(i,v):
        sum_ref[i:i+1,:]+=jnp.sum(v,axis=0,keepdims=True)
    dq=dq_ref[...]; dv=dv_ref[...]
    dh=nt(dq,wq_ref[...].reshape(D,D))+nt(dk_ref[...],wk_ref[...].reshape(D,D))+nt(dv,wv_ref[...].reshape(D,D))
    n,r=norm_stats(x_ref[...].astype(f32))
    add(0,dh*n); add(1,dh)
    add(2,dq.astype(f32)); add(3,dv.astype(f32))
    t=dh*vec_ref[0:1,:]
    dx=dx1_ref[...]+r*(t-jnp.mean(t,axis=1,keepdims=True)-n*jnp.mean(t*n,axis=1,keepdims=True))
    gx_ref[...]=dx.astype(bf)


def input_grad(x,dq,dk,dv,dx1,vec,sums,w):
    rows=x.shape[0]
    n,r=w.shape[0],D//w.shape[0]
    blk=lambda b: pl.BlockSpec((n,r,D),lambda i:(0,b,0),pipeline_mode=pl.Buffered(1))
    return pl.pallas_call(input_kernel,grid=(rows//BM,),
        in_specs=[tile(D)]*5+[once((16,D)),once((16,D)),blk(0),blk(1),blk(2)],
        out_specs=[tile(D),pl.BlockSpec((16,D),lambda i:(0,0))],
        out_shape=[jax.ShapeDtypeStruct((rows,D),bf),jax.ShapeDtypeStruct((16,D),f32)],
        compiler_params=params(),name="input_grad",
        cost_estimate=pl.CostEstimate(flops=2*rows*D*3*D,bytes_accessed=20<<20,transcendentals=0))(x,dq,dk,dv,dx1,vec,sums,w,w,w)


def adam_update(weight, grad, first, second, rate, decay, fix_one, fix_two):
    first = BETA_ONE * first + (1.0 - BETA_ONE) * grad
    second = BETA_TWO * second + (1.0 - BETA_TWO) * grad * grad
    stride = first / fix_one / (jnp.sqrt(second / fix_two) + ADAM_EPS)
    return (weight - rate * (stride + decay * weight), first, second)


def split_columns(shard):
    r, width = shard.shape
    return jnp.concatenate([shard[:, b * D : (b + 1) * D] for b in range(width // D)], axis=0)


def join_columns(block, r):
    return jnp.concatenate([block[b * r : (b + 1) * r] for b in range(block.shape[0] // r)], axis=1)


def pack_rows(full):
    k = full.shape[1] // D
    return full.reshape(PACK, D // PACK, k, D).transpose(0, 2, 1, 3).reshape(PACK, -1, D)


def unpack_rows(packed):
    k = packed.shape[1] * PACK // D
    return packed.reshape(PACK, k, D // PACK, D).transpose(0, 2, 1, 3).reshape(D, k * D)


def swap(value, axis, size, flip):
    return lax.ppermute(value, axis, [(i, i ^ flip) for i in range(size)])


def by_xor(parts, me):
    if len(parts) == 2:
        odd = me % 2 == 1
        return jnp.stack([jnp.where(odd, parts[1], parts[0]), jnp.where(odd, parts[0], parts[1])])
    low, high = (me % 2 == 1, me // 2 == 1)
    return jnp.stack(
        [
            jnp.where(high, jnp.where(low, parts[j ^ 3], parts[j ^ 2]), jnp.where(low, parts[j ^ 1], parts[j]))
            for j in range(4)
        ]
    )


def places():
    inner = lax.axis_index("fsdp")
    return (lax.axis_index("dp"), inner // 2, inner % 2)


def gather_direct(shard):
    me_dp, me_z, me_core = places()
    part = by_xor([shard] + [swap(shard, "fsdp", 8, 2 * k) for k in (1, 2, 3)], me_z)
    part = by_xor([part] + [swap(part, "dp", 4, k) for k in (1, 2, 3)], me_dp)
    part = by_xor([part, swap(part, "fsdp", 8, 1)], me_core)
    return part.transpose(1, 2, 0, 3, 4).reshape(PACK, *shard.shape)


def scatter_direct(packed, small):
    me_dp, me_z, me_core = places()
    packed = packed.reshape(4, 4, 2, -1, D)
    small = small.reshape(4, 4, 2, -1, D)

    def of_core(core):
        return jnp.concatenate(
            [lax.dynamic_index_in_dim(v, core, 2, keepdims=False) for v in (packed, small)], axis=2
        )

    mine, other = (of_core(me_core), of_core(1 - me_core))
    total = (mine.astype(f32) + swap(other, "fsdp", 8, 1).astype(f32)).astype(bf)
    pick = lambda v, i: lax.dynamic_index_in_dim(v, i, 0, keepdims=False)
    parts = [swap(pick(total, me_dp ^ k), "dp", 4, k) for k in (1, 2, 3)]
    total = (pick(total, me_dp).astype(f32) + sum(p.astype(f32) for p in parts)).astype(bf)
    parts = [swap(pick(total, me_z ^ k), "fsdp", 8, 2 * k) for k in (1, 2, 3)]
    return pick(total, me_z).astype(f32) + sum(p.astype(f32) for p in parts)


def make_local(fast):
    def gather(shard):
        return lax.all_gather(shard, AXES, axis=0, tiled=True)

    def scatter(full):
        return lax.psum_scatter(full, AXES, scatter_dimension=0, tiled=True)

    def local(
        tokens,
        cotangent,
        lengths,
        step,
        weight_qkv,
        weight_proj,
        weight_fc1,
        weight_fc2,
        vectors,
        first_qkv,
        second_qkv,
        first_proj,
        second_proj,
        first_fc1,
        second_fc1,
        first_fc2,
        second_fc2,
        first_vectors,
        second_vectors,
    ):
        per = weight_qkv.shape[0]
        cols = vectors.shape[1]
        low = [w.astype(bf) for w in (weight_qkv, weight_proj, weight_fc1, weight_fc2, vectors)]
        if fast:
            rest = lax.all_gather(
                jnp.concatenate([low[3], split_columns(low[2]), low[1]], axis=0), AXES, axis=0, tiled=False
            )
            line = jnp.pad(low[4].T.reshape(1, cols * per), ((0, 7), (0, D - cols * per)))
            mats_qkv = gather_direct(jnp.concatenate([split_columns(low[0]), line], axis=0))
            vec = mats_qkv[:, 3 * per, : cols * per].reshape(PACK, cols, per).transpose(1, 0, 2).reshape(cols, D)
        else:
            full = [gather(w) for w in low]
            rest = jnp.concatenate(
                [full[3].reshape(PACK, FF // PACK, D), pack_rows(full[2]), pack_rows(full[1])], axis=1
            )
            mats_qkv = pack_rows(full[0])
            vec = full[4].T
        vec = jnp.pad(vec.astype(f32), ((0, 16 - cols), (0, 0)))
        rows_dev, row, _ = tokens.shape
        count = rows_dev * row
        inputs = tokens.reshape(count, D)
        normed, qkv = qkv_forward(inputs, vec, mats_qkv)
        each = lambda v, b: v[b * row : (b + 1) * row]
        done = [attn_fwd(lengths[b : b + 1], each(qkv, b)) for b in range(rows_dev)]
        mixed = jnp.concatenate([o for o, _ in done], axis=0)
        result, normed_two, grad_down, active, grad_inner, grad_middle, grad_branch, grad_mixed, sums = mlp_block(
            inputs, mixed, cotangent.reshape(count, D), vec, rest
        )
        grads = fc2_grad(active, grad_down, PACK, 5 * D // PACK)
        grads = fc1_proj_grad(normed_two, grad_inner, mixed, grad_branch, grads)
        if fast:
            rest_owned = lax.psum_scatter(grads, AXES, scatter_dimension=0, tiled=False).astype(f32)
        back = [
            attn_bwd(lengths[b : b + 1], each(qkv, b), done[b][0], each(grad_mixed, b), done[b][1])
            for b in range(rows_dev)
        ]
        dq, dk, dv = (jnp.concatenate([v[i] for v in back], axis=0) for i in range(3))
        grad_inputs, sums = input_grad(inputs, dq, dk, dv, grad_middle, vec, sums, mats_qkv)
        grads_qkv = qkv_grad(normed, dq, dk, dv, PACK, 0)
        grads_vec = sums[:cols]
        if fast:
            line = grads_vec.reshape(cols, PACK, per).transpose(1, 0, 2).reshape(PACK, 1, cols * per)
            line = jnp.pad(line.astype(bf), ((0, 0), (0, 7), (0, D - cols * per)))
            first_owned = scatter_direct(grads_qkv, line)
            owned = (
                join_columns(first_owned[: 3 * per], per),
                rest_owned[8 * per :],
                join_columns(rest_owned[4 * per : 8 * per], per),
                rest_owned[: 4 * per],
                first_owned[3 * per, : cols * per].reshape(cols, per).T,
            )
        else:
            wide = FF // PACK
            owned = (
                scatter(unpack_rows(grads_qkv)),
                scatter(unpack_rows(grads[:, 2 * wide :])),
                scatter(unpack_rows(grads[:, wide : 2 * wide])),
                scatter(grads[:, :wide].reshape(FF, D)),
                scatter(grads_vec.T),
            )
            owned = tuple(g.astype(f32) for g in owned)
        squares = sum(jnp.sum(g * g) for g in owned)
        if fast:
            squares = jnp.sum(
                lax.all_to_all(jnp.full((PACK, 128), squares), AXES, 0, 0, tiled=True), axis=0
            )[0]
        else:
            squares = lax.psum(squares, AXES)
        norm = jnp.sqrt(squares)
        factor = jnp.minimum(1.0, CLIP_LIMIT / (norm + 1e-06))
        taken = step[0].astype(f32)
        fix_one = 1.0 - jnp.power(BETA_ONE, taken)
        fix_two = 1.0 - jnp.power(BETA_TWO, taken)
        rate_in = 2.0 / math.sqrt(D)
        states = (
            (weight_qkv, first_qkv, second_qkv, rate_in, 0.04),
            (weight_proj, first_proj, second_proj, 2.0 / math.sqrt(D // 48), 0.04),
            (weight_fc1, first_fc1, second_fc1, rate_in, 0.04),
            (weight_fc2, first_fc2, second_fc2, 2.0 / math.sqrt(FF), 0.04),
            (vectors, first_vectors, second_vectors, 1.0, 0.0),
        )
        new = [
            adam_update(w, factor * g, m, v, rate, decay, fix_one, fix_two)
            for g, (w, m, v, rate, decay) in zip(owned, states)
        ]
        shape = (rows_dev, row, D)
        outs = [result.reshape(shape), grad_inputs.reshape(shape), norm.reshape(1)]
        outs += [w for w, _, _ in new]
        for _, m, v in new:
            outs += [m, v]
        return tuple(outs)

    return local


def solution(mesh):
    rows = P(AXES, None)
    tokens = P(AXES, None, None)
    fast = (mesh.shape["dp"], mesh.shape["fsdp"]) == (4, 8)
    return jax.shard_map(
        make_local(fast),
        mesh=mesh,
        in_specs=(tokens, tokens, rows, P()) + (rows,) * 15,
        out_specs=(tokens, tokens, P()) + (rows,) * 15,
        check_vma=False,
    )
```

```python
import functools
import math

import jax
import jax.numpy as jnp
from jax import lax
from jax.experimental import pallas as pl
from jax.experimental.pallas import tpu as pltpu
from jax.sharding import PartitionSpec as P

D = 768
FF = 3072
NORM_EPS = 1e-06
BETA_ONE = 0.9
BETA_TWO = 0.999
ADAM_EPS = 1e-08
CLIP_LIMIT = 3.0
AXES = ("dp", "fsdp")
PACK = 32
bf = jnp.bfloat16
f32 = jnp.float32


def nt(a, b):
    return lax.dot_general(a, b, (((1,), (1,)), ((), ())), preferred_element_type=f32)


def nn(a, b):
    return jnp.dot(a, b, preferred_element_type=f32)


def tn(a, b):
    return lax.dot_general(a, b, (((0,), (0,)), ((), ())), preferred_element_type=f32)


ROW=1536
BQ=256
NQ=ROW//BQ
SEGS=6
LOG2E=1.4426950408889634
BIG=float(2**30)


def seg_onehot(len_ref):
    lane=lax.broadcasted_iota(jnp.int32,(1,128),1)
    start=jnp.zeros((1,128),jnp.int32); stop=jnp.zeros((1,128),jnp.int32)
    end=jnp.int32(0)
    for s in range(SEGS):
        start=jnp.where(lane==s,end,start)
        end=end+len_ref[0,s]
        stop=jnp.where(lane==s,end,stop)
    start=jnp.where(lane==SEGS,end,start)
    stop=jnp.where(lane==SEGS,ROW,stop)
    pos=lax.broadcasted_iota(jnp.int32,(ROW,128),0)
    return jnp.where((pos>=start)&(pos<stop),1.0,0.0)


def segments(len_ref,seg,mask):
    @pl.when(pl.program_id(0)==0)
    def _():
        oh=seg_onehot(len_ref)
        seg[...]=oh.astype(bf)
        mask[...]=((oh-1.0)*BIG).astype(bf)


def half(v,r):
    low=lax.broadcasted_iota(jnp.int32,v.shape,1)<64
    return jnp.where(low,v,jnp.zeros_like(v)) if r==0 else jnp.where(low,jnp.zeros_like(v),v)


MAIN=1376
CHUNKS=((0,256),(256,512),(512,768),(768,1024),(1024,MAIN))
LAST=slice(ROW-BQ,ROW)
TAIL=slice(MAIN,ROW)
EIGHTH=0.125


def tile_rows(j):
    return pl.ds(pl.multiple_of(j*BQ,BQ),BQ)


def fwd_kernel(len_ref,qkv_ref,o_ref,lse_ref,seg,mask,va,vb,sa,sb,ma,mb,ot,last):
    segments(len_ref,seg,mask)
    q_ref,k_ref,v_ref=(qkv_ref.at[:,128*b:128*b+128] for b in range(3))
    def query(rows,r):
        return jnp.concatenate([half(q_ref[rows,:]*jnp.asarray(EIGHTH,bf),r),seg[rows,:]],axis=1)
    def keys(rows):
        return jnp.concatenate([k_ref[rows,:],mask[rows,:]],axis=1)
    vt=v_ref[...].T
    one=(lax.broadcasted_iota(jnp.int32,(16,ROW),0)==0).astype(bf)
    va[64:80,:]=one; vb[64:80,:]=one
    va[0:64,:]=vt[0:64,:]; vb[0:64,:]=vt[64:128,:]
    for r,v_sc in enumerate((va,vb)):
        s=nt(keys(TAIL),query(LAST,r))*LOG2E
        m=jnp.max(s,axis=0,keepdims=True)
        o=nn(v_sc[:,TAIL],jnp.exp2(s-m).astype(bf))
        last[72*r:72*r+64,:]=o[0:64,:]*(1.0/o[64:65,:])
        last[72*r+64:72*r+65,:]=m+jnp.log2(o[64:65,:])
    def first(rows,r,s_sc,m_sc):
        q=query(rows,r)
        m=None
        for lo,hi in CHUNKS:
            s=nt(keys(slice(lo,hi)),q)
            s_sc[lo:hi,:]=s
            t=jnp.max(s,axis=0,keepdims=True)
            m=t if m is None else jnp.maximum(m,t)
        m_sc[0:1,:]=m*LOG2E
    def step(s_sc,m_sc,v_sc,j,r,rows,r2,s_next,m_next):
        q=query(rows,r2)
        m=m_sc[0:1,:]
        top=None
        o=0.0
        for lo,hi in CHUNKS:
            s=nt(keys(slice(lo,hi)),q)
            s_next[lo:hi,:]=s
            t=jnp.max(s,axis=0,keepdims=True)
            top=t if top is None else jnp.maximum(top,t)
        m_next[0:1,:]=top*LOG2E
        for lo,hi in CHUNKS:
            o=o+nn(v_sc[:,lo:hi],jnp.exp2(s_sc[lo:hi,:]*LOG2E-m).astype(bf))
        l=o[64:65,:]
        cols=tile_rows(j)
        ot[64*r:64*r+64,cols]=o[0:64,:]*(1.0/l)
        lse_ref[0,r:r+1,cols]=m+jnp.log2(l)
    first(pl.ds(0,BQ),0,sa,ma)
    def body(j,c):
        step(sa,ma,va,j,0,tile_rows(j),1,sb,mb)
        step(sb,mb,vb,j,1,tile_rows(jnp.minimum(j+1,NQ-1)),0,sa,ma)
        return c
    lax.fori_loop(0,NQ,body,0)
    for r in range(2):
        old=lse_ref[0,r:r+1,LAST]
        lse=last[72*r+64:72*r+65,:]
        top=jnp.maximum(old,lse)
        a=jnp.exp2(old-top); b=jnp.exp2(lse-top); t=1.0/(a+b)
        ot[64*r:64*r+64,LAST]=ot[64*r:64*r+64,LAST]*(a*t)+last[72*r:72*r+64,:]*(b*t)
        lse_ref[0,r:r+1,LAST]=top-jnp.log2(t)
    o_ref[...]=ot[...].T.astype(bf)


def attn_fwd(lengths,qkv):
    blk=lambda width: pl.BlockSpec((ROW,width),lambda h:(0,h))
    return pl.pallas_call(fwd_kernel,grid=(6,),
        in_specs=[pl.BlockSpec(memory_space=pltpu.SMEM),blk(384)],
        out_specs=[blk(128),pl.BlockSpec((1,8,ROW),lambda h:(h,0,0))],
        out_shape=[jax.ShapeDtypeStruct((ROW,768),bf),jax.ShapeDtypeStruct((6,8,ROW),f32)],
        scratch_shapes=[pltpu.VMEM((ROW,128),bf)]*2+[pltpu.VMEM((80,ROW),bf)]*2+[pltpu.VMEM((MAIN,BQ),f32)]*2+[pltpu.VMEM((8,BQ),f32)]*2
          +[pltpu.VMEM((128,ROW),f32),pltpu.VMEM((144,BQ),f32)],
        compiler_params=pltpu.CompilerParams(vmem_limit_bytes=60<<20),name="attn_fwd",
        cost_estimate=pl.CostEstimate(flops=4*ROW*ROW*D,bytes_accessed=10<<20,transcendentals=12*ROW*ROW))(lengths,qkv)


def bwd_kernel(len_ref,qkv_ref,o_ref,do_ref,lse_ref,d_ref,
               seg,mask,kt,xa,ya,xb,yb,dqt,dqe,dka,dva):
    segments(len_ref,seg,mask)
    q_ref,k_ref,v_ref=(qkv_ref.at[:,128*b:128*b+128] for b in range(3))
    kt[...]=k_ref[...].T
    def query(rows,r):
        return half(q_ref[rows,:]*jnp.asarray(EIGHTH,bf),r)
    def keys(rows):
        return jnp.concatenate([k_ref[rows,:],mask[rows,:]],axis=1)
    def rowsums(rows):
        t=(do_ref[rows,:].astype(f32)*o_ref[rows,:].astype(f32)).T
        return [jnp.sum(t[64*r:64*r+64],axis=0,keepdims=True) for r in range(2)]
    def products(rows,r,span,x,y):
        q=jnp.concatenate([query(rows,r),seg[rows,:]],axis=1); d=half(do_ref[rows,:],r)
        for lo,hi in span:
            x[lo:hi,:]=nt(keys(slice(lo,hi)),q)
            y[lo:hi,:]=nt(v_ref[lo:hi,:],d)
    def grads(x,y,lse,total):
        p=jnp.exp2(x*LOG2E-lse)
        return p.astype(bf),(p*(y-total)).astype(bf)
    sums=rowsums(LAST)
    dv=0.0; dk=0.0
    for r in range(2):
        q=query(LAST,r); d=half(do_ref[LAST,:],r)
        p,ds=grads(nt(keys(TAIL),jnp.concatenate([q,seg[LAST,:]],axis=1)),nt(v_ref[TAIL,:],d),lse_ref[0,r:r+1,LAST],sums[r])
        dv=dv+nn(p,d); dk=dk+nn(ds,q)
        dqe[64*r:64*r+64,:]=nn(kt[64*r:64*r+64,TAIL],ds)
    dva[TAIL,:]=dv; dka[TAIL,:]=dk
    dva[0:MAIN,:]=jnp.zeros((MAIN,128),f32); dka[0:MAIN,:]=jnp.zeros((MAIN,128),f32)
    def rest(x,y,r,rows,total):
        q=query(rows,r); d=half(do_ref[rows,:],r); lse=lse_ref[0,r:r+1,rows]
        dq=0.0
        for lo,hi in CHUNKS:
            p,ds=grads(x[lo:hi,:],y[lo:hi,:],lse,total)
            dva[lo:hi,:]+=nn(p,d)
            dka[lo:hi,:]+=nn(ds,q)
            dq=dq+nn(kt[64*r:64*r+64,lo:hi],ds)
        dqt[64*r:64*r+64,rows]=dq
    def body(j,c):
        rows=tile_rows(j)
        sums=rowsums(rows)
        products(rows,0,CHUNKS,xa,ya)
        products(rows,1,CHUNKS,xb,yb)
        rest(xa,ya,0,rows,sums[0])
        rest(xb,yb,1,rows,sums[1])
        return c
    lax.fori_loop(0,NQ,body,0)
    dqt[:,LAST]+=dqe[...]
    d_ref[:,0:128]=(dqt[...].T*EIGHTH).astype(bf)
    d_ref[:,128:256]=dka[...].astype(bf)
    d_ref[:,256:384]=dva[...].astype(bf)


def attn_bwd(lengths,qkv,o,do,lse):
    blk=lambda width: pl.BlockSpec((ROW,width),lambda h:(0,h))
    return pl.pallas_call(bwd_kernel,grid=(6,),
        in_specs=[pl.BlockSpec(memory_space=pltpu.SMEM),blk(384),blk(128),blk(128),pl.BlockSpec((1,8,ROW),lambda h:(h,0,0))],
        out_specs=blk(384),
        out_shape=jax.ShapeDtypeStruct((ROW,3*D),bf),
        scratch_shapes=[pltpu.VMEM((ROW,128),bf)]*2+[pltpu.VMEM((128,ROW),bf)]+[pltpu.VMEM((MAIN,BQ),f32)]*4
          +[pltpu.VMEM((128,ROW),f32),pltpu.VMEM((128,BQ),f32)]+[pltpu.VMEM((ROW,128),f32)]*2,
        compiler_params=pltpu.CompilerParams(vmem_limit_bytes=62<<20),name="attn_bwd",
        cost_estimate=pl.CostEstimate(flops=10*ROW*ROW*D,bytes_accessed=20<<20,transcendentals=12*ROW*ROW))(lengths,qkv,o,do,lse)


BM=512
INV_SQRT2=0.7071067811865476
INV_SQRT_2PI=0.3989422804014327
VMEM_CAP=62<<20


def norm_stats(v):
    center=v-jnp.mean(v,axis=1,keepdims=True)
    rstd=lax.rsqrt(jnp.mean(center*center,axis=1,keepdims=True)+NORM_EPS)
    return center*rstd,rstd


def params(**kw):
    return pltpu.CompilerParams(vmem_limit_bytes=VMEM_CAP,**kw)


def once(shape,index=None):
    return pl.BlockSpec(shape,index or (lambda i:(0,)*len(shape)),pipeline_mode=pl.Buffered(1))


def tile(width):
    return pl.BlockSpec((BM,width),lambda i:(i,0))


WIDE=3*D+128


def norm_kernel(x_ref,n_ref,r_ref):
    n,r=norm_stats(x_ref[...].astype(f32))
    n_ref[...]=n
    r_ref[...]=jnp.broadcast_to(r,r_ref.shape)


def norm_input(x):
    rows=x.shape[0]
    return pl.pallas_call(norm_kernel,grid=(rows//BM,),
        in_specs=[tile(D)],out_specs=[tile(D),tile(128)],
        out_shape=[jax.ShapeDtypeStruct((rows,D),f32),jax.ShapeDtypeStruct((rows,128),f32)],
        compiler_params=params(),name="norm_input",
        cost_estimate=pl.CostEstimate(flops=12*rows*D,bytes_accessed=8<<20,transcendentals=0))(x)


def qkv_kernel(n_ref,w_ref,v_ref,h_ref,qkv_ref,vec_ref):
    @pl.when(pl.program_id(0)==0)
    def _():
        vec_ref[...]=v_ref[...].reshape(D,128).astype(f32).T[0:16]
    h=(n_ref[...]*vec_ref[0:1,:]+vec_ref[1:2,:]).astype(bf)
    h_ref[...]=h
    zero=jnp.zeros((1,128),f32)
    bias=jnp.concatenate([b for p in range(6) for b in (vec_ref[2:3,128*p:128*p+128],zero,vec_ref[3:4,128*p:128*p+128])],axis=1)
    qkv_ref[...]=(nn(h,w_ref[...].reshape(D,3*D))+bias).astype(bf)


def packed_specs(w):
    n,r=w.shape[:2]
    return [once((n,r,3*D),lambda i:(0,0,0)),once((n,r,128),lambda i:(0,0,3*D//128))]


def qkv_forward(n,w):
    rows=n.shape[0]
    sd=jax.ShapeDtypeStruct
    return pl.pallas_call(qkv_kernel,grid=(rows//BM,),
        in_specs=[tile(D)]+packed_specs(w),
        out_specs=[tile(D),tile(3*D),pl.BlockSpec((16,D),lambda i:(0,0))],
        out_shape=[sd((rows,D),bf),sd((rows,3*D),bf),sd((16,D),f32)],
        compiler_params=params(),name="qkv_forward",
        cost_estimate=pl.CostEstimate(flops=2*rows*D*3*D,bytes_accessed=18<<20,transcendentals=0))(n,w,w)


CH=768


def mlp_kernel(x_ref,o_ref,dy_ref,vec_ref,w2_ref,wa_ref,wb_ref,wc_ref,wd_ref,wp_ref,
               out_ref,h_ref,dm_ref,z_ref,du_ref,dx_ref,da_ref,do_ref,sum_ref,
               a_s,x1_s,n2_s,mo_s,dh_s,ua,ub,ga,gb,w1_s):
    step=pl.program_id(0)
    @pl.when(step==0)
    def _():
        for b,ref in enumerate((wa_ref,wb_ref,wc_ref,wd_ref)):
            w1_s[b]=ref[...].reshape(D,D)
        sum_ref[...]=jnp.zeros_like(sum_ref)
    row=lambda i: vec_ref[i:i+1,:]
    def add(i,v):
        sum_ref[i:i+1,:]+=jnp.sum(v,axis=0,keepdims=True)
    wp=wp_ref[...].reshape(D,D)
    a=nn(o_ref[...],wp)+row(4)
    a_s[...]=a
    x1=x_ref[...].astype(f32)+row(5)*a
    x1_s[...]=x1
    n2,r2=norm_stats(x1)
    n2_s[...]=n2
    h=(n2*row(6)+row(7)).astype(bf)
    h_ref[...]=h
    dm=(row(13)*dy_ref[...].astype(f32)).astype(bf)
    dm_ref[...]=dm
    add(12,dm.astype(f32))
    mo_s[...]=jnp.zeros_like(mo_s)
    dh_s[...]=jnp.zeros_like(dh_s)
    def w2(c):
        return w2_ref[pl.ds(8*c,8)].reshape(D,D)
    def up(c,u,g):
        u[...]=nn(h_ref[...],w1_s[c])
        g[...]=nt(dm_ref[...],w2(c))
    def down(c,u,g):
        cols=pl.ds(pl.multiple_of(c*CH,CH),CH)
        v=u[...]+vec_ref[pl.ds(8+c,1),:]
        cdf=0.5+0.5*lax.erf(v*INV_SQRT2)
        z=(v*cdf).astype(bf)
        z_ref[:,cols]=z
        slope=cdf+v*(INV_SQRT_2PI*jnp.exp(v*v*(-0.5)))
        du=(g[...]*slope).astype(bf)
        du_ref[:,cols]=du
        sum_ref[pl.ds(8+c,1),:]+=jnp.sum(du.astype(f32),axis=0,keepdims=True)
        mo_s[...]+=nn(z,w2(c))
        dh_s[...]+=nt(du,w1_s[c])
    def body(i,carry):
        up(2*i,ua,ga)
        up(2*i+1,ub,gb)
        down(2*i,ua,ga)
        down(2*i+1,ub,gb)
        return carry
    lax.fori_loop(0,FF//CH//2,body,0)
    mo=mo_s[...]+row(12)
    out_ref[...]=(x1_s[...]+row(13)*mo).astype(bf)
    dy=dy_ref[...].astype(f32)
    add(13,dy*mo)
    dh=dh_s[...]; n2=n2_s[...]
    add(6,dh*n2); add(7,dh)
    t=dh*row(6)
    dx=dy+r2*(t-jnp.mean(t,axis=1,keepdims=True)-n2*jnp.mean(t*n2,axis=1,keepdims=True))
    dx_ref[...]=dx
    add(5,dx*a_s[...])
    da=(row(5)*dx).astype(bf)
    da_ref[...]=da
    add(4,da.astype(f32))
    do_ref[...]=nt(da,wp_ref[...].reshape(D,D)).astype(bf)


def mlp_block(x,o,dy,vec,packed):
    rows=x.shape[0]
    n,r=packed.shape[0],D//packed.shape[0]
    sd=jax.ShapeDtypeStruct
    return pl.pallas_call(mlp_kernel,grid=(rows//BM,),
        in_specs=[tile(D),tile(D),tile(D),once((16,D)),once((n,4*r,D))]+[once((n,r,D),lambda i,b=b:(0,b,0)) for b in range(4,9)],
        out_specs=[tile(D),tile(D),tile(D),tile(FF),tile(FF),tile(D),tile(D),tile(D),pl.BlockSpec((16,D),lambda i:(0,0))],
        out_shape=[sd((rows,D),bf),sd((rows,D),bf),sd((rows,D),bf),sd((rows,FF),bf),sd((rows,FF),bf),sd((rows,D),f32),sd((rows,D),bf),sd((rows,D),bf),sd((16,D),f32)],
        scratch_shapes=[pltpu.VMEM((BM,D),f32)]*5+[pltpu.VMEM((BM,CH),f32)]*4+[pltpu.VMEM((4,D,D),bf)],
        compiler_params=params(),name="mlp_block",
        cost_estimate=pl.CostEstimate(flops=2*rows*D*(2*D+4*FF),bytes_accessed=48<<20,transcendentals=0))(x,o,dy,vec,*[packed]*6)


def outer_kernel(a_ref,b_ref,g_ref):
    g_ref[...]=tn(a_ref[...],b_ref[...]).reshape(g_ref.shape).astype(bf)


def fc2_grad(z,dm,n,extra):
    rows=z.shape[0]
    per=FF//n
    return pl.pallas_call(outer_kernel,grid=(FF//D,),
        in_specs=[pl.BlockSpec((rows,D),lambda i:(0,i)),once((rows,D))],
        out_specs=pl.BlockSpec((n*D//FF,per,D),lambda i:(i,0,0)),
        out_shape=jax.ShapeDtypeStruct((n,per+extra,D),bf),
        compiler_params=params(),name="fc2_grad",
        cost_estimate=pl.CostEstimate(flops=2*rows*D*FF,bytes_accessed=16<<20,transcendentals=0))(z,dm)


def fc1_proj_kernel(h_ref,du_ref,o_ref,da_ref,old_ref,g_ref):
    i=pl.program_id(0)
    @pl.when(i<4)
    def _():
        g_ref[...]=tn(h_ref[...],du_ref[...]).reshape(g_ref.shape).astype(bf)
    @pl.when(i==4)
    def _():
        g_ref[...]=tn(o_ref[...],da_ref[...]).reshape(g_ref.shape).astype(bf)


def fc1_proj_grad(h,du,o,da,packed):
    rows=h.shape[0]
    n=packed.shape[0]; r=D//n
    base=packed.shape[1]//r-5
    return pl.pallas_call(fc1_proj_kernel,grid=(5,),
        in_specs=[once((rows,D)),pl.BlockSpec((rows,D),lambda i:(0,jnp.minimum(i,3))),once((rows,D)),once((rows,D)),pl.BlockSpec(memory_space=pl.ANY)],
        out_specs=pl.BlockSpec((n,r,D),lambda i:(0,base+i,0)),
        out_shape=jax.ShapeDtypeStruct(packed.shape,bf),input_output_aliases={4:0},
        compiler_params=params(),name="fc1_proj_grad",
        cost_estimate=pl.CostEstimate(flops=2*rows*D*(FF+D),bytes_accessed=24<<20,transcendentals=0))(h,du,o,da,packed)


def qkv_grad_kernel(core_ref,h_ref,d_ref,sum_ref,mine_ref,other_ref):
    i=pl.program_id(0)
    even=core_ref[0]==0
    def put(v,cols):
        v=v.reshape(mine_ref.shape[0],2,mine_ref.shape[1],v.shape[1])
        mine_ref[:,:,cols]=jnp.where(even,v[:,0],v[:,1]).astype(bf)
        other_ref[:,:,cols]=jnp.where(even,v[:,1],v[:,0]).astype(bf)
    @pl.when(i==0)
    def _():
        sums=jnp.concatenate([sum_ref[...],jnp.zeros((112,D),f32)],axis=0)
        put(sums.T,slice(3*D,WIDE))
    put(tn(h_ref[...],d_ref[...]),pl.ds(pl.multiple_of(i*D,D),D))


def qkv_grad(core,h,d,sums):
    rows=h.shape[0]
    half_shape=(PACK//2,D//PACK,WIDE)
    out=pl.BlockSpec(half_shape,lambda i:(0,0,0))
    return pl.pallas_call(qkv_grad_kernel,grid=(3,),
        in_specs=[pl.BlockSpec(memory_space=pltpu.SMEM),once((rows,D)),pl.BlockSpec((rows,D),lambda i:(0,i)),once((16,D))],
        out_specs=[out,out],
        out_shape=[jax.ShapeDtypeStruct(half_shape,bf)]*2,
        compiler_params=params(),name="qkv_grad",
        cost_estimate=pl.CostEstimate(flops=2*rows*D*3*D,bytes_accessed=14<<20,transcendentals=0))(core,h,d,sums)


def input_kernel(n_ref,r_ref,d_ref,dx1_ref,vec_ref,old_ref,w_ref,gx_ref,sum_ref):
    @pl.when(pl.program_id(0)==0)
    def _():
        sum_ref[...]=old_ref[...]
    def add(i,v):
        sum_ref[i:i+1,:]+=v
    d=d_ref[...]
    dh=nt(d,w_ref[...].reshape(D,3*D))
    total=jnp.sum(d.astype(f32),axis=0,keepdims=True)
    n=n_ref[...]; r=r_ref[:,0:1]
    add(0,jnp.sum(dh*n,axis=0,keepdims=True))
    add(1,jnp.sum(dh,axis=0,keepdims=True))
    for i,b in ((2,0),(3,2)):
        add(i,jnp.concatenate([total[:,384*p+128*b:384*p+128*b+128] for p in range(6)],axis=1))
    t=dh*vec_ref[0:1,:]
    dx=dx1_ref[...]+r*(t-jnp.mean(t,axis=1,keepdims=True)-n*jnp.mean(t*n,axis=1,keepdims=True))
    gx_ref[...]=dx.astype(bf)


def input_grad(n,r,d,dx1,vec,sums,w):
    rows=n.shape[0]
    return pl.pallas_call(input_kernel,grid=(rows//BM,),
        in_specs=[tile(D),tile(128),tile(3*D),tile(D),once((16,D)),once((16,D))]+packed_specs(w)[:1],
        out_specs=[tile(D),pl.BlockSpec((16,D),lambda i:(0,0))],
        out_shape=[jax.ShapeDtypeStruct((rows,D),bf),jax.ShapeDtypeStruct((16,D),f32)],
        compiler_params=params(),name="input_grad",
        cost_estimate=pl.CostEstimate(flops=2*rows*D*3*D,bytes_accessed=24<<20,transcendentals=0))(n,r,d,dx1,vec,sums,w)


def stage_kernel(count,place_ref,*refs):
    ins,outs=refs[:count],refs[count:]
    for k,out in enumerate(outs):
        at=place_ref[0]^k
        out[...]=sum(ref[at].astype(f32) for ref in ins).astype(bf)


def stage_sum(place,parts):
    shape=parts[0].shape
    whole=lambda s: pl.BlockSpec(s,lambda i:(0,)*len(s))
    return pl.pallas_call(functools.partial(stage_kernel,len(parts)),grid=(1,),
        in_specs=[pl.BlockSpec(memory_space=pltpu.SMEM)]+[whole(shape)]*len(parts),
        out_specs=[whole(shape[1:])]*4,
        out_shape=[jax.ShapeDtypeStruct(shape[1:],bf)]*4,
        compiler_params=params(),name="stage_sum")(place,*parts)


def finish_kernel(a_ref,b_ref,c_ref,d_ref,rest_ref,g_ref,square_ref):
    g=sum(ref[...].astype(f32) for ref in (a_ref,b_ref,c_ref,d_ref))
    g_ref[...]=g
    rest=rest_ref[...].astype(f32)
    total=jnp.sum(g*g,keepdims=True)+jnp.sum(rest*rest,keepdims=True)
    square_ref[...]=jnp.broadcast_to(total,square_ref.shape)


def finish_sum(parts,rest):
    whole=lambda s: pl.BlockSpec(s,lambda i:(0,)*len(s))
    shape=parts[0].shape
    return pl.pallas_call(finish_kernel,grid=(1,),
        in_specs=[whole(shape)]*4+[whole(rest.shape)],
        out_specs=[whole(shape),whole((PACK,128))],
        out_shape=[jax.ShapeDtypeStruct(shape,f32),jax.ShapeDtypeStruct((PACK,128),f32)],
        compiler_params=params(),name="finish_sum")(*parts,rest)


def adam_update(weight, grad, first, second, rate, decay, fix_one, fix_two):
    first = BETA_ONE * first + (1.0 - BETA_ONE) * grad
    second = BETA_TWO * second + (1.0 - BETA_TWO) * grad * grad
    stride = first / fix_one / (jnp.sqrt(second / fix_two) + ADAM_EPS)
    return (weight - rate * (stride + decay * weight), first, second)


def split_columns(shard):
    r, width = shard.shape
    return jnp.concatenate([shard[:, b * D : (b + 1) * D] for b in range(width // D)], axis=0)


def join_columns(block, r):
    return jnp.concatenate([block[b * r : (b + 1) * r] for b in range(block.shape[0] // r)], axis=1)


def pack_rows(full):
    k = full.shape[1] // D
    return full.reshape(PACK, D // PACK, k, D).transpose(0, 2, 1, 3).reshape(PACK, -1, D)


def unpack_rows(packed):
    k = packed.shape[1] * PACK // D
    return packed.reshape(PACK, k, D // PACK, D).transpose(0, 2, 1, 3).reshape(D, k * D)


def swap(value, axis, size, flip):
    return lax.ppermute(value, axis, [(i, i ^ flip) for i in range(size)])


def by_xor(parts, me):
    if len(parts) == 2:
        odd = me % 2 == 1
        return jnp.stack([jnp.where(odd, parts[1], parts[0]), jnp.where(odd, parts[0], parts[1])])
    low, high = (me % 2 == 1, me // 2 == 1)
    return jnp.stack(
        [
            jnp.where(high, jnp.where(low, parts[j ^ 3], parts[j ^ 2]), jnp.where(low, parts[j ^ 1], parts[j]))
            for j in range(4)
        ]
    )


def places():
    inner = lax.axis_index("fsdp")
    return (lax.axis_index("dp"), inner // 2, inner % 2)


def gather_direct(shard):
    me_dp, me_z, me_core = places()
    part = by_xor([shard] + [swap(shard, "fsdp", 8, 2 * k) for k in (1, 2, 3)], me_z)
    part = by_xor([part] + [swap(part, "dp", 4, k) for k in (1, 2, 3)], me_dp)
    part = by_xor([part, swap(part, "fsdp", 8, 1)], me_core)
    return part.transpose(1, 2, 0, 3, 4).reshape(PACK, *shard.shape)


def scatter_direct(mine, other):
    me_dp, me_z, _ = places()
    got = swap(other, "fsdp", 8, 1)
    shape = (4, 4) + mine.shape[1:]
    keep, *send = stage_sum(me_dp.reshape(1), [mine.reshape(shape), got.reshape(shape)])
    parts = [swap(v, "dp", 4, k + 1) for k, v in enumerate(send)]
    keep, *send = stage_sum(me_z.reshape(1), [keep] + parts)
    return [keep] + [swap(v, "fsdp", 8, 2 * k + 2) for k, v in enumerate(send)]


def to_pairs(w):
    return w.reshape(-1, 3, 6, 128).transpose(0, 2, 1, 3).reshape(-1, 3 * D)


def from_pairs(w):
    return w.reshape(-1, 6, 3, 128).transpose(0, 2, 1, 3).reshape(-1, 3 * D)


def make_local(fast):
    def gather(shard):
        return lax.all_gather(shard, AXES, axis=0, tiled=True)

    def scatter(full):
        return lax.psum_scatter(full, AXES, scatter_dimension=0, tiled=True)

    def local(
        tokens,
        cotangent,
        lengths,
        step,
        weight_qkv,
        weight_proj,
        weight_fc1,
        weight_fc2,
        vectors,
        first_qkv,
        second_qkv,
        first_proj,
        second_proj,
        first_fc1,
        second_fc1,
        first_fc2,
        second_fc2,
        first_vectors,
        second_vectors,
    ):
        per = weight_qkv.shape[0]
        cols = vectors.shape[1]
        low = [w.astype(bf) for w in (weight_qkv, weight_proj, weight_fc1, weight_fc2, vectors)]
        first = jnp.concatenate([to_pairs(low[0]), jnp.pad(low[4], ((0, 0), (0, 128 - cols)))], axis=1)
        if fast:
            mats_qkv = gather_direct(first)
            rest = lax.all_gather(
                jnp.concatenate([low[3], split_columns(low[2]), low[1]], axis=0), AXES, axis=0, tiled=False
            )
        else:
            mats_qkv = gather(first).reshape(PACK, D // PACK, WIDE)
            full = [gather(w) for w in low[1:4]]
            rest = jnp.concatenate(
                [full[2].reshape(PACK, FF // PACK, D), pack_rows(full[1]), pack_rows(full[0])], axis=1
            )
        rows_dev, row, _ = tokens.shape
        count = rows_dev * row
        inputs = tokens.reshape(count, D)
        centered, spread = norm_input(inputs)
        normed, qkv, vec = qkv_forward(centered, mats_qkv)
        each = lambda v, b: v[b * row : (b + 1) * row]
        done = [attn_fwd(lengths[b : b + 1], each(qkv, b)) for b in range(rows_dev)]
        mixed = jnp.concatenate([o for o, _ in done], axis=0)
        result, normed_two, grad_down, active, grad_inner, grad_middle, grad_branch, grad_mixed, sums = mlp_block(
            inputs, mixed, cotangent.reshape(count, D), vec, rest
        )
        grads = fc2_grad(active, grad_down, PACK, 5 * D // PACK)
        grads = fc1_proj_grad(normed_two, grad_inner, mixed, grad_branch, grads)
        if fast:
            rest_owned = lax.psum_scatter(grads, AXES, scatter_dimension=0, tiled=False)
        back = [
            attn_bwd(lengths[b : b + 1], each(qkv, b), done[b][0], each(grad_mixed, b), done[b][1])
            for b in range(rows_dev)
        ]
        grad_qkv = jnp.concatenate(back, axis=0)
        grad_inputs, sums = input_grad(centered, spread, grad_qkv, grad_middle, vec, sums, mats_qkv)
        core = places()[2].reshape(1) if fast else jnp.zeros((1,), jnp.int32)
        mine, other = qkv_grad(core, normed, grad_qkv, sums)
        if fast:
            first_owned, squares = finish_sum(scatter_direct(mine, other), rest_owned)
            rest_owned = rest_owned.astype(f32)
            owned = (
                from_pairs(first_owned[:, : 3 * D]),
                rest_owned[8 * per :],
                join_columns(rest_owned[4 * per : 8 * per], per),
                rest_owned[: 4 * per],
                first_owned[:, 3 * D : 3 * D + cols],
            )
            squares = jnp.sum(lax.all_to_all(squares, AXES, 0, 0, tiled=True), axis=0)[0]
        else:
            wide = FF // PACK
            grads_first = jnp.stack([mine, other], axis=1).reshape(D, WIDE)
            owned = (
                scatter(from_pairs(grads_first[:, : 3 * D])),
                scatter(unpack_rows(grads[:, 2 * wide :])),
                scatter(unpack_rows(grads[:, wide : 2 * wide])),
                scatter(grads[:, :wide].reshape(FF, D)),
                scatter(grads_first[:, 3 * D : 3 * D + cols]),
            )
            owned = tuple(g.astype(f32) for g in owned)
            squares = lax.psum(sum(jnp.sum(g * g) for g in owned), AXES)
        norm = jnp.sqrt(squares)
        factor = jnp.minimum(1.0, CLIP_LIMIT / (norm + 1e-06))
        taken = step[0].astype(f32)
        fix_one = 1.0 - jnp.power(BETA_ONE, taken)
        fix_two = 1.0 - jnp.power(BETA_TWO, taken)
        rate_in = 2.0 / math.sqrt(D)
        states = (
            (weight_qkv, first_qkv, second_qkv, rate_in, 0.04),
            (weight_proj, first_proj, second_proj, 2.0 / math.sqrt(D // 48), 0.04),
            (weight_fc1, first_fc1, second_fc1, rate_in, 0.04),
            (weight_fc2, first_fc2, second_fc2, 2.0 / math.sqrt(FF), 0.04),
            (vectors, first_vectors, second_vectors, 1.0, 0.0),
        )
        new = [
            adam_update(w, factor * g, m, v, rate, decay, fix_one, fix_two)
            for g, (w, m, v, rate, decay) in zip(owned, states)
        ]
        shape = (rows_dev, row, D)
        outs = [result.reshape(shape), grad_inputs.reshape(shape), norm.reshape(1)]
        outs += [w for w, _, _ in new]
        for _, m, v in new:
            outs += [m, v]
        return tuple(outs)

    return local


def solution(mesh):
    rows = P(AXES, None)
    tokens = P(AXES, None, None)
    fast = (mesh.shape["dp"], mesh.shape["fsdp"]) == (4, 8)
    return jax.shard_map(
        make_local(fast),
        mesh=mesh,
        in_specs=(tokens, tokens, rows, P()) + (rows,) * 15,
        out_specs=(tokens, tokens, P()) + (rows,) * 15,
        check_vma=False,
    )
```

```python
import functools
import math

import jax
import jax.numpy as jnp
from jax import lax
from jax.experimental import pallas as pl
from jax.experimental.pallas import tpu as pltpu
from jax.sharding import PartitionSpec as P

D = 768
FF = 3072
NORM_EPS = 1e-06
BETA_ONE = 0.9
BETA_TWO = 0.999
ADAM_EPS = 1e-08
CLIP_LIMIT = 3.0
AXES = ("dp", "fsdp")
PACK = 32
bf = jnp.bfloat16
f32 = jnp.float32


def nt(a, b):
    return lax.dot_general(a, b, (((1,), (1,)), ((), ())), preferred_element_type=f32)


def nn(a, b):
    return jnp.dot(a, b, preferred_element_type=f32)


def tn(a, b):
    return lax.dot_general(a, b, (((0,), (0,)), ((), ())), preferred_element_type=f32)


ROW=1536
BQ=256
NQ=ROW//BQ
SEGS=6
LOG2E=1.4426950408889634
BIG=float(2**30)


def seg_onehot(len_ref):
    lane=lax.broadcasted_iota(jnp.int32,(1,128),1)
    start=jnp.zeros((1,128),jnp.int32); stop=jnp.zeros((1,128),jnp.int32)
    end=jnp.int32(0)
    for s in range(SEGS):
        start=jnp.where(lane==s,end,start)
        end=end+len_ref[0,s]
        stop=jnp.where(lane==s,end,stop)
    start=jnp.where(lane==SEGS,end,start)
    stop=jnp.where(lane==SEGS,ROW,stop)
    pos=lax.broadcasted_iota(jnp.int32,(ROW,128),0)
    return jnp.where((pos>=start)&(pos<stop),1.0,0.0)


def segments(len_ref,seg,mask):
    @pl.when(pl.program_id(0)==0)
    def _():
        oh=seg_onehot(len_ref)
        seg[...]=oh.astype(bf)
        mask[...]=((oh-1.0)*BIG).astype(bf)


def half(v,r):
    low=lax.broadcasted_iota(jnp.int32,v.shape,1)<64
    return jnp.where(low,v,jnp.zeros_like(v)) if r==0 else jnp.where(low,jnp.zeros_like(v),v)


MAIN=1376
CHUNKS=((0,256),(256,512),(512,768),(768,1024),(1024,MAIN))
LAST=slice(ROW-BQ,ROW)
TAIL=slice(MAIN,ROW)
EIGHTH=0.125


def tile_rows(j):
    return pl.ds(pl.multiple_of(j*BQ,BQ),BQ)


def fwd_kernel(len_ref,qkv_ref,left_ref,o_ref,lse_ref,seg,mask,va,vb,sa,sb,ma,mb,ot,last):
    segments(len_ref,seg,mask)
    q_ref,k_ref,v_ref=(qkv_ref.at[:,128*b:128*b+128] for b in range(3))
    def query(rows,r):
        return jnp.concatenate([half(q_ref[rows,:]*jnp.asarray(EIGHTH,bf),r),seg[rows,:]],axis=1)
    def keys(rows):
        return jnp.concatenate([k_ref[rows,:],mask[rows,:]],axis=1)
    vt=v_ref[...].T
    one=(lax.broadcasted_iota(jnp.int32,(16,ROW),0)==0).astype(bf)
    va[64:80,:]=one; vb[64:80,:]=one
    va[0:64,:]=vt[0:64,:]; vb[0:64,:]=vt[64:128,:]
    for r,v_sc in enumerate((va,vb)):
        s=nt(keys(TAIL),query(LAST,r))*LOG2E
        m=jnp.max(s,axis=0,keepdims=True)
        o=nn(v_sc[:,TAIL],jnp.exp2(s-m).astype(bf))
        last[72*r:72*r+64,:]=o[0:64,:]*(1.0/o[64:65,:])
        last[72*r+64:72*r+65,:]=m+jnp.log2(o[64:65,:])
    def first(rows,r,s_sc,m_sc):
        q=query(rows,r)
        m=None
        for lo,hi in CHUNKS:
            s=nt(keys(slice(lo,hi)),q)
            s_sc[lo:hi,:]=s
            t=jnp.max(s,axis=0,keepdims=True)
            m=t if m is None else jnp.maximum(m,t)
        m_sc[0:1,:]=m*LOG2E
    def step(s_sc,m_sc,v_sc,j,r,rows,r2,s_next,m_next):
        q=query(rows,r2)
        m=m_sc[0:1,:]
        top=None
        o=0.0
        for lo,hi in CHUNKS:
            s=nt(keys(slice(lo,hi)),q)
            s_next[lo:hi,:]=s
            t=jnp.max(s,axis=0,keepdims=True)
            top=t if top is None else jnp.maximum(top,t)
        m_next[0:1,:]=top*LOG2E
        for lo,hi in CHUNKS:
            o=o+nn(v_sc[:,lo:hi],jnp.exp2(s_sc[lo:hi,:]*LOG2E-m).astype(bf))
        l=o[64:65,:]
        cols=tile_rows(j)
        ot[64*r:64*r+64,cols]=o[0:64,:]*(1.0/l)
        lse_ref[0,r:r+1,cols]=m+jnp.log2(l)
    first(pl.ds(0,BQ),0,sa,ma)
    def body(j,c):
        step(sa,ma,va,j,0,tile_rows(j),1,sb,mb)
        step(sb,mb,vb,j,1,tile_rows(jnp.minimum(j+1,NQ-1)),0,sa,ma)
        return c
    lax.fori_loop(0,NQ,body,0)
    for r in range(2):
        old=lse_ref[0,r:r+1,LAST]
        lse=last[72*r+64:72*r+65,:]
        top=jnp.maximum(old,lse)
        a=jnp.exp2(old-top); b=jnp.exp2(lse-top); t=1.0/(a+b)
        ot[64*r:64*r+64,LAST]=ot[64*r:64*r+64,LAST]*(a*t)+last[72*r:72*r+64,:]*(b*t)
        lse_ref[0,r:r+1,LAST]=top-jnp.log2(t)
    o_ref[...]=ot[...].T.astype(bf)


def attn_fwd(lengths,qkv,left):
    blk=lambda width: pl.BlockSpec((ROW,width),lambda h:(0,h))
    return pl.pallas_call(fwd_kernel,grid=(6,),
        in_specs=[pl.BlockSpec(memory_space=pltpu.SMEM),blk(384),pl.BlockSpec(memory_space=pl.ANY)],
        out_specs=[pl.BlockSpec((ROW,128),lambda h:(0,6+h)),pl.BlockSpec((1,8,ROW),lambda h:(h,0,0))],
        out_shape=[jax.ShapeDtypeStruct((ROW,2*D),bf),jax.ShapeDtypeStruct((6,8,ROW),f32)],input_output_aliases={2:0},
        scratch_shapes=[pltpu.VMEM((ROW,128),bf)]*2+[pltpu.VMEM((80,ROW),bf)]*2+[pltpu.VMEM((MAIN,BQ),f32)]*2+[pltpu.VMEM((8,BQ),f32)]*2
          +[pltpu.VMEM((128,ROW),f32),pltpu.VMEM((144,BQ),f32)],
        compiler_params=pltpu.CompilerParams(vmem_limit_bytes=60<<20),name="attn_fwd",
        cost_estimate=pl.CostEstimate(flops=4*ROW*ROW*D,bytes_accessed=10<<20,transcendentals=12*ROW*ROW))(lengths,qkv,left)


def bwd_kernel(len_ref,qkv_ref,o_ref,do_ref,lse_ref,right_ref,d_ref,
               seg,mask,kt,xa,ya,xb,yb,dqt,dqe,dka,dva):
    segments(len_ref,seg,mask)
    q_ref,k_ref,v_ref=(qkv_ref.at[:,128*b:128*b+128] for b in range(3))
    kt[...]=k_ref[...].T
    def query(rows,r):
        return half(q_ref[rows,:]*jnp.asarray(EIGHTH,bf),r)
    def keys(rows):
        return jnp.concatenate([k_ref[rows,:],mask[rows,:]],axis=1)
    def rowsums(rows):
        t=(do_ref[rows,:].astype(f32)*o_ref[rows,:].astype(f32)).T
        return [jnp.sum(t[64*r:64*r+64],axis=0,keepdims=True) for r in range(2)]
    def products(rows,r,span,x,y):
        q=jnp.concatenate([query(rows,r),seg[rows,:]],axis=1); d=half(do_ref[rows,:],r)
        for lo,hi in span:
            x[lo:hi,:]=nt(keys(slice(lo,hi)),q)
            y[lo:hi,:]=nt(v_ref[lo:hi,:],d)
    def grads(x,y,lse,total):
        p=jnp.exp2(x*LOG2E-lse)
        return p.astype(bf),(p*(y-total)).astype(bf)
    sums=rowsums(LAST)
    dv=0.0; dk=0.0
    for r in range(2):
        q=query(LAST,r); d=half(do_ref[LAST,:],r)
        p,ds=grads(nt(keys(TAIL),jnp.concatenate([q,seg[LAST,:]],axis=1)),nt(v_ref[TAIL,:],d),lse_ref[0,r:r+1,LAST],sums[r])
        dv=dv+nn(p,d); dk=dk+nn(ds,q)
        dqe[64*r:64*r+64,:]=nn(kt[64*r:64*r+64,TAIL],ds)
    dva[TAIL,:]=dv; dka[TAIL,:]=dk
    dva[0:MAIN,:]=jnp.zeros((MAIN,128),f32); dka[0:MAIN,:]=jnp.zeros((MAIN,128),f32)
    def rest(x,y,r,rows,total):
        q=query(rows,r); d=half(do_ref[rows,:],r); lse=lse_ref[0,r:r+1,rows]
        dq=0.0
        for lo,hi in CHUNKS:
            p,ds=grads(x[lo:hi,:],y[lo:hi,:],lse,total)
            dva[lo:hi,:]+=nn(p,d)
            dka[lo:hi,:]+=nn(ds,q)
            dq=dq+nn(kt[64*r:64*r+64,lo:hi],ds)
        dqt[64*r:64*r+64,rows]=dq
    def body(j,c):
        rows=tile_rows(j)
        sums=rowsums(rows)
        products(rows,0,CHUNKS,xa,ya)
        products(rows,1,CHUNKS,xb,yb)
        rest(xa,ya,0,rows,sums[0])
        rest(xb,yb,1,rows,sums[1])
        return c
    lax.fori_loop(0,NQ,body,0)
    dqt[:,LAST]+=dqe[...]
    d_ref[:,0:128]=(dqt[...].T*EIGHTH).astype(bf)
    d_ref[:,128:256]=dka[...].astype(bf)
    d_ref[:,256:384]=dva[...].astype(bf)


def attn_bwd(lengths,qkv,left,do,lse,right):
    blk=lambda width: pl.BlockSpec((ROW,width),lambda h:(0,h))
    return pl.pallas_call(bwd_kernel,grid=(6,),
        in_specs=[pl.BlockSpec(memory_space=pltpu.SMEM),blk(384),pl.BlockSpec((ROW,128),lambda h:(0,6+h)),blk(128),pl.BlockSpec((1,8,ROW),lambda h:(h,0,0)),pl.BlockSpec(memory_space=pl.ANY)],
        out_specs=blk(384),
        out_shape=jax.ShapeDtypeStruct((ROW,4*D),bf),input_output_aliases={5:0},
        scratch_shapes=[pltpu.VMEM((ROW,128),bf)]*2+[pltpu.VMEM((128,ROW),bf)]+[pltpu.VMEM((MAIN,BQ),f32)]*4
          +[pltpu.VMEM((128,ROW),f32),pltpu.VMEM((128,BQ),f32)]+[pltpu.VMEM((ROW,128),f32)]*2,
        compiler_params=pltpu.CompilerParams(vmem_limit_bytes=62<<20),name="attn_bwd",
        cost_estimate=pl.CostEstimate(flops=10*ROW*ROW*D,bytes_accessed=20<<20,transcendentals=12*ROW*ROW))(lengths,qkv,left,do,lse,right)


BM=512
INV_SQRT2=0.7071067811865476
INV_SQRT_2PI=0.3989422804014327
VMEM_CAP=62<<20


def norm_stats(v):
    center=v-jnp.mean(v,axis=1,keepdims=True)
    rstd=lax.rsqrt(jnp.mean(center*center,axis=1,keepdims=True)+NORM_EPS)
    return center*rstd,rstd


def params(**kw):
    return pltpu.CompilerParams(vmem_limit_bytes=VMEM_CAP,**kw)


def once(shape,index=None):
    return pl.BlockSpec(shape,index or (lambda i:(0,)*len(shape)),pipeline_mode=pl.Buffered(1))


def tile(width):
    return pl.BlockSpec((BM,width),lambda i:(i,0))


WIDE=3*D+128


def norm_kernel(x_ref,n_ref,r_ref):
    n,r=norm_stats(x_ref[...].astype(f32))
    n_ref[...]=n
    r_ref[...]=jnp.broadcast_to(r,r_ref.shape)


def norm_input(x):
    rows=x.shape[0]
    return pl.pallas_call(norm_kernel,grid=(rows//BM,),
        in_specs=[tile(D)],out_specs=[tile(D),tile(128)],
        out_shape=[jax.ShapeDtypeStruct((rows,D),f32),jax.ShapeDtypeStruct((rows,128),f32)],
        compiler_params=params(),name="norm_input",
        cost_estimate=pl.CostEstimate(flops=1000,bytes_accessed=1000,transcendentals=0))(x)


def pack_kernel(qkv_ref,proj_ref,fc1_ref,fc2_ref,vec_ref,first_ref,rest_ref):
    r=qkv_ref.shape[0]
    for p in range(6):
        for part in range(3):
            at=384*p+128*part
            first_ref[:,at:at+128]=qkv_ref[:,D*part+128*p:D*part+128*p+128].astype(bf)
    vec=vec_ref[...]
    vec=jnp.concatenate([vec,jnp.zeros((128-vec.shape[0],r),f32)],axis=0)
    first_ref[:,3*D:WIDE]=vec.T.astype(bf)
    rest_ref[0:4*r,:]=fc2_ref[...].astype(bf)
    for c in range(4):
        rest_ref[(4+c)*r:(5+c)*r,:]=fc1_ref[:,D*c:D*c+D].astype(bf)
    rest_ref[8*r:9*r,:]=proj_ref[...].astype(bf)


def pack_shards(qkv,proj,fc1,fc2,vectors):
    r=qkv.shape[0]
    ins=(qkv,proj,fc1,fc2,vectors.T)
    shapes=[(r,WIDE),(9*r,D)]
    whole=lambda s: pl.BlockSpec(s,lambda i:(0,)*len(s))
    return pl.pallas_call(pack_kernel,grid=(1,),
        in_specs=[whole(v.shape) for v in ins],out_specs=[whole(v) for v in shapes],
        out_shape=[jax.ShapeDtypeStruct(v,bf) for v in shapes],
        compiler_params=params(),name="pack_shards")(*ins)


def qkv_kernel(place_ref,n_ref,*refs):
    parts,(left_ref,qkv_ref,vec_ref,w_ref,w,sems,out_sem)=refs[:8],refs[8:]
    step=pl.program_id(0)
    keep=pltpu.make_async_copy(w,w_ref,out_sem)
    @pl.when(step==0)
    def _():
        copies=[]
        for i,part in enumerate(parts):
            core,dp=place_ref[2]^(i//4),place_ref[0]^(i%4)
            for k in range(4):
                copies.append(pltpu.make_async_copy(part.at[k],w.at[dp,place_ref[1]^k,core],sems.at[4*i+k]))
        for copy in copies:
            copy.start()
        for copy in copies:
            copy.wait()
        keep.start()
        vec_ref[...]=w[:,:,:,:,3*D:WIDE].reshape(D,128).astype(f32).T[0:16]
    h=(n_ref[...]*vec_ref[0:1,:]+vec_ref[1:2,:]).astype(bf)
    left_ref[...]=h
    zero=jnp.zeros((1,128),f32)
    bias=jnp.concatenate([b for p in range(6) for b in (vec_ref[2:3,128*p:128*p+128],zero,vec_ref[3:4,128*p:128*p+128])],axis=1)
    qkv_ref[...]=(nn(h,w[:,:,:,:,0:3*D].reshape(D,3*D))+bias).astype(bf)
    @pl.when(step==pl.num_programs(0)-1)
    def _():
        keep.wait()


def qkv_forward(place,n,parts):
    rows=n.shape[0]
    sd=jax.ShapeDtypeStruct
    wide=(4,4,2,D//PACK,WIDE)
    return pl.pallas_call(qkv_kernel,grid=(rows//BM,),
        in_specs=[pl.BlockSpec(memory_space=pltpu.SMEM),tile(D)]+[pl.BlockSpec(memory_space=pl.ANY)]*8,
        out_specs=[tile(D),tile(3*D),pl.BlockSpec((16,D),lambda i:(0,0)),pl.BlockSpec(memory_space=pl.ANY)],
        out_shape=[sd((rows,2*D),bf),sd((rows,3*D),bf),sd((16,D),f32),sd(wide,bf)],
        scratch_shapes=[pltpu.VMEM(wide,bf),pltpu.SemaphoreType.DMA((32,)),pltpu.SemaphoreType.DMA],
        compiler_params=params(),name="qkv_forward",
        cost_estimate=pl.CostEstimate(flops=2*rows*D*3*D,bytes_accessed=18<<20,transcendentals=0))(place,n,*parts)


CH=768


def mlp_kernel(x_ref,o_ref,dy_ref,vec_ref,w2_ref,wa_ref,wb_ref,wc_ref,wd_ref,wp_ref,
               out_ref,h_ref,dm_ref,z_ref,du_ref,dx_ref,da_ref,do_ref,sum_ref,
               a_s,x1_s,n2_s,mo_s,dh_s,ua,ub,ga,gb,w1_s):
    step=pl.program_id(0)
    @pl.when(step==0)
    def _():
        for b,ref in enumerate((wa_ref,wb_ref,wc_ref,wd_ref)):
            w1_s[b]=ref[...].reshape(D,D)
        sum_ref[...]=jnp.zeros_like(sum_ref)
    row=lambda i: vec_ref[i:i+1,:]
    def add(i,v):
        sum_ref[i:i+1,:]+=jnp.sum(v,axis=0,keepdims=True)
    wp=wp_ref[...].reshape(D,D)
    a=nn(o_ref[...],wp)+row(4)
    a_s[...]=a
    x1=x_ref[...].astype(f32)+row(5)*a
    x1_s[...]=x1
    n2,r2=norm_stats(x1)
    n2_s[...]=n2
    h=(n2*row(6)+row(7)).astype(bf)
    h_ref[...]=h
    dm=(row(13)*dy_ref[...].astype(f32)).astype(bf)
    dm_ref[...]=dm
    add(12,dm.astype(f32))
    mo_s[...]=jnp.zeros_like(mo_s)
    dh_s[...]=jnp.zeros_like(dh_s)
    def w2(c):
        return w2_ref[pl.ds(8*c,8)].reshape(D,D)
    def up(c,u,g):
        u[...]=nn(h_ref[...],w1_s[c])
        g[...]=nt(dm_ref[...],w2(c))
    def down(c,u,g):
        cols=pl.ds(pl.multiple_of(c*CH,CH),CH)
        v=u[...]+vec_ref[pl.ds(8+c,1),:]
        cdf=0.5+0.5*lax.erf(v*INV_SQRT2)
        z=(v*cdf).astype(bf)
        z_ref[:,cols]=z
        slope=cdf+v*(INV_SQRT_2PI*jnp.exp(v*v*(-0.5)))
        du=(g[...]*slope).astype(bf)
        du_ref[:,cols]=du
        sum_ref[pl.ds(8+c,1),:]+=jnp.sum(du.astype(f32),axis=0,keepdims=True)
        mo_s[...]+=nn(z,w2(c))
        dh_s[...]+=nt(du,w1_s[c])
    def body(i,carry):
        up(2*i,ua,ga)
        up(2*i+1,ub,gb)
        down(2*i,ua,ga)
        down(2*i+1,ub,gb)
        return carry
    lax.fori_loop(0,FF//CH//2,body,0)
    mo=mo_s[...]+row(12)
    out_ref[...]=(x1_s[...]+row(13)*mo).astype(bf)
    dy=dy_ref[...].astype(f32)
    add(13,dy*mo)
    dh=dh_s[...]; n2=n2_s[...]
    add(6,dh*n2); add(7,dh)
    t=dh*row(6)
    dx=dy+r2*(t-jnp.mean(t,axis=1,keepdims=True)-n2*jnp.mean(t*n2,axis=1,keepdims=True))
    dx_ref[...]=dx
    add(5,dx*a_s[...])
    da=(row(5)*dx).astype(bf)
    da_ref[...]=da
    add(4,da.astype(f32))
    do_ref[...]=nt(da,wp_ref[...].reshape(D,D)).astype(bf)


def mlp_block(x,o,dy,vec,packed):
    rows=x.shape[0]
    n,r=packed.shape[0],D//packed.shape[0]
    sd=jax.ShapeDtypeStruct
    return pl.pallas_call(mlp_kernel,grid=(rows//BM,),
        in_specs=[tile(D),pl.BlockSpec((BM,D),lambda i:(i,1)),tile(D),once((16,D)),once((n,4*r,D))]+[once((n,r,D),lambda i,b=b:(0,b,0)) for b in range(4,9)],
        out_specs=[tile(D),tile(D),tile(D),tile(FF),tile(FF),tile(D),pl.BlockSpec((BM,D),lambda i:(i,3)),tile(D),pl.BlockSpec((16,D),lambda i:(0,0))],
        out_shape=[sd((rows,D),bf),sd((rows,D),bf),sd((rows,D),bf),sd((rows,FF),bf),sd((rows,FF),bf),sd((rows,D),f32),sd((rows,4*D),bf),sd((rows,D),bf),sd((16,D),f32)],
        scratch_shapes=[pltpu.VMEM((BM,D),f32)]*5+[pltpu.VMEM((BM,CH),f32)]*4+[pltpu.VMEM((4,D,D),bf)],
        compiler_params=params(),name="mlp_block",
        cost_estimate=pl.CostEstimate(flops=2*rows*D*(2*D+4*FF),bytes_accessed=48<<20,transcendentals=0))(x,o,dy,vec,*[packed]*6)


def outer_kernel(a_ref,b_ref,g_ref):
    g_ref[...]=tn(a_ref[...],b_ref[...]).reshape(g_ref.shape).astype(bf)


def fc2_grad(z,dm,n,extra):
    rows=z.shape[0]
    per=FF//n
    return pl.pallas_call(outer_kernel,grid=(FF//D,),
        in_specs=[pl.BlockSpec((rows,D),lambda i:(0,i)),once((rows,D))],
        out_specs=pl.BlockSpec((n*D//FF,per,D),lambda i:(i,0,0)),
        out_shape=jax.ShapeDtypeStruct((n,per+extra,D),bf),
        compiler_params=params(),name="fc2_grad",
        cost_estimate=pl.CostEstimate(flops=2*rows*D*FF,bytes_accessed=16<<20,transcendentals=0))(z,dm)


def fc1_kernel(a_ref,b_ref,old_ref,g_ref):
    outer_kernel(a_ref,b_ref,g_ref)


def fc1_grad(h,du,packed):
    rows=h.shape[0]
    n=packed.shape[0]; r=D//n
    return pl.pallas_call(fc1_kernel,grid=(FF//D,),
        in_specs=[once((rows,D)),pl.BlockSpec((rows,D),lambda i:(0,i)),pl.BlockSpec(memory_space=pl.ANY)],
        out_specs=pl.BlockSpec((n,r,D),lambda i:(0,FF//D+i,0)),
        out_shape=jax.ShapeDtypeStruct(packed.shape,bf),input_output_aliases={2:0},
        compiler_params=params(),name="fc1_grad",
        cost_estimate=pl.CostEstimate(flops=2*rows*D*FF,bytes_accessed=20<<20,transcendentals=0))(h,du,packed)


def split_kernel(core_ref,left_ref,right_ref,*refs):
    sum_ref,(mine_ref,other_ref)=refs[:-2],refs[-2:]
    i=pl.program_id(0)
    even=core_ref[0]==0
    def put(v,cols):
        v=v.reshape(mine_ref.shape[0],2,mine_ref.shape[1],v.shape[1])
        mine_ref[:,:,cols]=jnp.where(even,v[:,0],v[:,1]).astype(bf)
        other_ref[:,:,cols]=jnp.where(even,v[:,1],v[:,0]).astype(bf)
    if sum_ref:
        @pl.when(i==0)
        def _():
            sums=jnp.concatenate([sum_ref[0][...],jnp.zeros((112,D),f32)],axis=0)
            put(sums.T,slice(2*D,2*D+128))
    put(tn(left_ref[...],right_ref[...]),pl.ds(pl.multiple_of(i*D,D),D))


def split_grad(core,left,right,sums=None):
    rows=left.shape[0]
    more=[] if sums is None else [sums]
    index=(lambda i:(0,1-i),lambda i:(0,3-3*i)) if sums is None else (lambda i:(0,0),lambda i:(0,1+i))
    shape=(PACK//2,D//PACK,2*D+128*len(more))
    out=pl.BlockSpec(memory_space=pltpu.VMEM)
    return pl.pallas_call(split_kernel,grid=(2,),
        in_specs=[pl.BlockSpec(memory_space=pltpu.SMEM)]+[pl.BlockSpec((rows,D),f) for f in index]+[once((16,D))]*len(more),
        out_specs=[out,out],
        out_shape=[jax.ShapeDtypeStruct(shape,bf)]*2,
        compiler_params=pltpu.CompilerParams(vmem_limit_bytes=48<<20),name="split_grad",
        cost_estimate=pl.CostEstimate(flops=1000,bytes_accessed=1000,transcendentals=0))(core,left,right,*more)


def input_kernel(n_ref,r_ref,d_ref,dx1_ref,vec_ref,old_ref,w_ref,gx_ref,sum_ref):
    @pl.when(pl.program_id(0)==0)
    def _():
        sum_ref[...]=old_ref[...]
    def add(i,v):
        sum_ref[i:i+1,:]+=v
    d=d_ref[...]
    dh=nt(d,w_ref[...].reshape(D,3*D))
    total=jnp.sum(d.astype(f32),axis=0,keepdims=True)
    n=n_ref[...]; r=r_ref[:,0:1]
    add(0,jnp.sum(dh*n,axis=0,keepdims=True))
    add(1,jnp.sum(dh,axis=0,keepdims=True))
    for i,b in ((2,0),(3,2)):
        add(i,jnp.concatenate([total[:,384*p+128*b:384*p+128*b+128] for p in range(6)],axis=1))
    t=dh*vec_ref[0:1,:]
    dx=dx1_ref[...]+r*(t-jnp.mean(t,axis=1,keepdims=True)-n*jnp.mean(t*n,axis=1,keepdims=True))
    gx_ref[...]=dx.astype(bf)


def input_grad(n,r,d,dx1,vec,sums,w):
    rows=n.shape[0]
    return pl.pallas_call(input_kernel,grid=(rows//BM,),
        in_specs=[tile(D),tile(128),tile(3*D),tile(D),once((16,D)),once((16,D)),once(w.shape[:-1]+(3*D,),lambda i:(0,)*len(w.shape))],
        out_specs=[tile(D),pl.BlockSpec((16,D),lambda i:(0,0))],
        out_shape=[jax.ShapeDtypeStruct((rows,D),bf),jax.ShapeDtypeStruct((16,D),f32)],
        compiler_params=params(),name="input_grad",
        cost_estimate=pl.CostEstimate(flops=1000,bytes_accessed=1000,transcendentals=0))(n,r,d,dx1,vec,sums,w)


def stage_kernel(count,place_ref,*refs):
    ins,outs=refs[:count],refs[count:]
    for k,out in enumerate(outs):
        at=place_ref[0]^k
        out[...]=sum(ref[at].astype(f32) for ref in ins).astype(bf)


def stage_sum(place,parts):
    shape=parts[0].shape
    near=pl.BlockSpec(memory_space=pltpu.VMEM)
    return pl.pallas_call(functools.partial(stage_kernel,len(parts)),
        in_specs=[pl.BlockSpec(memory_space=pltpu.SMEM)]+[near]*len(parts),
        out_specs=[near]*4,
        out_shape=[jax.ShapeDtypeStruct(shape[1:],bf)]*4,
        compiler_params=pltpu.CompilerParams(vmem_limit_bytes=16<<20),name="stage_sum",
        cost_estimate=pl.CostEstimate(flops=1000,bytes_accessed=1000,transcendentals=0))(place,*parts)


def finish_kernel(*refs):
    first,second,(rest_ref,qkv_ref,proj_ref,fc1_ref,fc2_ref,vec_ref,square_ref)=refs[:4],refs[4:8],refs[8:]
    a=sum(ref[...].astype(f32) for ref in first)
    b=sum(ref[...].astype(f32) for ref in second)
    rest=rest_ref[...].astype(f32)
    total=jnp.sum(a*a,keepdims=True)+jnp.sum(b*b,keepdims=True)+jnp.sum(rest*rest,keepdims=True)
    square_ref[...]=jnp.broadcast_to(total,square_ref.shape)
    r=a.shape[0]
    proj_ref[...]=a[:,0:D]
    for p in range(6):
        for part in range(3):
            at=384*p+128*part
            qkv_ref[:,D*part+128*p:D*part+128*p+128]=a[:,D+at:D+at+128] if p<2 else b[:,at-D:at-D+128]
    vec_ref[...]=b[:,2*D:2*D+128].T
    fc2_ref[...]=rest[0:4*r]
    for c in range(4):
        fc1_ref[:,D*c:D*c+D]=rest[(4+c)*r:(5+c)*r]


def finish_sum(first,second,rest):
    near=pl.BlockSpec(memory_space=pltpu.VMEM)
    r=rest.shape[0]//8
    shapes=[(r,3*D),(r,D),(r,FF),(4*r,D),(128,r),(PACK,128)]
    return pl.pallas_call(finish_kernel,
        in_specs=[near]*9,
        out_specs=[near]*6,
        out_shape=[jax.ShapeDtypeStruct(v,f32) for v in shapes],
        compiler_params=pltpu.CompilerParams(vmem_limit_bytes=24<<20),name="finish_sum",
        cost_estimate=pl.CostEstimate(flops=1000,bytes_accessed=1000,transcendentals=0))(*first,*second,rest)


def adam_update(weight, grad, first, second, rate, decay, fix_one, fix_two):
    first = BETA_ONE * first + (1.0 - BETA_ONE) * grad
    second = BETA_TWO * second + (1.0 - BETA_TWO) * grad * grad
    stride = first / fix_one / (jnp.sqrt(second / fix_two) + ADAM_EPS)
    return (weight - rate * (stride + decay * weight), first, second)


def pack_rows(full):
    k = full.shape[1] // D
    return full.reshape(PACK, D // PACK, k, D).transpose(0, 2, 1, 3).reshape(PACK, -1, D)


def unpack_rows(packed):
    k = packed.shape[1] * PACK // D
    return packed.reshape(PACK, k, D // PACK, D).transpose(0, 2, 1, 3).reshape(D, k * D)


def swap(value, axis, size, flip):
    return lax.ppermute(value, axis, [(i, i ^ flip) for i in range(size)])


def places():
    inner = lax.axis_index("fsdp")
    return (lax.axis_index("dp"), inner // 2, inner % 2)


def first_stage(me, mine, other):
    got = swap(other, "fsdp", 8, 1)
    shape = (4, 4) + mine.shape[1:]
    return stage_sum(me, [mine.reshape(shape), got.reshape(shape)])


def second_stage(me, parts):
    keep, *send = parts
    return stage_sum(me, [keep] + [swap(v, "dp", 4, k + 1) for k, v in enumerate(send)])


def third_stage(parts):
    keep, *send = parts
    return [keep] + [swap(v, "fsdp", 8, 2 * k + 2) for k, v in enumerate(send)]


def to_pairs(w):
    return w.reshape(-1, 3, 6, 128).transpose(0, 2, 1, 3).reshape(-1, 3 * D)


def from_pairs(w):
    return w.reshape(-1, 6, 3, 128).transpose(0, 2, 1, 3).reshape(-1, 3 * D)


def make_local(fast):
    def gather(shard):
        return lax.all_gather(shard, AXES, axis=0, tiled=True)

    def scatter(full):
        return lax.psum_scatter(full, AXES, scatter_dimension=0, tiled=True)

    def local(
        tokens,
        cotangent,
        lengths,
        step,
        weight_qkv,
        weight_proj,
        weight_fc1,
        weight_fc2,
        vectors,
        first_qkv,
        second_qkv,
        first_proj,
        second_proj,
        first_fc1,
        second_fc1,
        first_fc2,
        second_fc2,
        first_vectors,
        second_vectors,
    ):
        per = weight_qkv.shape[0]
        cols = vectors.shape[1]
        rows_dev, row, _ = tokens.shape
        count = rows_dev * row
        inputs = tokens.reshape(count, D)
        centered, spread = norm_input(inputs)
        if fast:
            first, packed = pack_shards(weight_qkv, weight_proj, weight_fc1, weight_fc2, vectors)
            rest = lax.all_gather(packed, AXES, axis=0, tiled=False)
            along = jnp.stack([first] + [swap(first, "fsdp", 8, 2 * k) for k in (1, 2, 3)])
            parts = [along] + [swap(along, "dp", 4, k) for k in (1, 2, 3)]
            far = parts.pop()
            parts = [parts, [swap(v, "fsdp", 8, 1) for v in parts]]
            far, parts, centered, spread = lax.optimization_barrier((far, parts, centered, spread))
            parts = parts[0] + [far] + parts[1] + [swap(far, "fsdp", 8, 1)]
            place = jnp.stack(places()).astype(jnp.int32)
        else:
            low = [w.astype(bf) for w in (weight_qkv, weight_proj, weight_fc1, weight_fc2, vectors)]
            first = jnp.concatenate([to_pairs(low[0]), jnp.pad(low[4], ((0, 0), (0, 128 - cols)))], axis=1)
            whole = gather(first).reshape(4, 4, 2, D // PACK, WIDE)
            parts = [whole[k, :, c] for c in range(2) for k in range(4)]
            place = jnp.zeros((3,), jnp.int32)
            full = [gather(w) for w in low[1:4]]
            rest = jnp.concatenate(
                [full[2].reshape(PACK, FF // PACK, D), pack_rows(full[1]), pack_rows(full[0])], axis=1
            )
        left, qkv, vec, mats_qkv = qkv_forward(place, centered, parts)
        each = lambda v, b: v[b * row : (b + 1) * row]
        done = [attn_fwd(lengths[b : b + 1], each(qkv, b), each(left, b)) for b in range(rows_dev)]
        left = jnp.concatenate([v for v, _ in done], axis=0)
        result, normed_two, grad_down, active, grad_inner, grad_middle, right, grad_mixed, sums = mlp_block(
            inputs, left, cotangent.reshape(count, D), vec, rest
        )
        grads = fc2_grad(active, grad_down, PACK, FF // PACK)
        grads = fc1_grad(normed_two, grad_inner, grads)
        if fast:
            rest_owned = lax.psum_scatter(grads, AXES, scatter_dimension=0, tiled=False)
        right = jnp.concatenate(
            [
                attn_bwd(
                    lengths[b : b + 1], each(qkv, b), each(left, b), each(grad_mixed, b), done[b][1], each(right, b)
                )
                for b in range(rows_dev)
            ],
            axis=0,
        )
        core = place[2:]
        mine_a, other_a = split_grad(core, left, right)
        if fast:
            me_dp, me_z = place[0:1], place[1:2]
            stage_a = first_stage(me_dp, mine_a, other_a)
            *stage_a, vec = lax.optimization_barrier((*stage_a, vec))
        grad_inputs, sums = input_grad(centered, spread, right, grad_middle, vec, sums, mats_qkv)
        if fast:
            stage_a = second_stage(me_z, stage_a)
            *stage_a, sums = lax.optimization_barrier((*stage_a, sums))
            owned_a = third_stage(stage_a)
            mine_b, other_b = split_grad(core, left, right, sums)
            *owned_a, other_b = lax.optimization_barrier((*owned_a, other_b))
            owned_b = third_stage(second_stage(me_z, first_stage(me_dp, mine_b, other_b)))
            *owned, squares = finish_sum(owned_a, owned_b, rest_owned)
            owned[4] = owned[4][:cols]
            squares = jnp.sum(lax.all_to_all(squares, AXES, 0, 0, tiled=True), axis=0)[0]
        else:
            mine_b, other_b = split_grad(core, left, right, sums)
            wide = FF // PACK
            part_a = jnp.stack([mine_a, other_a], axis=1).reshape(D, 2 * D)
            part_b = jnp.stack([mine_b, other_b], axis=1).reshape(D, 2 * D + 128)
            owned = [
                scatter(from_pairs(jnp.concatenate([part_a[:, D:], part_b[:, : 2 * D]], axis=1))),
                scatter(part_a[:, :D]),
                scatter(unpack_rows(grads[:, wide:])),
                scatter(grads[:, :wide].reshape(FF, D)),
                scatter(part_b[:, 2 * D : 2 * D + cols]),
            ]
            owned = [g.astype(f32) for g in owned]
            squares = lax.psum(sum(jnp.sum(g * g) for g in owned), AXES)
            owned[4] = owned[4].T
        norm = jnp.sqrt(squares)
        factor = jnp.minimum(1.0, CLIP_LIMIT / (norm + 1e-06))
        taken = step[0].astype(f32)
        fix_one = 1.0 - jnp.power(BETA_ONE, taken)
        fix_two = 1.0 - jnp.power(BETA_TWO, taken)
        rate_in = 2.0 / math.sqrt(D)
        states = (
            (weight_qkv, first_qkv, second_qkv, rate_in, 0.04),
            (weight_proj, first_proj, second_proj, 2.0 / math.sqrt(D // 48), 0.04),
            (weight_fc1, first_fc1, second_fc1, rate_in, 0.04),
            (weight_fc2, first_fc2, second_fc2, 2.0 / math.sqrt(FF), 0.04),
            (vectors.T, first_vectors.T, second_vectors.T, 1.0, 0.0),
        )
        new = [
            adam_update(w, factor * g, m, v, rate, decay, fix_one, fix_two)
            for g, (w, m, v, rate, decay) in zip(owned, states)
        ]
        new[4] = tuple(v.T for v in new[4])
        shape = (rows_dev, row, D)
        outs = [result.reshape(shape), grad_inputs.reshape(shape), norm.reshape(1)]
        outs += [w for w, _, _ in new]
        for _, m, v in new:
            outs += [m, v]
        return tuple(outs)

    return local


def solution(mesh):
    rows = P(AXES, None)
    tokens = P(AXES, None, None)
    fast = (mesh.shape["dp"], mesh.shape["fsdp"]) == (4, 8)
    return jax.shard_map(
        make_local(fast),
        mesh=mesh,
        in_specs=(tokens, tokens, rows, P()) + (rows,) * 15,
        out_specs=(tokens, tokens, P()) + (rows,) * 15,
        check_vma=False,
    )
```

```python
import functools
import math

import jax
import jax.numpy as jnp
from jax import lax
from jax.experimental import pallas as pl
from jax.experimental.pallas import tpu as pltpu
from jax.sharding import PartitionSpec as P

D = 768
FF = 3072
NORM_EPS = 1e-06
BETA_ONE = 0.9
BETA_TWO = 0.999
ADAM_EPS = 1e-08
CLIP_LIMIT = 3.0
AXES = ("dp", "fsdp")
PACK = 32
bf = jnp.bfloat16
f32 = jnp.float32


def nt(a, b):
    return lax.dot_general(a, b, (((1,), (1,)), ((), ())), preferred_element_type=f32)


def nn(a, b):
    return jnp.dot(a, b, preferred_element_type=f32)


def tn(a, b):
    return lax.dot_general(a, b, (((0,), (0,)), ((), ())), preferred_element_type=f32)


ROW=1536
BQ=256
NQ=ROW//BQ
SEGS=6
LOG2E=1.4426950408889634
BIG=float(2**30)


def seg_onehot(len_ref):
    lane=lax.broadcasted_iota(jnp.int32,(1,128),1)
    start=jnp.zeros((1,128),jnp.int32); stop=jnp.zeros((1,128),jnp.int32)
    end=jnp.int32(0)
    for s in range(SEGS):
        start=jnp.where(lane==s,end,start)
        end=end+len_ref[0,s]
        stop=jnp.where(lane==s,end,stop)
    start=jnp.where(lane==SEGS,end,start)
    stop=jnp.where(lane==SEGS,ROW,stop)
    pos=lax.broadcasted_iota(jnp.int32,(ROW,128),0)
    return jnp.where((pos>=start)&(pos<stop),1.0,0.0)


def segments(len_ref,seg,mask):
    @pl.when(pl.program_id(0)==0)
    def _():
        oh=seg_onehot(len_ref)
        seg[...]=oh.astype(bf)
        mask[...]=((oh-1.0)*BIG).astype(bf)


def half(v,r):
    low=lax.broadcasted_iota(jnp.int32,v.shape,1)<64
    return jnp.where(low,v,jnp.zeros_like(v)) if r==0 else jnp.where(low,jnp.zeros_like(v),v)


MAIN=1376
CHUNKS=((0,256),(256,512),(512,768),(768,1024),(1024,MAIN))
LAST=slice(ROW-BQ,ROW)
TAIL=slice(MAIN,ROW)
EIGHTH=0.125


def tile_rows(j):
    return pl.ds(pl.multiple_of(j*BQ,BQ),BQ)


def fwd_kernel(len_ref,qkv_ref,left_ref,o_ref,lse_ref,seg,mask,va,vb,sa,sb,ma,mb,ot,last):
    segments(len_ref,seg,mask)
    q_ref,k_ref,v_ref=(qkv_ref.at[:,128*b:128*b+128] for b in range(3))
    def query(rows,r):
        return jnp.concatenate([half(q_ref[rows,:]*jnp.asarray(EIGHTH,bf),r),seg[rows,:]],axis=1)
    def keys(rows):
        return jnp.concatenate([k_ref[rows,:],mask[rows,:]],axis=1)
    vt=v_ref[...].T
    one=(lax.broadcasted_iota(jnp.int32,(16,ROW),0)==0).astype(bf)
    va[64:80,:]=one; vb[64:80,:]=one
    va[0:64,:]=vt[0:64,:]; vb[0:64,:]=vt[64:128,:]
    for r,v_sc in enumerate((va,vb)):
        s=nt(keys(TAIL),query(LAST,r))*LOG2E
        m=jnp.max(s,axis=0,keepdims=True)
        o=nn(v_sc[:,TAIL],jnp.exp2(s-m).astype(bf))
        last[72*r:72*r+64,:]=o[0:64,:]*(1.0/o[64:65,:])
        last[72*r+64:72*r+65,:]=m+jnp.log2(o[64:65,:])
    def first(rows,r,s_sc,m_sc):
        q=query(rows,r)
        m=None
        for lo,hi in CHUNKS:
            s=nt(keys(slice(lo,hi)),q)
            s_sc[lo:hi,:]=s
            t=jnp.max(s,axis=0,keepdims=True)
            m=t if m is None else jnp.maximum(m,t)
        m_sc[0:1,:]=m*LOG2E
    def step(s_sc,m_sc,v_sc,j,r,rows,r2,s_next,m_next):
        q=query(rows,r2)
        m=m_sc[0:1,:]
        top=None
        o=0.0
        for lo,hi in CHUNKS:
            s=nt(keys(slice(lo,hi)),q)
            s_next[lo:hi,:]=s
            t=jnp.max(s,axis=0,keepdims=True)
            top=t if top is None else jnp.maximum(top,t)
        m_next[0:1,:]=top*LOG2E
        for lo,hi in CHUNKS:
            o=o+nn(v_sc[:,lo:hi],jnp.exp2(s_sc[lo:hi,:]*LOG2E-m).astype(bf))
        l=o[64:65,:]
        cols=tile_rows(j)
        ot[64*r:64*r+64,cols]=o[0:64,:]*(1.0/l)
        lse_ref[0,r:r+1,cols]=m+jnp.log2(l)
    first(pl.ds(0,BQ),0,sa,ma)
    def body(j,c):
        step(sa,ma,va,j,0,tile_rows(j),1,sb,mb)
        step(sb,mb,vb,j,1,tile_rows(jnp.minimum(j+1,NQ-1)),0,sa,ma)
        return c
    lax.fori_loop(0,NQ,body,0)
    for r in range(2):
        old=lse_ref[0,r:r+1,LAST]
        lse=last[72*r+64:72*r+65,:]
        top=jnp.maximum(old,lse)
        a=jnp.exp2(old-top); b=jnp.exp2(lse-top); t=1.0/(a+b)
        ot[64*r:64*r+64,LAST]=ot[64*r:64*r+64,LAST]*(a*t)+last[72*r:72*r+64,:]*(b*t)
        lse_ref[0,r:r+1,LAST]=top-jnp.log2(t)
    o_ref[...]=ot[...].T.astype(bf)


def attn_fwd(lengths,qkv,left):
    blk=lambda width: pl.BlockSpec((ROW,width),lambda h:(0,h))
    return pl.pallas_call(fwd_kernel,grid=(6,),
        in_specs=[pl.BlockSpec(memory_space=pltpu.SMEM),blk(384),pl.BlockSpec(memory_space=pl.ANY)],
        out_specs=[pl.BlockSpec((ROW,128),lambda h:(0,6+h)),pl.BlockSpec((1,8,ROW),lambda h:(h,0,0))],
        out_shape=[jax.ShapeDtypeStruct((ROW,2*D),bf),jax.ShapeDtypeStruct((6,8,ROW),f32)],input_output_aliases={2:0},
        scratch_shapes=[pltpu.VMEM((ROW,128),bf)]*2+[pltpu.VMEM((80,ROW),bf)]*2+[pltpu.VMEM((MAIN,BQ),f32)]*2+[pltpu.VMEM((8,BQ),f32)]*2
          +[pltpu.VMEM((128,ROW),f32),pltpu.VMEM((144,BQ),f32)],
        compiler_params=pltpu.CompilerParams(vmem_limit_bytes=60<<20),name="attn_fwd",
        cost_estimate=pl.CostEstimate(flops=4*ROW*ROW*D,bytes_accessed=10<<20,transcendentals=12*ROW*ROW))(lengths,qkv,left)


def bwd_kernel(len_ref,qkv_ref,o_ref,do_ref,lse_ref,right_ref,d_ref,
               seg,mask,kt,xa,ya,xb,yb,dqt,dqe,dka,dva):
    segments(len_ref,seg,mask)
    q_ref,k_ref,v_ref=(qkv_ref.at[:,128*b:128*b+128] for b in range(3))
    kt[...]=k_ref[...].T
    def query(rows,r):
        return half(q_ref[rows,:]*jnp.asarray(EIGHTH,bf),r)
    def keys(rows):
        return jnp.concatenate([k_ref[rows,:],mask[rows,:]],axis=1)
    def rowsums(rows):
        t=(do_ref[rows,:].astype(f32)*o_ref[rows,:].astype(f32)).T
        return [jnp.sum(t[64*r:64*r+64],axis=0,keepdims=True) for r in range(2)]
    def products(rows,r,span,x,y):
        q=jnp.concatenate([query(rows,r),seg[rows,:]],axis=1); d=half(do_ref[rows,:],r)
        for lo,hi in span:
            x[lo:hi,:]=nt(keys(slice(lo,hi)),q)
            y[lo:hi,:]=nt(v_ref[lo:hi,:],d)
    def grads(x,y,lse,total):
        p=jnp.exp2(x*LOG2E-lse)
        return p.astype(bf),(p*(y-total)).astype(bf)
    sums=rowsums(LAST)
    dv=0.0; dk=0.0
    for r in range(2):
        q=query(LAST,r); d=half(do_ref[LAST,:],r)
        p,ds=grads(nt(keys(TAIL),jnp.concatenate([q,seg[LAST,:]],axis=1)),nt(v_ref[TAIL,:],d),lse_ref[0,r:r+1,LAST],sums[r])
        dv=dv+nn(p,d); dk=dk+nn(ds,q)
        dqe[64*r:64*r+64,:]=nn(kt[64*r:64*r+64,TAIL],ds)
    dva[TAIL,:]=dv; dka[TAIL,:]=dk
    dva[0:MAIN,:]=jnp.zeros((MAIN,128),f32); dka[0:MAIN,:]=jnp.zeros((MAIN,128),f32)
    def rest(x,y,r,rows,total):
        q=query(rows,r); d=half(do_ref[rows,:],r); lse=lse_ref[0,r:r+1,rows]
        dq=0.0
        for lo,hi in CHUNKS:
            p,ds=grads(x[lo:hi,:],y[lo:hi,:],lse,total)
            dva[lo:hi,:]+=nn(p,d)
            dka[lo:hi,:]+=nn(ds,q)
            dq=dq+nn(kt[64*r:64*r+64,lo:hi],ds)
        dqt[64*r:64*r+64,rows]=dq
    def body(j,c):
        rows=tile_rows(j)
        sums=rowsums(rows)
        products(rows,0,CHUNKS,xa,ya)
        products(rows,1,CHUNKS,xb,yb)
        rest(xa,ya,0,rows,sums[0])
        rest(xb,yb,1,rows,sums[1])
        return c
    lax.fori_loop(0,NQ,body,0)
    dqt[:,LAST]+=dqe[...]
    d_ref[:,0:128]=(dqt[...].T*EIGHTH).astype(bf)
    d_ref[:,128:256]=dka[...].astype(bf)
    d_ref[:,256:384]=dva[...].astype(bf)


def attn_bwd(lengths,qkv,left,do,lse,right):
    blk=lambda width: pl.BlockSpec((ROW,width),lambda h:(0,h))
    return pl.pallas_call(bwd_kernel,grid=(6,),
        in_specs=[pl.BlockSpec(memory_space=pltpu.SMEM),blk(384),pl.BlockSpec((ROW,128),lambda h:(0,6+h)),blk(128),pl.BlockSpec((1,8,ROW),lambda h:(h,0,0)),pl.BlockSpec(memory_space=pl.ANY)],
        out_specs=blk(384),
        out_shape=jax.ShapeDtypeStruct((ROW,4*D),bf),input_output_aliases={5:0},
        scratch_shapes=[pltpu.VMEM((ROW,128),bf)]*2+[pltpu.VMEM((128,ROW),bf)]+[pltpu.VMEM((MAIN,BQ),f32)]*4
          +[pltpu.VMEM((128,ROW),f32),pltpu.VMEM((128,BQ),f32)]+[pltpu.VMEM((ROW,128),f32)]*2,
        compiler_params=pltpu.CompilerParams(vmem_limit_bytes=62<<20),name="attn_bwd",
        cost_estimate=pl.CostEstimate(flops=10*ROW*ROW*D,bytes_accessed=20<<20,transcendentals=12*ROW*ROW))(lengths,qkv,left,do,lse,right)


BM=512
INV_SQRT2=0.7071067811865476
INV_SQRT_2PI=0.3989422804014327
VMEM_CAP=62<<20


def norm_stats(v):
    center=v-jnp.mean(v,axis=1,keepdims=True)
    rstd=lax.rsqrt(jnp.mean(center*center,axis=1,keepdims=True)+NORM_EPS)
    return center*rstd,rstd


def params(**kw):
    return pltpu.CompilerParams(vmem_limit_bytes=VMEM_CAP,**kw)


def once(shape,index=None):
    return pl.BlockSpec(shape,index or (lambda i:(0,)*len(shape)),pipeline_mode=pl.Buffered(1))


def tile(width):
    return pl.BlockSpec((BM,width),lambda i:(i,0))


WIDE=3*D+128


def norm_kernel(x_ref,n_ref,r_ref):
    n,r=norm_stats(x_ref[...].astype(f32))
    n_ref[...]=n
    r_ref[...]=jnp.broadcast_to(r,r_ref.shape)


def norm_input(x):
    rows=x.shape[0]
    return pl.pallas_call(norm_kernel,grid=(rows//BM,),
        in_specs=[tile(D)],out_specs=[tile(D),tile(128)],
        out_shape=[jax.ShapeDtypeStruct((rows,D),f32),jax.ShapeDtypeStruct((rows,128),f32)],
        compiler_params=params(),name="norm_input",
        cost_estimate=pl.CostEstimate(flops=1000,bytes_accessed=1000,transcendentals=0))(x)


def pack_kernel(qkv_ref,proj_ref,fc1_ref,fc2_ref,vec_ref,first_ref,rest_ref):
    r=qkv_ref.shape[0]
    for p in range(6):
        for part in range(3):
            at=384*p+128*part
            first_ref[:,at:at+128]=qkv_ref[:,D*part+128*p:D*part+128*p+128].astype(bf)
    vec=vec_ref[...]
    vec=jnp.concatenate([vec,jnp.zeros((128-vec.shape[0],r),f32)],axis=0)
    first_ref[:,3*D:WIDE]=vec.T.astype(bf)
    rest_ref[0:4*r,:]=fc2_ref[...].astype(bf)
    for c in range(4):
        rest_ref[(4+c)*r:(5+c)*r,:]=fc1_ref[:,D*c:D*c+D].astype(bf)
    rest_ref[8*r:9*r,:]=proj_ref[...].astype(bf)


def pack_shards(qkv,proj,fc1,fc2,vectors):
    r=qkv.shape[0]
    ins=(qkv,proj,fc1,fc2,vectors.T)
    shapes=[(r,WIDE),(9*r,D)]
    whole=lambda s: pl.BlockSpec(s,lambda i:(0,)*len(s))
    return pl.pallas_call(pack_kernel,grid=(1,),
        in_specs=[whole(v.shape) for v in ins],out_specs=[whole(v) for v in shapes],
        out_shape=[jax.ShapeDtypeStruct(v,bf) for v in shapes],
        compiler_params=params(),name="pack_shards")(*ins)


def qkv_kernel(place_ref,n_ref,*refs):
    parts,(left_ref,qkv_ref,vec_ref,w_ref,w,sems,out_sem)=refs[:8],refs[8:]
    step=pl.program_id(0)
    keep=pltpu.make_async_copy(w,w_ref,out_sem)
    @pl.when(step==0)
    def _():
        copies=[]
        for i,part in enumerate(parts):
            core,dp=place_ref[2]^(i//4),place_ref[0]^(i%4)
            for k in range(4):
                copies.append(pltpu.make_async_copy(part.at[k],w.at[dp,place_ref[1]^k,core],sems.at[4*i+k]))
        for copy in copies:
            copy.start()
        for copy in copies:
            copy.wait()
        keep.start()
        vec_ref[...]=w[:,:,:,:,3*D:WIDE].reshape(D,128).astype(f32).T[0:16]
    h=(n_ref[...]*vec_ref[0:1,:]+vec_ref[1:2,:]).astype(bf)
    left_ref[...]=h
    zero=jnp.zeros((1,128),f32)
    bias=jnp.concatenate([b for p in range(6) for b in (vec_ref[2:3,128*p:128*p+128],zero,vec_ref[3:4,128*p:128*p+128])],axis=1)
    qkv_ref[...]=(nn(h,w[:,:,:,:,0:3*D].reshape(D,3*D))+bias).astype(bf)
    @pl.when(step==pl.num_programs(0)-1)
    def _():
        keep.wait()


def qkv_forward(place,n,parts):
    rows=n.shape[0]
    sd=jax.ShapeDtypeStruct
    wide=(4,4,2,D//PACK,WIDE)
    return pl.pallas_call(qkv_kernel,grid=(rows//BM,),
        in_specs=[pl.BlockSpec(memory_space=pltpu.SMEM),tile(D)]+[pl.BlockSpec(memory_space=pl.ANY)]*8,
        out_specs=[tile(D),tile(3*D),pl.BlockSpec((16,D),lambda i:(0,0)),pl.BlockSpec(memory_space=pl.ANY)],
        out_shape=[sd((rows,2*D),bf),sd((rows,3*D),bf),sd((16,D),f32),sd(wide,bf)],
        scratch_shapes=[pltpu.VMEM(wide,bf),pltpu.SemaphoreType.DMA((32,)),pltpu.SemaphoreType.DMA],
        compiler_params=params(),name="qkv_forward",
        cost_estimate=pl.CostEstimate(flops=2*rows*D*3*D,bytes_accessed=18<<20,transcendentals=0))(place,n,*parts)


CH=768


def mlp_kernel(x_ref,o_ref,dy_ref,vec_ref,rest_ref,wp_ref,
               out_ref,h_ref,dm_ref,z_ref,du_ref,dx_ref,da_ref,do_ref,sum_ref,
               a_s,x1_s,n2_s,mo_s,dh_s,ua,ub,ga,gb,w1_s,w2_s,sems):
    step=pl.program_id(0)
    r=wp_ref.shape[1]
    copies=[pltpu.make_async_copy(rest_ref.at[:,0:4*r],w2_s,sems.at[4])]
    copies+=[pltpu.make_async_copy(rest_ref.at[:,(4+b)*r:(5+b)*r],w1_s.at[b],sems.at[b]) for b in range(4)]
    @pl.when(step==0)
    def _():
        for copy in copies:
            copy.start()
        sum_ref[...]=jnp.zeros_like(sum_ref)
    row=lambda i: vec_ref[i:i+1,:]
    def add(i,v):
        sum_ref[i:i+1,:]+=jnp.sum(v,axis=0,keepdims=True)
    wp=wp_ref[...].reshape(D,D)
    a=nn(o_ref[...],wp)+row(4)
    a_s[...]=a
    x1=x_ref[...].astype(f32)+row(5)*a
    x1_s[...]=x1
    n2,r2=norm_stats(x1)
    n2_s[...]=n2
    h=(n2*row(6)+row(7)).astype(bf)
    h_ref[...]=h
    dm=(row(13)*dy_ref[...].astype(f32)).astype(bf)
    dm_ref[...]=dm
    add(12,dm.astype(f32))
    mo_s[...]=jnp.zeros_like(mo_s)
    dh_s[...]=jnp.zeros_like(dh_s)
    def w2(c):
        return w2_s[pl.ds(8*c,8)].reshape(D,D)
    @pl.when(step==0)
    def _():
        for copy in copies:
            copy.wait()
    def up(c,u,g):
        u[...]=nn(h_ref[...],w1_s[c].reshape(D,D))
        g[...]=nt(dm_ref[...],w2(c))
    def down(c,u,g):
        cols=pl.ds(pl.multiple_of(c*CH,CH),CH)
        v=u[...]+vec_ref[pl.ds(8+c,1),:]
        cdf=0.5+0.5*lax.erf(v*INV_SQRT2)
        z=(v*cdf).astype(bf)
        z_ref[:,cols]=z
        slope=cdf+v*(INV_SQRT_2PI*jnp.exp(v*v*(-0.5)))
        du=(g[...]*slope).astype(bf)
        du_ref[:,cols]=du
        sum_ref[pl.ds(8+c,1),:]+=jnp.sum(du.astype(f32),axis=0,keepdims=True)
        mo_s[...]+=nn(z,w2(c))
        dh_s[...]+=nt(du,w1_s[c].reshape(D,D))
    def body(i,carry):
        up(2*i,ua,ga)
        up(2*i+1,ub,gb)
        down(2*i,ua,ga)
        down(2*i+1,ub,gb)
        return carry
    lax.fori_loop(0,FF//CH//2,body,0)
    mo=mo_s[...]+row(12)
    out_ref[...]=(x1_s[...]+row(13)*mo).astype(bf)
    dy=dy_ref[...].astype(f32)
    add(13,dy*mo)
    dh=dh_s[...]; n2=n2_s[...]
    add(6,dh*n2); add(7,dh)
    t=dh*row(6)
    dx=dy+r2*(t-jnp.mean(t,axis=1,keepdims=True)-n2*jnp.mean(t*n2,axis=1,keepdims=True))
    dx_ref[...]=dx
    add(5,dx*a_s[...])
    da=(row(5)*dx).astype(bf)
    da_ref[...]=da
    add(4,da.astype(f32))
    do_ref[...]=nt(da,wp_ref[...].reshape(D,D)).astype(bf)


def mlp_block(x,o,dy,vec,packed):
    rows=x.shape[0]
    n,r=packed.shape[0],D//packed.shape[0]
    sd=jax.ShapeDtypeStruct
    return pl.pallas_call(mlp_kernel,grid=(rows//BM,),
        in_specs=[tile(D),pl.BlockSpec((BM,D),lambda i:(i,1)),tile(D),once((16,D)),pl.BlockSpec(memory_space=pl.ANY),once((n,r,D),lambda i:(0,8,0))],
        out_specs=[tile(D),tile(D),tile(D),tile(FF),tile(FF),tile(D),pl.BlockSpec((BM,D),lambda i:(i,3)),tile(D),pl.BlockSpec((16,D),lambda i:(0,0))],
        out_shape=[sd((rows,D),bf),sd((rows,D),bf),sd((rows,D),bf),sd((rows,FF),bf),sd((rows,FF),bf),sd((rows,D),f32),sd((rows,4*D),bf),sd((rows,D),bf),sd((16,D),f32)],
        scratch_shapes=[pltpu.VMEM((BM,D),f32)]*5+[pltpu.VMEM((BM,CH),f32)]*4+[pltpu.VMEM((4,n,r,D),bf),pltpu.VMEM((n,4*r,D),bf),pltpu.SemaphoreType.DMA((5,))],
        compiler_params=params(),name="mlp_block",
        cost_estimate=pl.CostEstimate(flops=2*rows*D*(2*D+4*FF),bytes_accessed=48<<20,transcendentals=0))(x,o,dy,vec,packed,packed)


def outer_kernel(a_ref,b_ref,g_ref):
    g_ref[...]=tn(a_ref[...],b_ref[...]).reshape(g_ref.shape).astype(bf)


def fc2_grad(z,dm,n,extra):
    rows=z.shape[0]
    per=FF//n
    return pl.pallas_call(outer_kernel,grid=(FF//D,),
        in_specs=[pl.BlockSpec((rows,D),lambda i:(0,i)),once((rows,D))],
        out_specs=pl.BlockSpec((n*D//FF,per,D),lambda i:(i,0,0)),
        out_shape=jax.ShapeDtypeStruct((n,per+extra,D),bf),
        compiler_params=params(),name="fc2_grad",
        cost_estimate=pl.CostEstimate(flops=2*rows*D*FF,bytes_accessed=16<<20,transcendentals=0))(z,dm)


def fc1_kernel(a_ref,b_ref,old_ref,g_ref):
    outer_kernel(a_ref,b_ref,g_ref)


def fc1_grad(h,du,packed):
    rows=h.shape[0]
    n=packed.shape[0]; r=D//n
    return pl.pallas_call(fc1_kernel,grid=(FF//D,),
        in_specs=[once((rows,D)),pl.BlockSpec((rows,D),lambda i:(0,i)),pl.BlockSpec(memory_space=pl.ANY)],
        out_specs=pl.BlockSpec((n,r,D),lambda i:(0,FF//D+i,0)),
        out_shape=jax.ShapeDtypeStruct(packed.shape,bf),input_output_aliases={2:0},
        compiler_params=params(),name="fc1_grad",
        cost_estimate=pl.CostEstimate(flops=2*rows*D*FF,bytes_accessed=20<<20,transcendentals=0))(h,du,packed)


def split_kernel(core_ref,left_ref,right_ref,*refs):
    sum_ref,(mine_ref,other_ref)=refs[:-2],refs[-2:]
    i=pl.program_id(0)
    even=core_ref[0]==0
    def put(v,cols):
        v=v.reshape(mine_ref.shape[0],2,mine_ref.shape[1],v.shape[1])
        mine_ref[:,:,cols]=jnp.where(even,v[:,0],v[:,1]).astype(bf)
        other_ref[:,:,cols]=jnp.where(even,v[:,1],v[:,0]).astype(bf)
    if sum_ref:
        @pl.when(i==0)
        def _():
            sums=jnp.concatenate([sum_ref[0][...],jnp.zeros((112,D),f32)],axis=0)
            put(sums.T,slice(2*D,2*D+128))
    put(tn(left_ref[...],right_ref[...]),pl.ds(pl.multiple_of(i*D,D),D))


def split_grad(core,left,right,sums=None):
    rows=left.shape[0]
    more=[] if sums is None else [sums]
    index=(lambda i:(0,1-i),lambda i:(0,3-3*i)) if sums is None else (lambda i:(0,0),lambda i:(0,1+i))
    shape=(PACK//2,D//PACK,2*D+128*len(more))
    out=pl.BlockSpec(memory_space=pltpu.VMEM)
    return pl.pallas_call(split_kernel,grid=(2,),
        in_specs=[pl.BlockSpec(memory_space=pltpu.SMEM)]+[pl.BlockSpec((rows,D),f) for f in index]+[once((16,D))]*len(more),
        out_specs=[out,out],
        out_shape=[jax.ShapeDtypeStruct(shape,bf)]*2,
        compiler_params=pltpu.CompilerParams(vmem_limit_bytes=48<<20),name="split_grad",
        cost_estimate=pl.CostEstimate(flops=1000,bytes_accessed=1000,transcendentals=0))(core,left,right,*more)


def input_kernel(n_ref,r_ref,d_ref,dx1_ref,vec_ref,old_ref,w_ref,gx_ref,sum_ref):
    @pl.when(pl.program_id(0)==0)
    def _():
        sum_ref[...]=old_ref[...]
    def add(i,v):
        sum_ref[i:i+1,:]+=v
    d=d_ref[...]
    dh=nt(d,w_ref[...].reshape(D,3*D))
    total=jnp.sum(d.astype(f32),axis=0,keepdims=True)
    n=n_ref[...]; r=r_ref[:,0:1]
    add(0,jnp.sum(dh*n,axis=0,keepdims=True))
    add(1,jnp.sum(dh,axis=0,keepdims=True))
    for i,b in ((2,0),(3,2)):
        add(i,jnp.concatenate([total[:,384*p+128*b:384*p+128*b+128] for p in range(6)],axis=1))
    t=dh*vec_ref[0:1,:]
    dx=dx1_ref[...]+r*(t-jnp.mean(t,axis=1,keepdims=True)-n*jnp.mean(t*n,axis=1,keepdims=True))
    gx_ref[...]=dx.astype(bf)


def input_grad(n,r,d,dx1,vec,sums,w):
    rows=n.shape[0]
    return pl.pallas_call(input_kernel,grid=(rows//BM,),
        in_specs=[tile(D),tile(128),tile(3*D),tile(D),once((16,D)),once((16,D)),once(w.shape[:-1]+(3*D,),lambda i:(0,)*len(w.shape))],
        out_specs=[tile(D),pl.BlockSpec((16,D),lambda i:(0,0))],
        out_shape=[jax.ShapeDtypeStruct((rows,D),bf),jax.ShapeDtypeStruct((16,D),f32)],
        compiler_params=params(),name="input_grad",
        cost_estimate=pl.CostEstimate(flops=1000,bytes_accessed=1000,transcendentals=0))(n,r,d,dx1,vec,sums,w)


def stage_kernel(count,place_ref,*refs):
    ins,outs=refs[:count],refs[count:]
    for k,out in enumerate(outs):
        at=place_ref[0]^k
        out[...]=sum(ref[at].astype(f32) for ref in ins).astype(bf)


def stage_sum(place,parts):
    shape=parts[0].shape
    near=pl.BlockSpec(memory_space=pltpu.VMEM)
    return pl.pallas_call(functools.partial(stage_kernel,len(parts)),
        in_specs=[pl.BlockSpec(memory_space=pltpu.SMEM)]+[near]*len(parts),
        out_specs=[near]*4,
        out_shape=[jax.ShapeDtypeStruct(shape[1:],bf)]*4,
        compiler_params=pltpu.CompilerParams(vmem_limit_bytes=16<<20),name="stage_sum",
        cost_estimate=pl.CostEstimate(flops=1000,bytes_accessed=1000,transcendentals=0))(place,*parts)


def finish_kernel(*refs):
    first,second,(rest_ref,qkv_ref,proj_ref,fc1_ref,fc2_ref,vec_ref,square_ref)=refs[:4],refs[4:8],refs[8:]
    a=sum(ref[...].astype(f32) for ref in first)
    b=sum(ref[...].astype(f32) for ref in second)
    rest=rest_ref[...].astype(f32)
    total=jnp.sum(a*a,keepdims=True)+jnp.sum(b*b,keepdims=True)+jnp.sum(rest*rest,keepdims=True)
    square_ref[...]=jnp.broadcast_to(total,square_ref.shape)
    r=a.shape[0]
    proj_ref[...]=a[:,0:D]
    for p in range(6):
        for part in range(3):
            at=384*p+128*part
            qkv_ref[:,D*part+128*p:D*part+128*p+128]=a[:,D+at:D+at+128] if p<2 else b[:,at-D:at-D+128]
    vec_ref[...]=b[:,2*D:2*D+128].T
    fc2_ref[...]=rest[0:4*r]
    for c in range(4):
        fc1_ref[:,D*c:D*c+D]=rest[(4+c)*r:(5+c)*r]


def finish_sum(first,second,rest):
    near=pl.BlockSpec(memory_space=pltpu.VMEM)
    r=rest.shape[0]//8
    shapes=[(r,3*D),(r,D),(r,FF),(4*r,D),(128,r),(PACK,128)]
    return pl.pallas_call(finish_kernel,grid=(1,),
        in_specs=[near]*9,
        out_specs=[pl.BlockSpec(v,lambda i:(0,0)) for v in shapes[:5]]+[near],
        out_shape=[jax.ShapeDtypeStruct(v,f32) for v in shapes],
        compiler_params=pltpu.CompilerParams(vmem_limit_bytes=58<<20),name="finish_sum",
        cost_estimate=pl.CostEstimate(flops=1000,bytes_accessed=1000,transcendentals=0))(*first,*second,rest)


RATES=((2.0/math.sqrt(D),0.04),(2.0/math.sqrt(D//48),0.04),(2.0/math.sqrt(D),0.04),(2.0/math.sqrt(FF),0.04),(1.0,0.0))


def adam_kernel(fix_ref,square_ref,*refs):
    grads,states,outs=refs[:5],refs[5:20],refs[20:]
    norm=jnp.sqrt(jnp.sum(square_ref[...],axis=0,keepdims=True)[:,0:1])
    outs[0][...]=norm
    factor=jnp.minimum(1.0,CLIP_LIMIT/(norm+1e-06))
    for k,(rate,decay) in enumerate(RATES):
        weight,first,second=(ref[...] for ref in states[3*k:3*k+3])
        grad=factor*grads[k][0:weight.shape[0],:]
        first=BETA_ONE*first+(1.0-BETA_ONE)*grad
        second=BETA_TWO*second+(1.0-BETA_TWO)*grad*grad
        stride=first/fix_ref[0]/(jnp.sqrt(second/fix_ref[1])+ADAM_EPS)
        outs[3*k+1][...]=weight-rate*(stride+decay*weight)
        outs[3*k+2][...]=first
        outs[3*k+3][...]=second


def adam_all(fix,squares,grads,states):
    whole=lambda v: pl.BlockSpec(v,lambda i:(0,0))
    shapes=[(1,1)]+[v.shape for v in states]
    return pl.pallas_call(adam_kernel,grid=(1,),
        in_specs=[pl.BlockSpec(memory_space=pltpu.SMEM)]+[whole(v.shape) for v in (squares,*grads,*states)],
        out_specs=[whole(v) for v in shapes],
        out_shape=[jax.ShapeDtypeStruct(v,f32) for v in shapes],
        compiler_params=params(),name="adam_all")(fix,squares,*grads,*states)


def pack_rows(full):
    k = full.shape[1] // D
    return full.reshape(PACK, D // PACK, k, D).transpose(0, 2, 1, 3).reshape(PACK, -1, D)


def unpack_rows(packed):
    k = packed.shape[1] * PACK // D
    return packed.reshape(PACK, k, D // PACK, D).transpose(0, 2, 1, 3).reshape(D, k * D)


def swap(value, axis, size, flip):
    return lax.ppermute(value, axis, [(i, i ^ flip) for i in range(size)])


def places():
    inner = lax.axis_index("fsdp")
    return (lax.axis_index("dp"), inner // 2, inner % 2)


def first_stage(me, mine, other):
    got = swap(other, "fsdp", 8, 1)
    shape = (4, 4) + mine.shape[1:]
    return stage_sum(me, [mine.reshape(shape), got.reshape(shape)])


def second_stage(me, parts):
    keep, *send = parts
    return stage_sum(me, [keep] + [swap(v, "dp", 4, k + 1) for k, v in enumerate(send)])


def third_stage(parts):
    keep, *send = parts
    return [keep] + [swap(v, "fsdp", 8, 2 * k + 2) for k, v in enumerate(send)]


def to_pairs(w):
    return w.reshape(-1, 3, 6, 128).transpose(0, 2, 1, 3).reshape(-1, 3 * D)


def from_pairs(w):
    return w.reshape(-1, 6, 3, 128).transpose(0, 2, 1, 3).reshape(-1, 3 * D)


def make_local(fast):
    def gather(shard):
        return lax.all_gather(shard, AXES, axis=0, tiled=True)

    def scatter(full):
        return lax.psum_scatter(full, AXES, scatter_dimension=0, tiled=True)

    def local(
        tokens,
        cotangent,
        lengths,
        step,
        weight_qkv,
        weight_proj,
        weight_fc1,
        weight_fc2,
        vectors,
        first_qkv,
        second_qkv,
        first_proj,
        second_proj,
        first_fc1,
        second_fc1,
        first_fc2,
        second_fc2,
        first_vectors,
        second_vectors,
    ):
        per = weight_qkv.shape[0]
        cols = vectors.shape[1]
        rows_dev, row, _ = tokens.shape
        count = rows_dev * row
        inputs = tokens.reshape(count, D)
        centered, spread = norm_input(inputs)
        if fast:
            first, packed = pack_shards(weight_qkv, weight_proj, weight_fc1, weight_fc2, vectors)
            rest = lax.all_gather(packed, AXES, axis=0, tiled=False)
            along = jnp.stack([first] + [swap(first, "fsdp", 8, 2 * k) for k in (1, 2, 3)])
            parts = [along] + [swap(along, "dp", 4, k) for k in (1, 2, 3)]
            far = parts.pop()
            parts = [parts, [swap(v, "fsdp", 8, 1) for v in parts]]
            far, parts, centered, spread = lax.optimization_barrier((far, parts, centered, spread))
            parts = parts[0] + [far] + parts[1] + [swap(far, "fsdp", 8, 1)]
            place = jnp.stack(places()).astype(jnp.int32)
        else:
            low = [w.astype(bf) for w in (weight_qkv, weight_proj, weight_fc1, weight_fc2, vectors)]
            first = jnp.concatenate([to_pairs(low[0]), jnp.pad(low[4], ((0, 0), (0, 128 - cols)))], axis=1)
            whole = gather(first).reshape(4, 4, 2, D // PACK, WIDE)
            parts = [whole[k, :, c] for c in range(2) for k in range(4)]
            place = jnp.zeros((3,), jnp.int32)
            full = [gather(w) for w in low[1:4]]
            rest = jnp.concatenate(
                [full[2].reshape(PACK, FF // PACK, D), pack_rows(full[1]), pack_rows(full[0])], axis=1
            )
        left, qkv, vec, mats_qkv = qkv_forward(place, centered, parts)
        each = lambda v, b: v[b * row : (b + 1) * row]
        done = [attn_fwd(lengths[b : b + 1], each(qkv, b), each(left, b)) for b in range(rows_dev)]
        left = jnp.concatenate([v for v, _ in done], axis=0)
        result, normed_two, grad_down, active, grad_inner, grad_middle, right, grad_mixed, sums = mlp_block(
            inputs, left, cotangent.reshape(count, D), vec, rest
        )
        grads = fc2_grad(active, grad_down, PACK, FF // PACK)
        grads = fc1_grad(normed_two, grad_inner, grads)
        if fast:
            rest_owned = lax.psum_scatter(grads, AXES, scatter_dimension=0, tiled=False)
        right = jnp.concatenate(
            [
                attn_bwd(
                    lengths[b : b + 1], each(qkv, b), each(left, b), each(grad_mixed, b), done[b][1], each(right, b)
                )
                for b in range(rows_dev)
            ],
            axis=0,
        )
        core = place[2:]
        mine_a, other_a = split_grad(core, left, right)
        if fast:
            me_dp, me_z = place[0:1], place[1:2]
            stage_a = first_stage(me_dp, mine_a, other_a)
            *stage_a, vec = lax.optimization_barrier((*stage_a, vec))
        grad_inputs, sums = input_grad(centered, spread, right, grad_middle, vec, sums, mats_qkv)
        if fast:
            stage_a = second_stage(me_z, stage_a)
            *stage_a, sums = lax.optimization_barrier((*stage_a, sums))
            owned_a = third_stage(stage_a)
            mine_b, other_b = split_grad(core, left, right, sums)
            *owned_a, other_b = lax.optimization_barrier((*owned_a, other_b))
            owned_b = third_stage(second_stage(me_z, first_stage(me_dp, mine_b, other_b)))
            *owned, squares = finish_sum(owned_a, owned_b, rest_owned)
            squares = lax.all_to_all(squares, AXES, 0, 0, tiled=True)
        else:
            mine_b, other_b = split_grad(core, left, right, sums)
            wide = FF // PACK
            part_a = jnp.stack([mine_a, other_a], axis=1).reshape(D, 2 * D)
            part_b = jnp.stack([mine_b, other_b], axis=1).reshape(D, 2 * D + 128)
            owned = [
                scatter(from_pairs(jnp.concatenate([part_a[:, D:], part_b[:, : 2 * D]], axis=1))),
                scatter(part_a[:, :D]),
                scatter(unpack_rows(grads[:, wide:])),
                scatter(grads[:, :wide].reshape(FF, D)),
                scatter(part_b[:, 2 * D : 2 * D + cols]),
            ]
            owned = [g.astype(f32) for g in owned]
            squares = jnp.full((1, 128), lax.psum(sum(jnp.sum(g * g) for g in owned), AXES))
            owned[4] = owned[4].T
        taken = step[0].astype(f32)
        fix = jnp.stack([1.0 - jnp.power(BETA_ONE, taken), 1.0 - jnp.power(BETA_TWO, taken)])
        states = (weight_qkv, first_qkv, second_qkv, weight_proj, first_proj, second_proj)
        states += (weight_fc1, first_fc1, second_fc1, weight_fc2, first_fc2, second_fc2)
        norm, *new = adam_all(fix, squares, owned, states + (vectors.T, first_vectors.T, second_vectors.T))
        new[12:] = [v.T for v in new[12:]]
        shape = (rows_dev, row, D)
        outs = [result.reshape(shape), grad_inputs.reshape(shape), norm.reshape(1)] + new[0::3]
        for k in range(5):
            outs += new[3 * k + 1 : 3 * k + 3]
        return tuple(outs)

    return local


def solution(mesh):
    rows = P(AXES, None)
    tokens = P(AXES, None, None)
    fast = (mesh.shape["dp"], mesh.shape["fsdp"]) == (4, 8)
    return jax.shard_map(
        make_local(fast),
        mesh=mesh,
        in_specs=(tokens, tokens, rows, P()) + (rows,) * 15,
        out_specs=(tokens, tokens, P()) + (rows,) * 15,
        check_vma=False,
    )
```

```python
import functools
import math

import jax
import jax.numpy as jnp
from jax import lax
from jax.experimental import pallas as pl
from jax.experimental.pallas import tpu as pltpu
from jax.sharding import PartitionSpec as P

D = 768
FF = 3072
NORM_EPS = 1e-06
BETA_ONE = 0.9
BETA_TWO = 0.999
ADAM_EPS = 1e-08
CLIP_LIMIT = 3.0
AXES = ("dp", "fsdp")
PACK = 32
bf = jnp.bfloat16
f32 = jnp.float32


def nt(a, b):
    return lax.dot_general(a, b, (((1,), (1,)), ((), ())), preferred_element_type=f32)


def nn(a, b):
    return jnp.dot(a, b, preferred_element_type=f32)


def tn(a, b):
    return lax.dot_general(a, b, (((0,), (0,)), ((), ())), preferred_element_type=f32)


ROW=1536
BQ=256
NQ=ROW//BQ
SEGS=6
LOG2E=1.4426950408889634
BIG=float(2**30)


def seg_onehot(len_ref):
    lane=lax.broadcasted_iota(jnp.int32,(1,128),1)
    start=jnp.zeros((1,128),jnp.int32); stop=jnp.zeros((1,128),jnp.int32)
    end=jnp.int32(0)
    for s in range(SEGS):
        start=jnp.where(lane==s,end,start)
        end=end+len_ref[0,s]
        stop=jnp.where(lane==s,end,stop)
    start=jnp.where(lane==SEGS,end,start)
    stop=jnp.where(lane==SEGS,ROW,stop)
    pos=lax.broadcasted_iota(jnp.int32,(ROW,128),0)
    return jnp.where((pos>=start)&(pos<stop),1.0,0.0)


def segments(len_ref,seg,mask):
    @pl.when(pl.program_id(0)==0)
    def _():
        oh=seg_onehot(len_ref)
        seg[...]=oh.astype(bf)
        mask[...]=((oh-1.0)*BIG).astype(bf)


def half(v,r):
    low=lax.broadcasted_iota(jnp.int32,v.shape,1)<64
    return jnp.where(low,v,jnp.zeros_like(v)) if r==0 else jnp.where(low,jnp.zeros_like(v),v)


MAIN=1376
CHUNKS=((0,256),(256,512),(512,768),(768,1024),(1024,MAIN))
LAST=slice(ROW-BQ,ROW)
TAIL=slice(MAIN,ROW)
EIGHTH=0.125


def tile_rows(j):
    return pl.ds(pl.multiple_of(j*BQ,BQ),BQ)


def fwd_kernel(len_ref,qkv_ref,left_ref,o_ref,lse_ref,seg,mask,va,vb,sa,sb,ma,mb,ot,last):
    segments(len_ref,seg,mask)
    q_ref,k_ref,v_ref=(qkv_ref.at[:,128*b:128*b+128] for b in range(3))
    def query(rows,r):
        return jnp.concatenate([half(q_ref[rows,:]*jnp.asarray(EIGHTH,bf),r),seg[rows,:]],axis=1)
    def keys(rows):
        return jnp.concatenate([k_ref[rows,:],mask[rows,:]],axis=1)
    vt=v_ref[...].T
    one=(lax.broadcasted_iota(jnp.int32,(16,ROW),0)==0).astype(bf)
    va[64:80,:]=one; vb[64:80,:]=one
    va[0:64,:]=vt[0:64,:]; vb[0:64,:]=vt[64:128,:]
    for r,v_sc in enumerate((va,vb)):
        s=nt(keys(TAIL),query(LAST,r))*LOG2E
        m=jnp.max(s,axis=0,keepdims=True)
        o=nn(v_sc[:,TAIL],jnp.exp2(s-m).astype(bf))
        last[72*r:72*r+64,:]=o[0:64,:]*(1.0/o[64:65,:])
        last[72*r+64:72*r+65,:]=m+jnp.log2(o[64:65,:])
    def first(rows,r,s_sc,m_sc):
        q=query(rows,r)
        m=None
        for lo,hi in CHUNKS:
            s=nt(keys(slice(lo,hi)),q)
            s_sc[lo:hi,:]=s
            t=jnp.max(s,axis=0,keepdims=True)
            m=t if m is None else jnp.maximum(m,t)
        m_sc[0:1,:]=m*LOG2E
    def step(s_sc,m_sc,v_sc,j,r,rows,r2,s_next,m_next):
        q=query(rows,r2)
        m=m_sc[0:1,:]
        top=None
        o=0.0
        for lo,hi in CHUNKS:
            s=nt(keys(slice(lo,hi)),q)
            s_next[lo:hi,:]=s
            t=jnp.max(s,axis=0,keepdims=True)
            top=t if top is None else jnp.maximum(top,t)
        m_next[0:1,:]=top*LOG2E
        for lo,hi in CHUNKS:
            o=o+nn(v_sc[:,lo:hi],jnp.exp2(s_sc[lo:hi,:]*LOG2E-m).astype(bf))
        l=o[64:65,:]
        cols=tile_rows(j)
        ot[64*r:64*r+64,cols]=o[0:64,:]*(1.0/l)
        lse_ref[0,r:r+1,cols]=m+jnp.log2(l)
    first(pl.ds(0,BQ),0,sa,ma)
    def body(j,c):
        step(sa,ma,va,j,0,tile_rows(j),1,sb,mb)
        step(sb,mb,vb,j,1,tile_rows(jnp.minimum(j+1,NQ-1)),0,sa,ma)
        return c
    lax.fori_loop(0,NQ,body,0)
    for r in range(2):
        old=lse_ref[0,r:r+1,LAST]
        lse=last[72*r+64:72*r+65,:]
        top=jnp.maximum(old,lse)
        a=jnp.exp2(old-top); b=jnp.exp2(lse-top); t=1.0/(a+b)
        ot[64*r:64*r+64,LAST]=ot[64*r:64*r+64,LAST]*(a*t)+last[72*r:72*r+64,:]*(b*t)
        lse_ref[0,r:r+1,LAST]=top-jnp.log2(t)
    o_ref[...]=ot[...].T.astype(bf)


def attn_fwd(lengths,qkv,left):
    blk=lambda width: pl.BlockSpec((ROW,width),lambda h:(0,h))
    return pl.pallas_call(fwd_kernel,grid=(6,),
        in_specs=[pl.BlockSpec(memory_space=pltpu.SMEM),blk(384),pl.BlockSpec(memory_space=pl.ANY)],
        out_specs=[pl.BlockSpec((ROW,128),lambda h:(0,6+h)),pl.BlockSpec((1,8,ROW),lambda h:(h,0,0))],
        out_shape=[jax.ShapeDtypeStruct((ROW,2*D),bf),jax.ShapeDtypeStruct((6,8,ROW),f32)],input_output_aliases={2:0},
        scratch_shapes=[pltpu.VMEM((ROW,128),bf)]*2+[pltpu.VMEM((80,ROW),bf)]*2+[pltpu.VMEM((MAIN,BQ),f32)]*2+[pltpu.VMEM((8,BQ),f32)]*2
          +[pltpu.VMEM((128,ROW),f32),pltpu.VMEM((144,BQ),f32)],
        compiler_params=pltpu.CompilerParams(vmem_limit_bytes=60<<20),name="attn_fwd",
        cost_estimate=pl.CostEstimate(flops=4*ROW*ROW*D,bytes_accessed=10<<20,transcendentals=12*ROW*ROW))(lengths,qkv,left)


def bwd_kernel(len_ref,qkv_ref,o_ref,do_ref,lse_ref,right_ref,d_ref,
               seg,mask,kt,xa,ya,xb,yb,dqt,dqe,dka,dva):
    segments(len_ref,seg,mask)
    q_ref,k_ref,v_ref=(qkv_ref.at[:,128*b:128*b+128] for b in range(3))
    kt[...]=k_ref[...].T
    def query(rows,r):
        return half(q_ref[rows,:]*jnp.asarray(EIGHTH,bf),r)
    def keys(rows):
        return jnp.concatenate([k_ref[rows,:],mask[rows,:]],axis=1)
    def rowsums(rows):
        t=(do_ref[rows,:].astype(f32)*o_ref[rows,:].astype(f32)).T
        return [jnp.sum(t[64*r:64*r+64],axis=0,keepdims=True) for r in range(2)]
    def products(rows,r,span,x,y):
        q=jnp.concatenate([query(rows,r),seg[rows,:]],axis=1); d=half(do_ref[rows,:],r)
        for lo,hi in span:
            x[lo:hi,:]=nt(keys(slice(lo,hi)),q)
            y[lo:hi,:]=nt(v_ref[lo:hi,:],d)
    def grads(x,y,lse,total):
        p=jnp.exp2(x*LOG2E-lse)
        return p.astype(bf),(p*(y-total)).astype(bf)
    sums=rowsums(LAST)
    dv=0.0; dk=0.0
    for r in range(2):
        q=query(LAST,r); d=half(do_ref[LAST,:],r)
        p,ds=grads(nt(keys(TAIL),jnp.concatenate([q,seg[LAST,:]],axis=1)),nt(v_ref[TAIL,:],d),lse_ref[0,r:r+1,LAST],sums[r])
        dv=dv+nn(p,d); dk=dk+nn(ds,q)
        dqe[64*r:64*r+64,:]=nn(kt[64*r:64*r+64,TAIL],ds)
    dva[TAIL,:]=dv; dka[TAIL,:]=dk
    dva[0:MAIN,:]=jnp.zeros((MAIN,128),f32); dka[0:MAIN,:]=jnp.zeros((MAIN,128),f32)
    def rest(x,y,r,rows,total):
        q=query(rows,r); d=half(do_ref[rows,:],r); lse=lse_ref[0,r:r+1,rows]
        dq=0.0
        for lo,hi in CHUNKS:
            p,ds=grads(x[lo:hi,:],y[lo:hi,:],lse,total)
            dva[lo:hi,:]+=nn(p,d)
            dka[lo:hi,:]+=nn(ds,q)
            dq=dq+nn(kt[64*r:64*r+64,lo:hi],ds)
        dqt[64*r:64*r+64,rows]=dq
    def body(j,c):
        rows=tile_rows(j)
        sums=rowsums(rows)
        products(rows,0,CHUNKS,xa,ya)
        products(rows,1,CHUNKS,xb,yb)
        rest(xa,ya,0,rows,sums[0])
        rest(xb,yb,1,rows,sums[1])
        return c
    lax.fori_loop(0,NQ,body,0)
    dqt[:,LAST]+=dqe[...]
    d_ref[:,0:128]=(dqt[...].T*EIGHTH).astype(bf)
    d_ref[:,128:256]=dka[...].astype(bf)
    d_ref[:,256:384]=dva[...].astype(bf)


def attn_bwd(lengths,qkv,left,do,lse,right):
    blk=lambda width: pl.BlockSpec((ROW,width),lambda h:(0,h))
    return pl.pallas_call(bwd_kernel,grid=(6,),
        in_specs=[pl.BlockSpec(memory_space=pltpu.SMEM),blk(384),pl.BlockSpec((ROW,128),lambda h:(0,6+h)),blk(128),pl.BlockSpec((1,8,ROW),lambda h:(h,0,0)),pl.BlockSpec(memory_space=pl.ANY)],
        out_specs=blk(384),
        out_shape=jax.ShapeDtypeStruct((ROW,4*D),bf),input_output_aliases={5:0},
        scratch_shapes=[pltpu.VMEM((ROW,128),bf)]*2+[pltpu.VMEM((128,ROW),bf)]+[pltpu.VMEM((MAIN,BQ),f32)]*4
          +[pltpu.VMEM((128,ROW),f32),pltpu.VMEM((128,BQ),f32)]+[pltpu.VMEM((ROW,128),f32)]*2,
        compiler_params=pltpu.CompilerParams(vmem_limit_bytes=62<<20),name="attn_bwd",
        cost_estimate=pl.CostEstimate(flops=10*ROW*ROW*D,bytes_accessed=20<<20,transcendentals=12*ROW*ROW))(lengths,qkv,left,do,lse,right)


BM=512
INV_SQRT2=0.7071067811865476
INV_SQRT_2PI=0.3989422804014327
VMEM_CAP=62<<20


def norm_stats(v):
    center=v-jnp.mean(v,axis=1,keepdims=True)
    rstd=lax.rsqrt(jnp.mean(center*center,axis=1,keepdims=True)+NORM_EPS)
    return center*rstd,rstd


def params(**kw):
    return pltpu.CompilerParams(vmem_limit_bytes=VMEM_CAP,**kw)


def once(shape,index=None):
    return pl.BlockSpec(shape,index or (lambda i:(0,)*len(shape)),pipeline_mode=pl.Buffered(1))


def tile(width):
    return pl.BlockSpec((BM,width),lambda i:(i,0))


WIDE=3*D+128


def norm_kernel(x_ref,n_ref,r_ref):
    n,r=norm_stats(x_ref[...].astype(f32))
    n_ref[...]=n
    r_ref[...]=jnp.broadcast_to(r,r_ref.shape)


def norm_input(x):
    rows=x.shape[0]
    return pl.pallas_call(norm_kernel,grid=(rows//BM,),
        in_specs=[tile(D)],out_specs=[tile(D),tile(128)],
        out_shape=[jax.ShapeDtypeStruct((rows,D),f32),jax.ShapeDtypeStruct((rows,128),f32)],
        compiler_params=params(),name="norm_input",
        cost_estimate=pl.CostEstimate(flops=1000,bytes_accessed=1000,transcendentals=0))(x)


def pack_kernel(qkv_ref,proj_ref,fc1_ref,fc2_ref,vec_ref,first_ref,rest_ref):
    r=qkv_ref.shape[0]
    for p in range(6):
        for part in range(3):
            at=384*p+128*part
            first_ref[:,at:at+128]=qkv_ref[:,D*part+128*p:D*part+128*p+128].astype(bf)
    vec=vec_ref[...]
    vec=jnp.concatenate([vec,jnp.zeros((128-vec.shape[0],r),f32)],axis=0)
    first_ref[:,3*D:WIDE]=vec.T.astype(bf)
    rest_ref[0:4*r,:]=fc2_ref[...].astype(bf)
    for c in range(4):
        rest_ref[(4+c)*r:(5+c)*r,:]=fc1_ref[:,D*c:D*c+D].astype(bf)
    rest_ref[8*r:9*r,:]=proj_ref[...].astype(bf)


def pack_shards(qkv,proj,fc1,fc2,vectors):
    r=qkv.shape[0]
    ins=(qkv,proj,fc1,fc2,vectors.T)
    shapes=[(r,WIDE),(9*r,D)]
    whole=lambda s: pl.BlockSpec(s,lambda i:(0,)*len(s))
    return pl.pallas_call(pack_kernel,grid=(1,),
        in_specs=[whole(v.shape) for v in ins],out_specs=[whole(v) for v in shapes],
        out_shape=[jax.ShapeDtypeStruct(v,bf) for v in shapes],
        compiler_params=params(),name="pack_shards")(*ins)


def qkv_kernel(place_ref,n_ref,*refs):
    parts,(left_ref,qkv_ref,vec_ref,w_ref,w,sems,out_sem)=refs[:8],refs[8:]
    step=pl.program_id(0)
    keep=pltpu.make_async_copy(w,w_ref,out_sem)
    @pl.when(step==0)
    def _():
        copies=[]
        for i,part in enumerate(parts):
            core,dp=place_ref[2]^(i//4),place_ref[0]^(i%4)
            for k in range(4):
                copies.append(pltpu.make_async_copy(part.at[k],w.at[dp,place_ref[1]^k,core],sems.at[4*i+k]))
        for copy in copies:
            copy.start()
        for copy in copies:
            copy.wait()
        keep.start()
        vec_ref[...]=w[:,:,:,:,3*D:WIDE].reshape(D,128).astype(f32).T[0:16]
    h=(n_ref[...]*vec_ref[0:1,:]+vec_ref[1:2,:]).astype(bf)
    left_ref[...]=h
    zero=jnp.zeros((1,128),f32)
    bias=jnp.concatenate([b for p in range(6) for b in (vec_ref[2:3,128*p:128*p+128],zero,vec_ref[3:4,128*p:128*p+128])],axis=1)
    qkv_ref[...]=(nn(h,w[:,:,:,:,0:3*D].reshape(D,3*D))+bias).astype(bf)
    @pl.when(step==pl.num_programs(0)-1)
    def _():
        keep.wait()


def qkv_forward(place,n,parts):
    rows=n.shape[0]
    sd=jax.ShapeDtypeStruct
    wide=(4,4,2,D//PACK,WIDE)
    return pl.pallas_call(qkv_kernel,grid=(rows//BM,),
        in_specs=[pl.BlockSpec(memory_space=pltpu.SMEM),tile(D)]+[pl.BlockSpec(memory_space=pl.ANY)]*8,
        out_specs=[tile(D),tile(3*D),pl.BlockSpec((16,D),lambda i:(0,0)),pl.BlockSpec(memory_space=pl.ANY)],
        out_shape=[sd((rows,2*D),bf),sd((rows,3*D),bf),sd((16,D),f32),sd(wide,bf)],
        scratch_shapes=[pltpu.VMEM(wide,bf),pltpu.SemaphoreType.DMA((32,)),pltpu.SemaphoreType.DMA],
        compiler_params=params(),name="qkv_forward",
        cost_estimate=pl.CostEstimate(flops=2*rows*D*3*D,bytes_accessed=18<<20,transcendentals=0))(place,n,*parts)


CH=768


def mlp_kernel(x_ref,o_ref,dy_ref,vec_ref,rest_ref,wp_ref,
               out_ref,h_ref,dm_ref,z_ref,du_ref,dx_ref,da_ref,do_ref,sum_ref,
               a_s,x1_s,n2_s,mo_s,dh_s,ua,ub,ga,gb,w1_s,w2_s,sems):
    step=pl.program_id(0)
    r=wp_ref.shape[1]
    copies=[pltpu.make_async_copy(rest_ref.at[:,0:4*r],w2_s,sems.at[4])]
    copies+=[pltpu.make_async_copy(rest_ref.at[:,(4+b)*r:(5+b)*r],w1_s.at[b],sems.at[b]) for b in range(4)]
    @pl.when(step==0)
    def _():
        for copy in copies:
            copy.start()
        sum_ref[...]=jnp.zeros_like(sum_ref)
    row=lambda i: vec_ref[i:i+1,:]
    def add(i,v):
        sum_ref[i:i+1,:]+=jnp.sum(v,axis=0,keepdims=True)
    wp=wp_ref[...].reshape(D,D)
    a=nn(o_ref[...],wp)+row(4)
    a_s[...]=a
    x1=x_ref[...].astype(f32)+row(5)*a
    x1_s[...]=x1
    n2,r2=norm_stats(x1)
    n2_s[...]=n2
    h=(n2*row(6)+row(7)).astype(bf)
    h_ref[...]=h
    dm=(row(13)*dy_ref[...].astype(f32)).astype(bf)
    dm_ref[...]=dm
    add(12,dm.astype(f32))
    mo_s[...]=jnp.zeros_like(mo_s)
    dh_s[...]=jnp.zeros_like(dh_s)
    def w2(c):
        return w2_s[pl.ds(8*c,8)].reshape(D,D)
    @pl.when(step==0)
    def _():
        for copy in copies:
            copy.wait()
    def up(c,u,g):
        u[...]=nn(h_ref[...],w1_s[c].reshape(D,D))
        g[...]=nt(dm_ref[...],w2(c))
    def down(c,u,g):
        cols=pl.ds(pl.multiple_of(c*CH,CH),CH)
        v=u[...]+vec_ref[pl.ds(8+c,1),:]
        cdf=0.5+0.5*lax.erf(v*INV_SQRT2)
        z=(v*cdf).astype(bf)
        z_ref[:,cols]=z
        slope=cdf+v*(INV_SQRT_2PI*jnp.exp(v*v*(-0.5)))
        du=(g[...]*slope).astype(bf)
        du_ref[:,cols]=du
        sum_ref[pl.ds(8+c,1),:]+=jnp.sum(du.astype(f32),axis=0,keepdims=True)
        mo_s[...]+=nn(z,w2(c))
        dh_s[...]+=nt(du,w1_s[c].reshape(D,D))
    def body(i,carry):
        up(2*i,ua,ga)
        up(2*i+1,ub,gb)
        down(2*i,ua,ga)
        down(2*i+1,ub,gb)
        return carry
    lax.fori_loop(0,FF//CH//2,body,0)
    mo=mo_s[...]+row(12)
    out_ref[...]=(x1_s[...]+row(13)*mo).astype(bf)
    dy=dy_ref[...].astype(f32)
    add(13,dy*mo)
    dh=dh_s[...]; n2=n2_s[...]
    add(6,dh*n2); add(7,dh)
    t=dh*row(6)
    dx=dy+r2*(t-jnp.mean(t,axis=1,keepdims=True)-n2*jnp.mean(t*n2,axis=1,keepdims=True))
    dx_ref[...]=dx
    add(5,dx*a_s[...])
    da=(row(5)*dx).astype(bf)
    da_ref[...]=da
    add(4,da.astype(f32))
    do_ref[...]=nt(da,wp_ref[...].reshape(D,D)).astype(bf)


def mlp_block(x,o,dy,vec,packed):
    rows=x.shape[0]
    n,r=packed.shape[0],D//packed.shape[0]
    sd=jax.ShapeDtypeStruct
    return pl.pallas_call(mlp_kernel,grid=(rows//BM,),
        in_specs=[tile(D),pl.BlockSpec((BM,D),lambda i:(i,1)),tile(D),once((16,D)),pl.BlockSpec(memory_space=pl.ANY),once((n,r,D),lambda i:(0,8,0))],
        out_specs=[tile(D),tile(D),tile(D),tile(FF),tile(FF),tile(D),pl.BlockSpec((BM,D),lambda i:(i,3)),tile(D),pl.BlockSpec((16,D),lambda i:(0,0))],
        out_shape=[sd((rows,D),bf),sd((rows,D),bf),sd((rows,D),bf),sd((rows,FF),bf),sd((rows,FF),bf),sd((rows,D),f32),sd((rows,4*D),bf),sd((rows,D),bf),sd((16,D),f32)],
        scratch_shapes=[pltpu.VMEM((BM,D),f32)]*5+[pltpu.VMEM((BM,CH),f32)]*4+[pltpu.VMEM((4,n,r,D),bf),pltpu.VMEM((n,4*r,D),bf),pltpu.SemaphoreType.DMA((5,))],
        compiler_params=params(),name="mlp_block",
        cost_estimate=pl.CostEstimate(flops=2*rows*D*(2*D+4*FF),bytes_accessed=48<<20,transcendentals=0))(x,o,dy,vec,packed,packed)


def fc_kernel(z_ref,dm_ref,h_ref,du_ref,g_ref,down,up,sems):
    i=pl.program_id(0)
    per,r=down.shape[2],up.shape[2]
    n=down.shape[1]
    def down_copy(k):
        return pltpu.make_async_copy(down.at[k],g_ref.at[pl.ds(pl.multiple_of(k*n,n),n),0:per],sems.at[k])
    def up_copy(k):
        return pltpu.make_async_copy(up.at[k],g_ref.at[:,pl.ds(pl.multiple_of(per+k*r,r),r)],sems.at[4+k])
    @pl.when(i<4)
    def _():
        down[i]=tn(z_ref[...],dm_ref[...]).reshape(down.shape[1:]).astype(bf)
        down_copy(i).start()
    @pl.when(i>=4)
    def _():
        up[i-4]=tn(h_ref[...],du_ref[...]).reshape(up.shape[1:]).astype(bf)
        up_copy(i-4).start()
    @pl.when(i==7)
    def _():
        for k in range(4):
            down_copy(k).wait()
            up_copy(k).wait()


def fc_grads(z,dm,h,du):
    rows=z.shape[0]
    per,r=FF//PACK,D//PACK
    return pl.pallas_call(fc_kernel,grid=(8,),
        in_specs=[pl.BlockSpec((rows,D),lambda i:(0,jnp.minimum(i,3))),once((rows,D)),once((rows,D)),
            pl.BlockSpec((rows,D),lambda i:(0,jnp.maximum(i-4,0)))],
        out_specs=pl.BlockSpec(memory_space=pl.ANY),
        out_shape=jax.ShapeDtypeStruct((PACK,2*per,D),bf),
        scratch_shapes=[pltpu.VMEM((4,PACK//4,per,D),bf),pltpu.VMEM((4,PACK,r,D),bf),pltpu.SemaphoreType.DMA((8,))],
        compiler_params=params(),name="fc_grads",
        cost_estimate=pl.CostEstimate(flops=4*rows*D*FF,bytes_accessed=36<<20,transcendentals=0))(z,dm,h,du)


def split_kernel(core_ref,left_ref,right_ref,*refs):
    sum_ref,(mine_ref,other_ref)=refs[:-2],refs[-2:]
    i=pl.program_id(0)
    even=core_ref[0]==0
    def put(v,cols):
        v=v.reshape(mine_ref.shape[0],2,mine_ref.shape[1],v.shape[1])
        mine_ref[:,:,cols]=jnp.where(even,v[:,0],v[:,1]).astype(bf)
        other_ref[:,:,cols]=jnp.where(even,v[:,1],v[:,0]).astype(bf)
    if sum_ref:
        @pl.when(i==0)
        def _():
            sums=jnp.concatenate([sum_ref[0][...],jnp.zeros((112,D),f32)],axis=0)
            put(sums.T,slice(2*D,2*D+128))
    put(tn(left_ref[...],right_ref[...]),pl.ds(pl.multiple_of(i*D,D),D))


def split_grad(core,left,right,sums=None):
    rows=left.shape[0]
    more=[] if sums is None else [sums]
    index=(lambda i:(0,1-i),lambda i:(0,3-3*i)) if sums is None else (lambda i:(0,0),lambda i:(0,1+i))
    shape=(PACK//2,D//PACK,2*D+128*len(more))
    out=pl.BlockSpec(memory_space=pltpu.VMEM)
    return pl.pallas_call(split_kernel,grid=(2,),
        in_specs=[pl.BlockSpec(memory_space=pltpu.SMEM)]+[pl.BlockSpec((rows,D),f) for f in index]+[once((16,D))]*len(more),
        out_specs=[out,out],
        out_shape=[jax.ShapeDtypeStruct(shape,bf)]*2,
        compiler_params=pltpu.CompilerParams(vmem_limit_bytes=48<<20),name="split_grad",
        cost_estimate=pl.CostEstimate(flops=1000,bytes_accessed=1000,transcendentals=0))(core,left,right,*more)


def input_kernel(n_ref,r_ref,d_ref,dx1_ref,vec_ref,old_ref,w_ref,gx_ref,sum_ref):
    @pl.when(pl.program_id(0)==0)
    def _():
        sum_ref[...]=old_ref[...]
    def add(i,v):
        sum_ref[i:i+1,:]+=v
    d=d_ref[...]
    dh=nt(d,w_ref[...].reshape(D,3*D))
    total=jnp.sum(d.astype(f32),axis=0,keepdims=True)
    n=n_ref[...]; r=r_ref[:,0:1]
    add(0,jnp.sum(dh*n,axis=0,keepdims=True))
    add(1,jnp.sum(dh,axis=0,keepdims=True))
    for i,b in ((2,0),(3,2)):
        add(i,jnp.concatenate([total[:,384*p+128*b:384*p+128*b+128] for p in range(6)],axis=1))
    t=dh*vec_ref[0:1,:]
    dx=dx1_ref[...]+r*(t-jnp.mean(t,axis=1,keepdims=True)-n*jnp.mean(t*n,axis=1,keepdims=True))
    gx_ref[...]=dx.astype(bf)


def input_grad(n,r,d,dx1,vec,sums,w):
    rows=n.shape[0]
    return pl.pallas_call(input_kernel,grid=(rows//BM,),
        in_specs=[tile(D),tile(128),tile(3*D),tile(D),once((16,D)),once((16,D)),once(w.shape[:-1]+(3*D,),lambda i:(0,)*len(w.shape))],
        out_specs=[tile(D),pl.BlockSpec((16,D),lambda i:(0,0))],
        out_shape=[jax.ShapeDtypeStruct((rows,D),bf),jax.ShapeDtypeStruct((16,D),f32)],
        compiler_params=params(),name="input_grad",
        cost_estimate=pl.CostEstimate(flops=1000,bytes_accessed=1000,transcendentals=0))(n,r,d,dx1,vec,sums,w)


def stage_kernel(count,place_ref,*refs):
    ins,outs=refs[:count],refs[count:]
    for k,out in enumerate(outs):
        at=place_ref[0]^k
        out[...]=sum(ref[at].astype(f32) for ref in ins).astype(bf)


def stage_sum(place,parts):
    shape=parts[0].shape
    near=pl.BlockSpec(memory_space=pltpu.VMEM)
    return pl.pallas_call(functools.partial(stage_kernel,len(parts)),
        in_specs=[pl.BlockSpec(memory_space=pltpu.SMEM)]+[near]*len(parts),
        out_specs=[near]*4,
        out_shape=[jax.ShapeDtypeStruct(shape[1:],bf)]*4,
        compiler_params=pltpu.CompilerParams(vmem_limit_bytes=16<<20),name="stage_sum",
        cost_estimate=pl.CostEstimate(flops=1000,bytes_accessed=1000,transcendentals=0))(place,*parts)


def finish_kernel(*refs):
    first,second,(rest_ref,qkv_ref,proj_ref,fc1_ref,fc2_ref,vec_ref,square_ref)=refs[:4],refs[4:8],refs[8:]
    a=sum(ref[...].astype(f32) for ref in first)
    b=sum(ref[...].astype(f32) for ref in second)
    rest=rest_ref[...].astype(f32)
    total=jnp.sum(a*a,keepdims=True)+jnp.sum(b*b,keepdims=True)+jnp.sum(rest*rest,keepdims=True)
    square_ref[...]=jnp.broadcast_to(total,square_ref.shape)
    r=a.shape[0]
    proj_ref[...]=a[:,0:D]
    for p in range(6):
        for part in range(3):
            at=384*p+128*part
            qkv_ref[:,D*part+128*p:D*part+128*p+128]=a[:,D+at:D+at+128] if p<2 else b[:,at-D:at-D+128]
    vec_ref[...]=b[:,2*D:2*D+128].T
    fc2_ref[...]=rest[0:4*r]
    for c in range(4):
        fc1_ref[:,D*c:D*c+D]=rest[(4+c)*r:(5+c)*r]


def finish_sum(first,second,rest):
    near=pl.BlockSpec(memory_space=pltpu.VMEM)
    r=rest.shape[0]//8
    shapes=[(r,3*D),(r,D),(r,FF),(4*r,D),(128,r),(PACK,128)]
    return pl.pallas_call(finish_kernel,grid=(1,),
        in_specs=[near]*9,
        out_specs=[pl.BlockSpec(v,lambda i:(0,0)) for v in shapes[:5]]+[near],
        out_shape=[jax.ShapeDtypeStruct(v,f32) for v in shapes],
        compiler_params=pltpu.CompilerParams(vmem_limit_bytes=58<<20),name="finish_sum",
        cost_estimate=pl.CostEstimate(flops=1000,bytes_accessed=1000,transcendentals=0))(*first,*second,rest)


RATES=((2.0/math.sqrt(D),0.04),(2.0/math.sqrt(D//48),0.04),(2.0/math.sqrt(D),0.04),(2.0/math.sqrt(FF),0.04),(1.0,0.0))


def adam_kernel(fix_ref,square_ref,*refs):
    grads,states,outs=refs[:5],refs[5:20],refs[20:]
    norm=jnp.sqrt(jnp.sum(square_ref[...],axis=0,keepdims=True)[:,0:1])
    outs[0][...]=norm
    factor=jnp.minimum(1.0,CLIP_LIMIT/(norm+1e-06))
    for k,(rate,decay) in enumerate(RATES):
        weight,first,second=(ref[...] for ref in states[3*k:3*k+3])
        grad=factor*grads[k][0:weight.shape[0],:]
        first=BETA_ONE*first+(1.0-BETA_ONE)*grad
        second=BETA_TWO*second+(1.0-BETA_TWO)*grad*grad
        stride=first/fix_ref[0]/(jnp.sqrt(second/fix_ref[1])+ADAM_EPS)
        outs[3*k+1][...]=weight-rate*(stride+decay*weight)
        outs[3*k+2][...]=first
        outs[3*k+3][...]=second


def adam_all(fix,squares,grads,states):
    whole=lambda v: pl.BlockSpec(v,lambda i:(0,0))
    shapes=[(1,1)]+[v.shape for v in states]
    return pl.pallas_call(adam_kernel,grid=(1,),
        in_specs=[pl.BlockSpec(memory_space=pltpu.SMEM)]+[whole(v.shape) for v in (squares,*grads,*states)],
        out_specs=[whole(v) for v in shapes],
        out_shape=[jax.ShapeDtypeStruct(v,f32) for v in shapes],
        compiler_params=params(),name="adam_all")(fix,squares,*grads,*states)


def pack_rows(full):
    k = full.shape[1] // D
    return full.reshape(PACK, D // PACK, k, D).transpose(0, 2, 1, 3).reshape(PACK, -1, D)


def unpack_rows(packed):
    k = packed.shape[1] * PACK // D
    return packed.reshape(PACK, k, D // PACK, D).transpose(0, 2, 1, 3).reshape(D, k * D)


def swap(value, axis, size, flip):
    return lax.ppermute(value, axis, [(i, i ^ flip) for i in range(size)])


def places():
    inner = lax.axis_index("fsdp")
    return (lax.axis_index("dp"), inner // 2, inner % 2)


def first_stage(me, mine, other):
    got = swap(other, "fsdp", 8, 1)
    shape = (4, 4) + mine.shape[1:]
    return stage_sum(me, [mine.reshape(shape), got.reshape(shape)])


def second_stage(me, parts):
    keep, *send = parts
    return stage_sum(me, [keep] + [swap(v, "dp", 4, k + 1) for k, v in enumerate(send)])


def third_stage(parts):
    keep, *send = parts
    return [keep] + [swap(v, "fsdp", 8, 2 * k + 2) for k, v in enumerate(send)]


def to_pairs(w):
    return w.reshape(-1, 3, 6, 128).transpose(0, 2, 1, 3).reshape(-1, 3 * D)


def from_pairs(w):
    return w.reshape(-1, 6, 3, 128).transpose(0, 2, 1, 3).reshape(-1, 3 * D)


def make_local(fast):
    def gather(shard):
        return lax.all_gather(shard, AXES, axis=0, tiled=True)

    def scatter(full):
        return lax.psum_scatter(full, AXES, scatter_dimension=0, tiled=True)

    def local(
        tokens,
        cotangent,
        lengths,
        step,
        weight_qkv,
        weight_proj,
        weight_fc1,
        weight_fc2,
        vectors,
        first_qkv,
        second_qkv,
        first_proj,
        second_proj,
        first_fc1,
        second_fc1,
        first_fc2,
        second_fc2,
        first_vectors,
        second_vectors,
    ):
        per = weight_qkv.shape[0]
        cols = vectors.shape[1]
        rows_dev, row, _ = tokens.shape
        count = rows_dev * row
        inputs = tokens.reshape(count, D)
        centered, spread = norm_input(inputs)
        if fast:
            first, packed = pack_shards(weight_qkv, weight_proj, weight_fc1, weight_fc2, vectors)
            rest = lax.all_gather(packed, AXES, axis=0, tiled=False)
            along = jnp.stack([first] + [swap(first, "fsdp", 8, 2 * k) for k in (1, 2, 3)])
            parts = [along] + [swap(along, "dp", 4, k) for k in (1, 2, 3)]
            far = parts.pop()
            parts = [parts, [swap(v, "fsdp", 8, 1) for v in parts]]
            far, parts, centered, spread = lax.optimization_barrier((far, parts, centered, spread))
            parts = parts[0] + [far] + parts[1] + [swap(far, "fsdp", 8, 1)]
            place = jnp.stack(places()).astype(jnp.int32)
        else:
            low = [w.astype(bf) for w in (weight_qkv, weight_proj, weight_fc1, weight_fc2, vectors)]
            first = jnp.concatenate([to_pairs(low[0]), jnp.pad(low[4], ((0, 0), (0, 128 - cols)))], axis=1)
            whole = gather(first).reshape(4, 4, 2, D // PACK, WIDE)
            parts = [whole[k, :, c] for c in range(2) for k in range(4)]
            place = jnp.zeros((3,), jnp.int32)
            full = [gather(w) for w in low[1:4]]
            rest = jnp.concatenate(
                [full[2].reshape(PACK, FF // PACK, D), pack_rows(full[1]), pack_rows(full[0])], axis=1
            )
        left, qkv, vec, mats_qkv = qkv_forward(place, centered, parts)
        each = lambda v, b: v[b * row : (b + 1) * row]
        done = [attn_fwd(lengths[b : b + 1], each(qkv, b), each(left, b)) for b in range(rows_dev)]
        left = jnp.concatenate([v for v, _ in done], axis=0)
        result, normed_two, grad_down, active, grad_inner, grad_middle, right, grad_mixed, sums = mlp_block(
            inputs, left, cotangent.reshape(count, D), vec, rest
        )
        grads = fc_grads(active, grad_down, normed_two, grad_inner)
        if fast:
            rest_owned = lax.psum_scatter(grads, AXES, scatter_dimension=0, tiled=False)
        right = jnp.concatenate(
            [
                attn_bwd(
                    lengths[b : b + 1], each(qkv, b), each(left, b), each(grad_mixed, b), done[b][1], each(right, b)
                )
                for b in range(rows_dev)
            ],
            axis=0,
        )
        core = place[2:]
        mine_a, other_a = split_grad(core, left, right)
        if fast:
            me_dp, me_z = place[0:1], place[1:2]
            stage_a = first_stage(me_dp, mine_a, other_a)
            *stage_a, vec = lax.optimization_barrier((*stage_a, vec))
        grad_inputs, sums = input_grad(centered, spread, right, grad_middle, vec, sums, mats_qkv)
        if fast:
            stage_a = second_stage(me_z, stage_a)
            *stage_a, sums = lax.optimization_barrier((*stage_a, sums))
            owned_a = third_stage(stage_a)
            mine_b, other_b = split_grad(core, left, right, sums)
            *owned_a, other_b = lax.optimization_barrier((*owned_a, other_b))
            owned_b = third_stage(second_stage(me_z, first_stage(me_dp, mine_b, other_b)))
            *owned, squares = finish_sum(owned_a, owned_b, rest_owned)
            squares = lax.all_to_all(squares, AXES, 0, 0, tiled=True)
        else:
            mine_b, other_b = split_grad(core, left, right, sums)
            wide = FF // PACK
            part_a = jnp.stack([mine_a, other_a], axis=1).reshape(D, 2 * D)
            part_b = jnp.stack([mine_b, other_b], axis=1).reshape(D, 2 * D + 128)
            owned = [
                scatter(from_pairs(jnp.concatenate([part_a[:, D:], part_b[:, : 2 * D]], axis=1))),
                scatter(part_a[:, :D]),
                scatter(unpack_rows(grads[:, wide:])),
                scatter(grads[:, :wide].reshape(FF, D)),
                scatter(part_b[:, 2 * D : 2 * D + cols]),
            ]
            owned = [g.astype(f32) for g in owned]
            squares = jnp.full((1, 128), lax.psum(sum(jnp.sum(g * g) for g in owned), AXES))
            owned[4] = owned[4].T
        taken = step[0].astype(f32)
        fix = jnp.stack([1.0 - jnp.power(BETA_ONE, taken), 1.0 - jnp.power(BETA_TWO, taken)])
        states = (weight_qkv, first_qkv, second_qkv, weight_proj, first_proj, second_proj)
        states += (weight_fc1, first_fc1, second_fc1, weight_fc2, first_fc2, second_fc2)
        norm, *new = adam_all(fix, squares, owned, states + (vectors.T, first_vectors.T, second_vectors.T))
        new[12:] = [v.T for v in new[12:]]
        shape = (rows_dev, row, D)
        outs = [result.reshape(shape), grad_inputs.reshape(shape), norm.reshape(1)] + new[0::3]
        for k in range(5):
            outs += new[3 * k + 1 : 3 * k + 3]
        return tuple(outs)

    return local


def solution(mesh):
    rows = P(AXES, None)
    tokens = P(AXES, None, None)
    fast = (mesh.shape["dp"], mesh.shape["fsdp"]) == (4, 8)
    return jax.shard_map(
        make_local(fast),
        mesh=mesh,
        in_specs=(tokens, tokens, rows, P()) + (rows,) * 15,
        out_specs=(tokens, tokens, P()) + (rows,) * 15,
        check_vma=False,
    )
```

```python
import functools
import math

import jax
import jax.numpy as jnp
from jax import lax
from jax.experimental import pallas as pl
from jax.experimental.pallas import tpu as pltpu
from jax.sharding import PartitionSpec as P

D = 768
FF = 3072
NORM_EPS = 1e-06
BETA_ONE = 0.9
BETA_TWO = 0.999
ADAM_EPS = 1e-08
CLIP_LIMIT = 3.0
AXES = ("dp", "fsdp")
PACK = 32
bf = jnp.bfloat16
f32 = jnp.float32


def nt(a, b):
    return lax.dot_general(a, b, (((1,), (1,)), ((), ())), preferred_element_type=f32)


def nn(a, b):
    return jnp.dot(a, b, preferred_element_type=f32)


def tn(a, b):
    return lax.dot_general(a, b, (((0,), (0,)), ((), ())), preferred_element_type=f32)


ROW=1536
BQ=256
NQ=ROW//BQ
SEGS=6
LOG2E=1.4426950408889634
BIG=float(2**30)


def seg_onehot(len_ref):
    lane=lax.broadcasted_iota(jnp.int32,(1,128),1)
    start=jnp.zeros((1,128),jnp.int32); stop=jnp.zeros((1,128),jnp.int32)
    end=jnp.int32(0)
    for s in range(SEGS):
        start=jnp.where(lane==s,end,start)
        end=end+len_ref[0,s]
        stop=jnp.where(lane==s,end,stop)
    start=jnp.where(lane==SEGS,end,start)
    stop=jnp.where(lane==SEGS,ROW,stop)
    pos=lax.broadcasted_iota(jnp.int32,(ROW,128),0)
    return jnp.where((pos>=start)&(pos<stop),1.0,0.0)


def segments(len_ref,seg,mask):
    @pl.when(pl.program_id(0)==0)
    def _():
        oh=seg_onehot(len_ref)
        seg[...]=oh.astype(bf)
        mask[...]=((oh-1.0)*BIG).astype(bf)


def half(v,r):
    low=lax.broadcasted_iota(jnp.int32,v.shape,1)<64
    return jnp.where(low,v,jnp.zeros_like(v)) if r==0 else jnp.where(low,jnp.zeros_like(v),v)


MAIN=1376
CHUNKS=((0,256),(256,512),(512,768),(768,1024),(1024,MAIN))
LAST=slice(ROW-BQ,ROW)
TAIL=slice(MAIN,ROW)
EIGHTH=0.125


def tile_rows(j):
    return pl.ds(pl.multiple_of(j*BQ,BQ),BQ)


def fwd_kernel(len_ref,qkv_ref,left_ref,o_ref,lse_ref,seg,mask,va,vb,sa,sb,ma,mb,ot,last):
    segments(len_ref,seg,mask)
    q_ref,k_ref,v_ref=(qkv_ref.at[:,128*b:128*b+128] for b in range(3))
    def query(rows,r):
        return jnp.concatenate([half(q_ref[rows,:]*jnp.asarray(EIGHTH,bf),r),seg[rows,:]],axis=1)
    def keys(rows):
        return jnp.concatenate([k_ref[rows,:],mask[rows,:]],axis=1)
    vt=v_ref[...].T
    one=(lax.broadcasted_iota(jnp.int32,(16,ROW),0)==0).astype(bf)
    va[64:80,:]=one; vb[64:80,:]=one
    va[0:64,:]=vt[0:64,:]; vb[0:64,:]=vt[64:128,:]
    for r,v_sc in enumerate((va,vb)):
        s=nt(keys(TAIL),query(LAST,r))*LOG2E
        m=jnp.max(s,axis=0,keepdims=True)
        o=nn(v_sc[:,TAIL],jnp.exp2(s-m).astype(bf))
        last[72*r:72*r+64,:]=o[0:64,:]*(1.0/o[64:65,:])
        last[72*r+64:72*r+65,:]=m+jnp.log2(o[64:65,:])
    def first(rows,r,s_sc,m_sc):
        q=query(rows,r)
        m=None
        for lo,hi in CHUNKS:
            s=nt(keys(slice(lo,hi)),q)
            s_sc[lo:hi,:]=s
            t=jnp.max(s,axis=0,keepdims=True)
            m=t if m is None else jnp.maximum(m,t)
        m_sc[0:1,:]=m*LOG2E
    def step(s_sc,m_sc,v_sc,j,r,rows,r2,s_next,m_next):
        q=query(rows,r2)
        m=m_sc[0:1,:]
        top=None
        o=0.0
        for lo,hi in CHUNKS:
            s=nt(keys(slice(lo,hi)),q)
            s_next[lo:hi,:]=s
            t=jnp.max(s,axis=0,keepdims=True)
            top=t if top is None else jnp.maximum(top,t)
        m_next[0:1,:]=top*LOG2E
        for lo,hi in CHUNKS:
            o=o+nn(v_sc[:,lo:hi],jnp.exp2(s_sc[lo:hi,:]*LOG2E-m).astype(bf))
        l=o[64:65,:]
        cols=tile_rows(j)
        ot[64*r:64*r+64,cols]=o[0:64,:]*(1.0/l)
        lse_ref[0,r:r+1,cols]=m+jnp.log2(l)
    first(pl.ds(0,BQ),0,sa,ma)
    def body(j,c):
        step(sa,ma,va,j,0,tile_rows(j),1,sb,mb)
        step(sb,mb,vb,j,1,tile_rows(jnp.minimum(j+1,NQ-1)),0,sa,ma)
        return c
    lax.fori_loop(0,NQ,body,0)
    for r in range(2):
        old=lse_ref[0,r:r+1,LAST]
        lse=last[72*r+64:72*r+65,:]
        top=jnp.maximum(old,lse)
        a=jnp.exp2(old-top); b=jnp.exp2(lse-top); t=1.0/(a+b)
        ot[64*r:64*r+64,LAST]=ot[64*r:64*r+64,LAST]*(a*t)+last[72*r:72*r+64,:]*(b*t)
        lse_ref[0,r:r+1,LAST]=top-jnp.log2(t)
    o_ref[...]=ot[...].T.astype(bf)


def attn_fwd(lengths,qkv,left):
    blk=lambda width: pl.BlockSpec((ROW,width),lambda h:(0,h))
    return pl.pallas_call(fwd_kernel,grid=(6,),
        in_specs=[pl.BlockSpec(memory_space=pltpu.SMEM),blk(384),pl.BlockSpec(memory_space=pl.ANY)],
        out_specs=[pl.BlockSpec((ROW,128),lambda h:(0,6+h)),pl.BlockSpec((1,8,ROW),lambda h:(h,0,0))],
        out_shape=[jax.ShapeDtypeStruct((ROW,2*D),bf),jax.ShapeDtypeStruct((6,8,ROW),f32)],input_output_aliases={2:0},
        scratch_shapes=[pltpu.VMEM((ROW,128),bf)]*2+[pltpu.VMEM((80,ROW),bf)]*2+[pltpu.VMEM((MAIN,BQ),f32)]*2+[pltpu.VMEM((8,BQ),f32)]*2
          +[pltpu.VMEM((128,ROW),f32),pltpu.VMEM((144,BQ),f32)],
        compiler_params=pltpu.CompilerParams(vmem_limit_bytes=60<<20),name="attn_fwd",
        cost_estimate=pl.CostEstimate(flops=4*ROW*ROW*D,bytes_accessed=10<<20,transcendentals=12*ROW*ROW))(lengths,qkv,left)


def bwd_kernel(len_ref,qkv_ref,o_ref,do_ref,lse_ref,right_ref,d_ref,
               seg,mask,kt,xa,ya,xb,yb,dqt,dqe,dka,dva):
    segments(len_ref,seg,mask)
    q_ref,k_ref,v_ref=(qkv_ref.at[:,128*b:128*b+128] for b in range(3))
    kt[...]=k_ref[...].T
    def query(rows,r):
        return half(q_ref[rows,:]*jnp.asarray(EIGHTH,bf),r)
    def keys(rows):
        return jnp.concatenate([k_ref[rows,:],mask[rows,:]],axis=1)
    def rowsums(rows):
        t=(do_ref[rows,:].astype(f32)*o_ref[rows,:].astype(f32)).T
        return [jnp.sum(t[64*r:64*r+64],axis=0,keepdims=True) for r in range(2)]
    def products(rows,r,span,x,y):
        q=jnp.concatenate([query(rows,r),seg[rows,:]],axis=1); d=half(do_ref[rows,:],r)
        for lo,hi in span:
            x[lo:hi,:]=nt(keys(slice(lo,hi)),q)
            y[lo:hi,:]=nt(v_ref[lo:hi,:],d)
    def grads(x,y,lse,total):
        p=jnp.exp2(x*LOG2E-lse)
        return p.astype(bf),(p*(y-total)).astype(bf)
    sums=rowsums(LAST)
    dv=0.0; dk=0.0
    for r in range(2):
        q=query(LAST,r); d=half(do_ref[LAST,:],r)
        p,ds=grads(nt(keys(TAIL),jnp.concatenate([q,seg[LAST,:]],axis=1)),nt(v_ref[TAIL,:],d),lse_ref[0,r:r+1,LAST],sums[r])
        dv=dv+nn(p,d); dk=dk+nn(ds,q)
        dqe[64*r:64*r+64,:]=nn(kt[64*r:64*r+64,TAIL],ds)
    dva[TAIL,:]=dv; dka[TAIL,:]=dk
    dva[0:MAIN,:]=jnp.zeros((MAIN,128),f32); dka[0:MAIN,:]=jnp.zeros((MAIN,128),f32)
    def rest(x,y,r,rows,total):
        q=query(rows,r); d=half(do_ref[rows,:],r); lse=lse_ref[0,r:r+1,rows]
        dq=0.0
        for lo,hi in CHUNKS:
            p,ds=grads(x[lo:hi,:],y[lo:hi,:],lse,total)
            dva[lo:hi,:]+=nn(p,d)
            dka[lo:hi,:]+=nn(ds,q)
            dq=dq+nn(kt[64*r:64*r+64,lo:hi],ds)
        dqt[64*r:64*r+64,rows]=dq
    def body(j,c):
        rows=tile_rows(j)
        sums=rowsums(rows)
        products(rows,0,CHUNKS,xa,ya)
        products(rows,1,CHUNKS,xb,yb)
        rest(xa,ya,0,rows,sums[0])
        rest(xb,yb,1,rows,sums[1])
        return c
    lax.fori_loop(0,NQ,body,0)
    dqt[:,LAST]+=dqe[...]
    d_ref[:,0:128]=(dqt[...].T*EIGHTH).astype(bf)
    d_ref[:,128:256]=dka[...].astype(bf)
    d_ref[:,256:384]=dva[...].astype(bf)


def attn_bwd(lengths,qkv,left,do,lse,right):
    blk=lambda width: pl.BlockSpec((ROW,width),lambda h:(0,h))
    return pl.pallas_call(bwd_kernel,grid=(6,),
        in_specs=[pl.BlockSpec(memory_space=pltpu.SMEM),blk(384),pl.BlockSpec((ROW,128),lambda h:(0,6+h)),blk(128),pl.BlockSpec((1,8,ROW),lambda h:(h,0,0)),pl.BlockSpec(memory_space=pl.ANY)],
        out_specs=blk(384),
        out_shape=jax.ShapeDtypeStruct((ROW,4*D),bf),input_output_aliases={5:0},
        scratch_shapes=[pltpu.VMEM((ROW,128),bf)]*2+[pltpu.VMEM((128,ROW),bf)]+[pltpu.VMEM((MAIN,BQ),f32)]*4
          +[pltpu.VMEM((128,ROW),f32),pltpu.VMEM((128,BQ),f32)]+[pltpu.VMEM((ROW,128),f32)]*2,
        compiler_params=pltpu.CompilerParams(vmem_limit_bytes=62<<20),name="attn_bwd",
        cost_estimate=pl.CostEstimate(flops=10*ROW*ROW*D,bytes_accessed=20<<20,transcendentals=12*ROW*ROW))(lengths,qkv,left,do,lse,right)


BM=512
INV_SQRT2=0.7071067811865476
INV_SQRT_2PI=0.3989422804014327
VMEM_CAP=62<<20


def norm_stats(v):
    center=v-jnp.mean(v,axis=1,keepdims=True)
    rstd=lax.rsqrt(jnp.mean(center*center,axis=1,keepdims=True)+NORM_EPS)
    return center*rstd,rstd


def params(**kw):
    return pltpu.CompilerParams(vmem_limit_bytes=VMEM_CAP,**kw)


def once(shape,index=None):
    return pl.BlockSpec(shape,index or (lambda i:(0,)*len(shape)),pipeline_mode=pl.Buffered(1))


def tile(width):
    return pl.BlockSpec((BM,width),lambda i:(i,0))


WIDE=3*D+128


def norm_kernel(x_ref,n_ref,r_ref):
    n,r=norm_stats(x_ref[...].astype(f32))
    n_ref[...]=n
    r_ref[...]=jnp.broadcast_to(r,r_ref.shape)


def norm_input(x):
    rows=x.shape[0]
    return pl.pallas_call(norm_kernel,grid=(rows//BM,),
        in_specs=[tile(D)],out_specs=[tile(D),tile(128)],
        out_shape=[jax.ShapeDtypeStruct((rows,D),f32),jax.ShapeDtypeStruct((rows,128),f32)],
        compiler_params=params(),name="norm_input",
        cost_estimate=pl.CostEstimate(flops=1000,bytes_accessed=1000,transcendentals=0))(x)


def pack_kernel(qkv_ref,proj_ref,fc1_ref,fc2_ref,vec_ref,first_ref,rest_ref):
    r=qkv_ref.shape[0]
    for p in range(6):
        for part in range(3):
            at=384*p+128*part
            first_ref[:,at:at+128]=qkv_ref[:,D*part+128*p:D*part+128*p+128].astype(bf)
    vec=vec_ref[...]
    vec=jnp.concatenate([vec,jnp.zeros((128-vec.shape[0],r),f32)],axis=0)
    first_ref[:,3*D:WIDE]=vec.T.astype(bf)
    rest_ref[0:4*r,:]=fc2_ref[...].astype(bf)
    for c in range(4):
        rest_ref[(4+c)*r:(5+c)*r,:]=fc1_ref[:,D*c:D*c+D].astype(bf)
    rest_ref[8*r:9*r,:]=proj_ref[...].astype(bf)


def pack_shards(qkv,proj,fc1,fc2,vectors):
    r=qkv.shape[0]
    ins=(qkv,proj,fc1,fc2,vectors.T)
    shapes=[(r,WIDE),(9*r,D)]
    whole=lambda s: pl.BlockSpec(s,lambda i:(0,)*len(s))
    return pl.pallas_call(pack_kernel,grid=(1,),
        in_specs=[whole(v.shape) for v in ins],out_specs=[pl.BlockSpec(memory_space=pltpu.VMEM),whole(shapes[1])],
        out_shape=[jax.ShapeDtypeStruct(v,bf) for v in shapes],
        compiler_params=pltpu.CompilerParams(vmem_limit_bytes=48<<20),name="pack_shards")(*ins)


def qkv_kernel(place_ref,n_ref,*refs):
    parts,(left_ref,qkv_ref,vec_ref,w_ref,w,sems,out_sem)=refs[:8],refs[8:]
    step=pl.program_id(0)
    keep=pltpu.make_async_copy(w,w_ref,out_sem)
    @pl.when(step==0)
    def _():
        copies=[]
        for i,part in enumerate(parts):
            core,dp=place_ref[2]^(i//4),place_ref[0]^(i%4)
            for k in range(4):
                copies.append(pltpu.make_async_copy(part.at[k],w.at[dp,place_ref[1]^k,core],sems.at[4*i+k]))
        for copy in copies:
            copy.start()
        for copy in copies:
            copy.wait()
        keep.start()
        vec_ref[...]=w[:,:,:,:,3*D:WIDE].reshape(D,128).astype(f32).T[0:16]
    h=(n_ref[...]*vec_ref[0:1,:]+vec_ref[1:2,:]).astype(bf)
    left_ref[...]=h
    zero=jnp.zeros((1,128),f32)
    bias=jnp.concatenate([b for p in range(6) for b in (vec_ref[2:3,128*p:128*p+128],zero,vec_ref[3:4,128*p:128*p+128])],axis=1)
    qkv_ref[...]=(nn(h,w[:,:,:,:,0:3*D].reshape(D,3*D))+bias).astype(bf)
    @pl.when(step==pl.num_programs(0)-1)
    def _():
        keep.wait()


def qkv_forward(place,n,parts):
    rows=n.shape[0]
    sd=jax.ShapeDtypeStruct
    wide=(4,4,2,D//PACK,WIDE)
    return pl.pallas_call(qkv_kernel,grid=(rows//BM,),
        in_specs=[pl.BlockSpec(memory_space=pltpu.SMEM),tile(D)]+[pl.BlockSpec(memory_space=pl.ANY)]*8,
        out_specs=[tile(D),tile(3*D),pl.BlockSpec((16,D),lambda i:(0,0)),pl.BlockSpec(memory_space=pl.ANY)],
        out_shape=[sd((rows,2*D),bf),sd((rows,3*D),bf),sd((16,D),f32),sd(wide,bf)],
        scratch_shapes=[pltpu.VMEM(wide,bf),pltpu.SemaphoreType.DMA((32,)),pltpu.SemaphoreType.DMA],
        compiler_params=params(),name="qkv_forward",
        cost_estimate=pl.CostEstimate(flops=2*rows*D*3*D,bytes_accessed=18<<20,transcendentals=0))(place,n,*parts)


CH=768


def mlp_kernel(x_ref,o_ref,dy_ref,vec_ref,rest_ref,wp_ref,
               out_ref,h_ref,dm_ref,z_ref,du_ref,dx_ref,da_ref,do_ref,sum_ref,
               a_s,x1_s,n2_s,mo_s,dh_s,ua,ub,ga,gb,w1_s,w2_s,sems):
    step=pl.program_id(0)
    r=wp_ref.shape[1]
    copies=[pltpu.make_async_copy(rest_ref.at[:,0:4*r],w2_s,sems.at[4])]
    copies+=[pltpu.make_async_copy(rest_ref.at[:,(4+b)*r:(5+b)*r],w1_s.at[b],sems.at[b]) for b in range(4)]
    @pl.when(step==0)
    def _():
        for copy in copies:
            copy.start()
        sum_ref[...]=jnp.zeros_like(sum_ref)
    row=lambda i: vec_ref[i:i+1,:]
    def add(i,v):
        sum_ref[i:i+1,:]+=jnp.sum(v,axis=0,keepdims=True)
    wp=wp_ref[...].reshape(D,D)
    a=nn(o_ref[...],wp)+row(4)
    a_s[...]=a
    x1=x_ref[...].astype(f32)+row(5)*a
    x1_s[...]=x1
    n2,r2=norm_stats(x1)
    n2_s[...]=n2
    h=(n2*row(6)+row(7)).astype(bf)
    h_ref[...]=h
    dm=(row(13)*dy_ref[...].astype(f32)).astype(bf)
    dm_ref[...]=dm
    add(12,dm.astype(f32))
    mo_s[...]=jnp.zeros_like(mo_s)
    dh_s[...]=jnp.zeros_like(dh_s)
    def w2(c):
        return w2_s[pl.ds(8*c,8)].reshape(D,D)
    @pl.when(step==0)
    def _():
        for copy in copies:
            copy.wait()
    def up(c,u,g):
        u[...]=nn(h_ref[...],w1_s[c].reshape(D,D))
        g[...]=nt(dm_ref[...],w2(c))
    def down(c,u,g):
        cols=pl.ds(pl.multiple_of(c*CH,CH),CH)
        v=u[...]+vec_ref[pl.ds(8+c,1),:]
        cdf=0.5+0.5*lax.erf(v*INV_SQRT2)
        z=(v*cdf).astype(bf)
        z_ref[:,cols]=z
        slope=cdf+v*(INV_SQRT_2PI*jnp.exp(v*v*(-0.5)))
        du=(g[...]*slope).astype(bf)
        du_ref[:,cols]=du
        sum_ref[pl.ds(8+c,1),:]+=jnp.sum(du.astype(f32),axis=0,keepdims=True)
        mo_s[...]+=nn(z,w2(c))
        dh_s[...]+=nt(du,w1_s[c].reshape(D,D))
    def body(i,carry):
        up(2*i,ua,ga)
        up(2*i+1,ub,gb)
        down(2*i,ua,ga)
        down(2*i+1,ub,gb)
        return carry
    lax.fori_loop(0,FF//CH//2,body,0)
    mo=mo_s[...]+row(12)
    out_ref[...]=(x1_s[...]+row(13)*mo).astype(bf)
    dy=dy_ref[...].astype(f32)
    add(13,dy*mo)
    dh=dh_s[...]; n2=n2_s[...]
    add(6,dh*n2); add(7,dh)
    t=dh*row(6)
    dx=dy+r2*(t-jnp.mean(t,axis=1,keepdims=True)-n2*jnp.mean(t*n2,axis=1,keepdims=True))
    dx_ref[...]=dx
    add(5,dx*a_s[...])
    da=(row(5)*dx).astype(bf)
    da_ref[...]=da
    add(4,da.astype(f32))
    do_ref[...]=nt(da,wp_ref[...].reshape(D,D)).astype(bf)


def mlp_block(x,o,dy,vec,packed):
    rows=x.shape[0]
    n,r=packed.shape[0],D//packed.shape[0]
    sd=jax.ShapeDtypeStruct
    return pl.pallas_call(mlp_kernel,grid=(rows//BM,),
        in_specs=[tile(D),pl.BlockSpec((BM,D),lambda i:(i,1)),tile(D),once((16,D)),pl.BlockSpec(memory_space=pl.ANY),once((n,r,D),lambda i:(0,8,0))],
        out_specs=[tile(D),tile(D),tile(D),tile(FF),tile(FF),tile(D),pl.BlockSpec((BM,D),lambda i:(i,3)),tile(D),pl.BlockSpec((16,D),lambda i:(0,0))],
        out_shape=[sd((rows,D),bf),sd((rows,D),bf),sd((rows,D),bf),sd((rows,FF),bf),sd((rows,FF),bf),sd((rows,D),f32),sd((rows,4*D),bf),sd((rows,D),bf),sd((16,D),f32)],
        scratch_shapes=[pltpu.VMEM((BM,D),f32)]*5+[pltpu.VMEM((BM,CH),f32)]*4+[pltpu.VMEM((4,n,r,D),bf),pltpu.VMEM((n,4*r,D),bf),pltpu.SemaphoreType.DMA((5,))],
        compiler_params=params(),name="mlp_block",
        cost_estimate=pl.CostEstimate(flops=2*rows*D*(2*D+4*FF),bytes_accessed=48<<20,transcendentals=0))(x,o,dy,vec,packed,packed)


def fc_kernel(z_ref,dm_ref,h_ref,du_ref,g_ref,down,up,sems):
    i=pl.program_id(0)
    per,r=down.shape[2],up.shape[2]
    n=down.shape[1]
    def down_copy(k):
        return pltpu.make_async_copy(down.at[k],g_ref.at[pl.ds(pl.multiple_of(k*n,n),n),0:per],sems.at[k])
    def up_copy(k):
        return pltpu.make_async_copy(up.at[k],g_ref.at[:,pl.ds(pl.multiple_of(per+k*r,r),r)],sems.at[4+k])
    @pl.when(i<4)
    def _():
        down[i]=tn(z_ref[...],dm_ref[...]).reshape(down.shape[1:]).astype(bf)
        down_copy(i).start()
    @pl.when(i>=4)
    def _():
        up[i-4]=tn(h_ref[...],du_ref[...]).reshape(up.shape[1:]).astype(bf)
        up_copy(i-4).start()
    @pl.when(i==7)
    def _():
        for k in range(4):
            down_copy(k).wait()
            up_copy(k).wait()


def fc_grads(z,dm,h,du):
    rows=z.shape[0]
    per,r=FF//PACK,D//PACK
    return pl.pallas_call(fc_kernel,grid=(8,),
        in_specs=[pl.BlockSpec((rows,D),lambda i:(0,jnp.minimum(i,3))),once((rows,D)),once((rows,D)),
            pl.BlockSpec((rows,D),lambda i:(0,jnp.maximum(i-4,0)))],
        out_specs=pl.BlockSpec(memory_space=pl.ANY),
        out_shape=jax.ShapeDtypeStruct((PACK,2*per,D),bf),
        scratch_shapes=[pltpu.VMEM((4,PACK//4,per,D),bf),pltpu.VMEM((4,PACK,r,D),bf),pltpu.SemaphoreType.DMA((8,))],
        compiler_params=params(),name="fc_grads",
        cost_estimate=pl.CostEstimate(flops=4*rows*D*FF,bytes_accessed=36<<20,transcendentals=0))(z,dm,h,du)


def split_kernel(core_ref,left_ref,right_ref,*refs):
    sum_ref,(mine_ref,other_ref)=refs[:-2],refs[-2:]
    i=pl.program_id(0)
    even=core_ref[0]==0
    def put(v,cols):
        v=v.reshape(mine_ref.shape[0],2,mine_ref.shape[1],v.shape[1])
        mine_ref[:,:,cols]=jnp.where(even,v[:,0],v[:,1]).astype(bf)
        other_ref[:,:,cols]=jnp.where(even,v[:,1],v[:,0]).astype(bf)
    if sum_ref:
        @pl.when(i==0)
        def _():
            sums=jnp.concatenate([sum_ref[0][...],jnp.zeros((112,D),f32)],axis=0)
            put(sums.T,slice(2*D,2*D+128))
    put(tn(left_ref[...],right_ref[...]),pl.ds(pl.multiple_of(i*D,D),D))


def split_grad(core,left,right,sums=None):
    rows=left.shape[0]
    more=[] if sums is None else [sums]
    index=(lambda i:(0,1-i),lambda i:(0,3-3*i)) if sums is None else (lambda i:(0,0),lambda i:(0,1+i))
    shape=(PACK//2,D//PACK,2*D+128*len(more))
    out=pl.BlockSpec(memory_space=pltpu.VMEM)
    return pl.pallas_call(split_kernel,grid=(2,),
        in_specs=[pl.BlockSpec(memory_space=pltpu.SMEM)]+[pl.BlockSpec((rows,D),f) for f in index]+[once((16,D))]*len(more),
        out_specs=[out,out],
        out_shape=[jax.ShapeDtypeStruct(shape,bf)]*2,
        compiler_params=pltpu.CompilerParams(vmem_limit_bytes=48<<20),name="split_grad",
        cost_estimate=pl.CostEstimate(flops=1000,bytes_accessed=1000,transcendentals=0))(core,left,right,*more)


def input_kernel(n_ref,r_ref,d_ref,dx1_ref,vec_ref,old_ref,w_ref,gx_ref,sum_ref):
    @pl.when(pl.program_id(0)==0)
    def _():
        sum_ref[...]=old_ref[...]
    def add(i,v):
        sum_ref[i:i+1,:]+=v
    d=d_ref[...]
    dh=nt(d,w_ref[...].reshape(D,3*D))
    total=jnp.sum(d.astype(f32),axis=0,keepdims=True)
    n=n_ref[...]; r=r_ref[:,0:1]
    add(0,jnp.sum(dh*n,axis=0,keepdims=True))
    add(1,jnp.sum(dh,axis=0,keepdims=True))
    for i,b in ((2,0),(3,2)):
        add(i,jnp.concatenate([total[:,384*p+128*b:384*p+128*b+128] for p in range(6)],axis=1))
    t=dh*vec_ref[0:1,:]
    dx=dx1_ref[...]+r*(t-jnp.mean(t,axis=1,keepdims=True)-n*jnp.mean(t*n,axis=1,keepdims=True))
    gx_ref[...]=dx.astype(bf)


def input_grad(n,r,d,dx1,vec,sums,w):
    rows=n.shape[0]
    return pl.pallas_call(input_kernel,grid=(rows//BM,),
        in_specs=[tile(D),tile(128),tile(3*D),tile(D),once((16,D)),once((16,D)),once(w.shape[:-1]+(3*D,),lambda i:(0,)*len(w.shape))],
        out_specs=[tile(D),pl.BlockSpec((16,D),lambda i:(0,0))],
        out_shape=[jax.ShapeDtypeStruct((rows,D),bf),jax.ShapeDtypeStruct((16,D),f32)],
        compiler_params=params(),name="input_grad",
        cost_estimate=pl.CostEstimate(flops=1000,bytes_accessed=1000,transcendentals=0))(n,r,d,dx1,vec,sums,w)


def stage_kernel(count,place_ref,*refs):
    ins,outs=refs[:count],refs[count:]
    for k,out in enumerate(outs):
        at=place_ref[0]^k
        out[...]=sum(ref[at].astype(f32) for ref in ins).astype(bf)


def stage_sum(place,parts):
    shape=parts[0].shape
    near=pl.BlockSpec(memory_space=pltpu.VMEM)
    return pl.pallas_call(functools.partial(stage_kernel,len(parts)),
        in_specs=[pl.BlockSpec(memory_space=pltpu.SMEM)]+[near]*len(parts),
        out_specs=[near]*4,
        out_shape=[jax.ShapeDtypeStruct(shape[1:],bf)]*4,
        compiler_params=pltpu.CompilerParams(vmem_limit_bytes=16<<20),name="stage_sum",
        cost_estimate=pl.CostEstimate(flops=1000,bytes_accessed=1000,transcendentals=0))(place,*parts)


def finish_kernel(*refs):
    first,second,(rest_ref,qkv_ref,proj_ref,fc1_ref,fc2_ref,vec_ref,square_ref)=refs[:4],refs[4:8],refs[8:]
    a=sum(ref[...].astype(f32) for ref in first)
    b=sum(ref[...].astype(f32) for ref in second)
    rest=rest_ref[...].astype(f32)
    total=jnp.sum(a*a,keepdims=True)+jnp.sum(b*b,keepdims=True)+jnp.sum(rest*rest,keepdims=True)
    square_ref[...]=jnp.broadcast_to(total,square_ref.shape)
    r=a.shape[0]
    proj_ref[...]=a[:,0:D]
    for p in range(6):
        for part in range(3):
            at=384*p+128*part
            qkv_ref[:,D*part+128*p:D*part+128*p+128]=a[:,D+at:D+at+128] if p<2 else b[:,at-D:at-D+128]
    vec_ref[...]=b[:,2*D:2*D+128].T
    fc2_ref[...]=rest[0:4*r]
    for c in range(4):
        fc1_ref[:,D*c:D*c+D]=rest[(4+c)*r:(5+c)*r]


def finish_sum(first,second,rest):
    near=pl.BlockSpec(memory_space=pltpu.VMEM)
    r=rest.shape[0]//8
    shapes=[(r,3*D),(r,D),(r,FF),(4*r,D),(128,r),(PACK,128)]
    return pl.pallas_call(finish_kernel,grid=(1,),
        in_specs=[near]*9,
        out_specs=[pl.BlockSpec(v,lambda i:(0,0)) for v in shapes[:5]]+[near],
        out_shape=[jax.ShapeDtypeStruct(v,f32) for v in shapes],
        compiler_params=pltpu.CompilerParams(vmem_limit_bytes=58<<20),name="finish_sum",
        cost_estimate=pl.CostEstimate(flops=1000,bytes_accessed=1000,transcendentals=0))(*first,*second,rest)


RATES=((2.0/math.sqrt(D),0.04),(2.0/math.sqrt(D//48),0.04),(2.0/math.sqrt(D),0.04),(2.0/math.sqrt(FF),0.04),(1.0,0.0))


def adam_kernel(fix_ref,square_ref,*refs):
    grads,states,outs=refs[:5],refs[5:20],refs[20:]
    norm=jnp.sqrt(jnp.sum(square_ref[...],axis=0,keepdims=True)[:,0:1])
    outs[0][...]=norm
    factor=jnp.minimum(1.0,CLIP_LIMIT/(norm+1e-06))
    for k,(rate,decay) in enumerate(RATES):
        weight,first,second=(ref[...] for ref in states[3*k:3*k+3])
        grad=factor*grads[k][0:weight.shape[0],:]
        first=BETA_ONE*first+(1.0-BETA_ONE)*grad
        second=BETA_TWO*second+(1.0-BETA_TWO)*grad*grad
        stride=first/fix_ref[0]/(jnp.sqrt(second/fix_ref[1])+ADAM_EPS)
        outs[3*k+1][...]=weight-rate*(stride+decay*weight)
        outs[3*k+2][...]=first
        outs[3*k+3][...]=second


def adam_all(fix,squares,grads,states):
    whole=lambda v: pl.BlockSpec(v,lambda i:(0,0))
    shapes=[(1,1)]+[v.shape for v in states]
    return pl.pallas_call(adam_kernel,grid=(1,),
        in_specs=[pl.BlockSpec(memory_space=pltpu.SMEM)]+[whole(v.shape) for v in (squares,*grads,*states)],
        out_specs=[whole(v) for v in shapes],
        out_shape=[jax.ShapeDtypeStruct(v,f32) for v in shapes],
        compiler_params=params(),name="adam_all")(fix,squares,*grads,*states)


def pack_rows(full):
    k = full.shape[1] // D
    return full.reshape(PACK, D // PACK, k, D).transpose(0, 2, 1, 3).reshape(PACK, -1, D)


def unpack_rows(packed):
    k = packed.shape[1] * PACK // D
    return packed.reshape(PACK, k, D // PACK, D).transpose(0, 2, 1, 3).reshape(D, k * D)


def swap(value, axis, size, flip):
    return lax.ppermute(value, axis, [(i, i ^ flip) for i in range(size)])


def places():
    inner = lax.axis_index("fsdp")
    return (lax.axis_index("dp"), inner // 2, inner % 2)


def first_stage(me, mine, other):
    got = swap(other, "fsdp", 8, 1)
    shape = (4, 4) + mine.shape[1:]
    return stage_sum(me, [mine.reshape(shape), got.reshape(shape)])


def second_stage(me, parts):
    keep, *send = parts
    return stage_sum(me, [keep] + [swap(v, "dp", 4, k + 1) for k, v in enumerate(send)])


def third_stage(parts):
    keep, *send = parts
    return [keep] + [swap(v, "fsdp", 8, 2 * k + 2) for k, v in enumerate(send)]


def to_pairs(w):
    return w.reshape(-1, 3, 6, 128).transpose(0, 2, 1, 3).reshape(-1, 3 * D)


def from_pairs(w):
    return w.reshape(-1, 6, 3, 128).transpose(0, 2, 1, 3).reshape(-1, 3 * D)


def make_local(fast):
    def gather(shard):
        return lax.all_gather(shard, AXES, axis=0, tiled=True)

    def scatter(full):
        return lax.psum_scatter(full, AXES, scatter_dimension=0, tiled=True)

    def local(
        tokens,
        cotangent,
        lengths,
        step,
        weight_qkv,
        weight_proj,
        weight_fc1,
        weight_fc2,
        vectors,
        first_qkv,
        second_qkv,
        first_proj,
        second_proj,
        first_fc1,
        second_fc1,
        first_fc2,
        second_fc2,
        first_vectors,
        second_vectors,
    ):
        per = weight_qkv.shape[0]
        cols = vectors.shape[1]
        rows_dev, row, _ = tokens.shape
        count = rows_dev * row
        inputs = tokens.reshape(count, D)
        centered, spread = norm_input(inputs)
        if fast:
            first, packed = pack_shards(weight_qkv, weight_proj, weight_fc1, weight_fc2, vectors)
            rest = lax.all_gather(packed, AXES, axis=0, tiled=False)
            along = jnp.stack([first] + [swap(first, "fsdp", 8, 2 * k) for k in (1, 2, 3)])
            parts = [along] + [swap(along, "dp", 4, k) for k in (1, 2, 3)]
            far = parts.pop()
            parts = [parts, [swap(v, "fsdp", 8, 1) for v in parts]]
            far, parts, centered, spread = lax.optimization_barrier((far, parts, centered, spread))
            parts = parts[0] + [far] + parts[1] + [swap(far, "fsdp", 8, 1)]
            place = jnp.stack(places()).astype(jnp.int32)
        else:
            low = [w.astype(bf) for w in (weight_qkv, weight_proj, weight_fc1, weight_fc2, vectors)]
            first = jnp.concatenate([to_pairs(low[0]), jnp.pad(low[4], ((0, 0), (0, 128 - cols)))], axis=1)
            whole = gather(first).reshape(4, 4, 2, D // PACK, WIDE)
            parts = [whole[k, :, c] for c in range(2) for k in range(4)]
            place = jnp.zeros((3,), jnp.int32)
            full = [gather(w) for w in low[1:4]]
            rest = jnp.concatenate(
                [full[2].reshape(PACK, FF // PACK, D), pack_rows(full[1]), pack_rows(full[0])], axis=1
            )
        left, qkv, vec, mats_qkv = qkv_forward(place, centered, parts)
        each = lambda v, b: v[b * row : (b + 1) * row]
        done = [attn_fwd(lengths[b : b + 1], each(qkv, b), each(left, b)) for b in range(rows_dev)]
        left = jnp.concatenate([v for v, _ in done], axis=0)
        result, normed_two, grad_down, active, grad_inner, grad_middle, right, grad_mixed, sums = mlp_block(
            inputs, left, cotangent.reshape(count, D), vec, rest
        )
        grads = fc_grads(active, grad_down, normed_two, grad_inner)
        if fast:
            rest_owned = lax.psum_scatter(grads, AXES, scatter_dimension=0, tiled=False)
        right = jnp.concatenate(
            [
                attn_bwd(
                    lengths[b : b + 1], each(qkv, b), each(left, b), each(grad_mixed, b), done[b][1], each(right, b)
                )
                for b in range(rows_dev)
            ],
            axis=0,
        )
        core = place[2:]
        mine_a, other_a = split_grad(core, left, right)
        if fast:
            me_dp, me_z = place[0:1], place[1:2]
            stage_a = first_stage(me_dp, mine_a, other_a)
            *stage_a, vec = lax.optimization_barrier((*stage_a, vec))
        grad_inputs, sums = input_grad(centered, spread, right, grad_middle, vec, sums, mats_qkv)
        if fast:
            stage_a = second_stage(me_z, stage_a)
            *stage_a, sums = lax.optimization_barrier((*stage_a, sums))
            owned_a = third_stage(stage_a)
            mine_b, other_b = split_grad(core, left, right, sums)
            *owned_a, other_b = lax.optimization_barrier((*owned_a, other_b))
            owned_b = third_stage(second_stage(me_z, first_stage(me_dp, mine_b, other_b)))
            *owned, squares = finish_sum(owned_a, owned_b, rest_owned)
            squares = lax.all_to_all(squares, AXES, 0, 0, tiled=True)
        else:
            mine_b, other_b = split_grad(core, left, right, sums)
            wide = FF // PACK
            part_a = jnp.stack([mine_a, other_a], axis=1).reshape(D, 2 * D)
            part_b = jnp.stack([mine_b, other_b], axis=1).reshape(D, 2 * D + 128)
            owned = [
                scatter(from_pairs(jnp.concatenate([part_a[:, D:], part_b[:, : 2 * D]], axis=1))),
                scatter(part_a[:, :D]),
                scatter(unpack_rows(grads[:, wide:])),
                scatter(grads[:, :wide].reshape(FF, D)),
                scatter(part_b[:, 2 * D : 2 * D + cols]),
            ]
            owned = [g.astype(f32) for g in owned]
            squares = jnp.full((1, 128), lax.psum(sum(jnp.sum(g * g) for g in owned), AXES))
            owned[4] = owned[4].T
        taken = step[0].astype(f32)
        fix = jnp.stack([1.0 - jnp.power(BETA_ONE, taken), 1.0 - jnp.power(BETA_TWO, taken)])
        states = (weight_qkv, first_qkv, second_qkv, weight_proj, first_proj, second_proj)
        states += (weight_fc1, first_fc1, second_fc1, weight_fc2, first_fc2, second_fc2)
        norm, *new = adam_all(fix, squares, owned, states + (vectors.T, first_vectors.T, second_vectors.T))
        new[12:] = [v.T for v in new[12:]]
        shape = (rows_dev, row, D)
        outs = [result.reshape(shape), grad_inputs.reshape(shape), norm.reshape(1)] + new[0::3]
        for k in range(5):
            outs += new[3 * k + 1 : 3 * k + 3]
        return tuple(outs)

    return local


def solution(mesh):
    rows = P(AXES, None)
    tokens = P(AXES, None, None)
    fast = (mesh.shape["dp"], mesh.shape["fsdp"]) == (4, 8)
    return jax.shard_map(
        make_local(fast),
        mesh=mesh,
        in_specs=(tokens, tokens, rows, P()) + (rows,) * 15,
        out_specs=(tokens, tokens, P()) + (rows,) * 15,
        check_vma=False,
    )
```
